512 devices in a mesh: groups: 2 (over y), head: 64 (over z, core), state: 4 (over x).
Axes of the slice: x: 4, y: 2, z: 32, core: 2. Of those that a mesh axis runs over, the one named last changes fastest.
The devices are a block of a 4x8x32 slice.
Arguments:
- tokens: bfloat16 [512, 2048], P(('groups', 'head'), 'state'), parts along dimension 0, may hold values from -20 to 20
- mixer_norm: float32 [2048], P('state'), may hold values from 0.1 to 1.9
- input_proj: bfloat16 [2, 2048, 8192], P(None, 'state', 'head'), may hold values from -0.125 to 0.125
- conv_weight: float32 [4, 8192], P(None, 'head'), may hold values from -3 to 3
- conv_bias: float32 [8192], P('head'), may hold values from -3 to 3
- conv_state: float32 [3, 512, 8192], P(None, 'groups', 'head'), parts along dimension 1, may hold values from -6 to 6
- state_proj: bfloat16 [8192, 288], P('head'), may hold values from -0.125 to 0.125
- step_gain: float32 [256], replicated, may hold values from 0.1 to 1.9
- step_proj: bfloat16 [256, 8192], P(None, 'head'), may hold values from -0.375 to 0.375
- step_bias: float32 [8192], P('head'), may hold values from -6 to -1
- decay_log: float32 [16, 8192], P('state', 'head'), may hold values from 0 to 2.77
- skip_gain: float32 [8192], P('head'), may hold values from 0.5 to 1.5
- ssm_state: float32 [16, 512, 8192], P('state', 'groups', 'head'), parts along dimension 1, may hold values from -6 to 6
- output_proj: bfloat16 [8192, 2048], P('head', 'state'), may hold values from -0.0625 to 0.0625
- moe_norm: float32 [2048], replicated, may hold values from 0.1 to 1.9
- router_weight: float32 [2048, 8], replicated, may hold values from -0.125 to 0.125
- expert_ids: int32 [512, 2], P(('groups', 'head')), parts along dimension 0, may hold values from 0 to 7, as said below
- slot_ids: int32 [512, 2], P(('groups', 'head')), parts along dimension 0, may hold values from 0 to 3, as said below
- gate_proj: bfloat16 [64, 2048, 896], P('head', None, 'state'), may hold values from -0.125 to 0.125
- up_proj: bfloat16 [64, 2048, 896], P('head', None, 'state'), may hold values from -0.125 to 0.125
- down_proj: bfloat16 [64, 896, 2048], P('head', 'state'), may hold values from -0.0625 to 0.0625
Outputs:
- layer_out: bfloat16 [512, 2048], P(('groups', 'head'), 'state'), parts along dimension 0
- new_conv: float32 [3, 512, 8192], P(None, 'groups', 'head'), parts along dimension 1
- new_state: float32 [16, 512, 8192], P('state', 'groups', 'head'), parts along dimension 1
- expert_load: float32 [16], P('groups'), parts along dimension 0
- aux_loss: float32 [2], P('groups'), parts along dimension 0
The draws below stay inside these ranges and needn't reach their ends.
There are 2 independent parts, one for each index of `groups`. The reference program is written for one: setup_inputs(seed, part) draws one part's arguments, and reference() takes and returns one part's arrays. A program takes and returns all parts, laid end to end along the dimension named above; an argument that names none is the same for every part. Nothing has to cross between parts.
Inputs may be any that keep to these rules, and one draw needn't show every extreme that they name: `expert_ids`: each row names 2 different experts. One expert, the same on every device, is named by every row. `slot_ids`: among the choices of one aligned block of 4 rows that name one expert, the slot positions are distinct and run from 0 to their count less one.
All inputs are finite; a program needn't handle non-finite values.
Results may differ from the reference program's by a relative error of at most 0.007.
Values may be sent and summed in bfloat16 or wider, within the bound.
A program may use at most 64 MiB of HBM per device.

```python
import math
import jax
import jax.numpy as jnp
from jax import lax

D = 2048
D_INNER = 8192
D_STATE = 16
DT_RANK = 256
CONV = 4
EXPERTS = 8
TOPK = 2
FF = 7168
SEQ_DEV = 4
BATCH = 256
CAP = 2
SPLIT = 8
EXP_ROWS = 64
FF_PART = 896


def routing_pair(key):
    base_key = jax.random.fold_in(key, 11)
    key_hot = jax.random.fold_in(base_key, 0)
    key_score = jax.random.fold_in(base_key, 2)
    key_prio = jax.random.fold_in(base_key, 3)
    blocks = BATCH // SEQ_DEV
    assigned = SEQ_DEV * TOPK
    hot_expert = jax.random.randint(key_hot, (), 0, EXPERTS)
    expert_score = jax.random.randint(key_score, (blocks, SEQ_DEV, EXPERTS), 0, 1 << 20) * EXPERTS + jnp.arange(EXPERTS, dtype=jnp.int32)
    is_hot = jnp.arange(EXPERTS, dtype=jnp.int32) == hot_expert
    expert_score = jnp.where(is_hot[None, None, :], expert_score + (1 << 30), expert_score)
    chosen_ids = lax.top_k(expert_score, TOPK)[1].astype(jnp.int32)
    flat_ids = chosen_ids.reshape(blocks, assigned)
    priority = jax.random.randint(key_prio, (blocks, assigned), 0, 1 << 20) * assigned + jnp.arange(assigned, dtype=jnp.int32)
    earlier = (flat_ids[:, :, None] == flat_ids[:, None, :]) & (priority[:, None, :] < priority[:, :, None])
    slot_pos = jnp.sum(earlier.astype(jnp.int32), axis=2)
    return (chosen_ids.reshape(BATCH, TOPK), slot_pos.reshape(BATCH, TOPK).astype(jnp.int32))


def draw_expert_ids(key, part):
    return routing_pair(key)[0]


def draw_slot_ids(key, part):
    return routing_pair(key)[1]


def draw_tokens(key, part):
    base_key = jax.random.fold_in(key, 5)
    key_scale, key_value = jax.random.split(base_key, 2)
    row_scale = jnp.exp(jax.random.uniform(key_scale, (BATCH, 1), jnp.float32, math.log(0.3), math.log(3.0)))
    values = jax.random.normal(key_value, (BATCH, D), jnp.float32)
    return jnp.clip(values * row_scale, -20.0, 20.0).astype(jnp.bfloat16)


def block_scale(rng, dims, cuts, low, top_value):
    def one(position, blocks):
        heights = jax.random.uniform(jax.random.fold_in(jax.random.fold_in(rng, 6), position), (blocks,), jnp.float32, low / len(cuts), top_value / len(cuts))
        return jnp.repeat(jnp.exp(heights), dims[position] // blocks).reshape((-1,) + (1,) * (len(dims) - position - 1))

    loudness = one(*cuts[0])
    for cut in cuts[1:]:
        loudness = loudness * one(*cut)
    return loudness


def noise(rng, shape, spread, most, cuts=(), held_as=jnp.bfloat16):
    entries = jax.random.normal(rng, shape, jnp.float32) * spread
    if len(cuts) > 0:
        entries = block_scale(rng, shape, cuts, -0.22, 0.18) * entries
    return jnp.clip(entries, min=-most, max=most).astype(held_as)


def setup_inputs(seed: int = 0, part: int = 0) -> dict:
    key_list = jax.random.split(jax.random.key(seed), 22)
    own_keys = jax.random.split(jax.random.fold_in(key_list[21], part), 22)
    return {
        "tokens": draw_tokens(jax.random.fold_in(jax.random.fold_in(key_list[21], part), 71), part),
        "mixer_norm": jnp.clip(1.0 + 0.18 * jax.random.normal(key_list[1], (D,), jnp.float32), 0.1, 1.9),
        "input_proj": noise(key_list[2], (2, D, D_INNER), D ** -0.5, 0.125, ((1, 4), (2, 64))),
        "conv_weight": noise(key_list[3], (CONV, D_INNER), CONV ** -0.5, 3.0, ((1, 64),), jnp.float32),
        "conv_bias": noise(key_list[4], (D_INNER,), 0.5, 3.0, ((0, 64),), jnp.float32),
        "conv_state": noise(own_keys[5], (CONV - 1, BATCH, D_INNER), 1.0, 6.0, ((2, 64),), jnp.float32),
        "state_proj": noise(key_list[6], (D_INNER, DT_RANK + 2 * D_STATE), (D_INNER // 4) ** -0.5, 0.125, ((0, 64),)),
        "step_gain": jnp.clip(1.0 + 0.18 * jax.random.normal(key_list[7], (DT_RANK,), jnp.float32), 0.1, 1.9),
        "step_proj": noise(key_list[8], (DT_RANK, D_INNER), DT_RANK ** -0.5, 0.375, ((1, 64),)),
        "step_bias": jnp.clip(-6.0 + 5.0 * jax.random.uniform(key_list[9], (D_INNER,), jnp.float32) ** block_scale(key_list[9], (D_INNER,), ((0, 64),), -0.2, 0.2), -6.0, -1.0),
        "decay_log": jnp.clip(2.77 * jax.random.uniform(key_list[10], (D_STATE, D_INNER), jnp.float32) ** block_scale(key_list[10], (D_STATE, D_INNER), ((0, 4), (1, 64)), -0.2, 0.2), 0.0, 2.77),
        "skip_gain": jnp.clip(0.5 + 1.0 * jax.random.uniform(key_list[11], (D_INNER,), jnp.float32) ** block_scale(key_list[11], (D_INNER,), ((0, 64),), -0.2, 0.2), 0.5, 1.5),
        "ssm_state": noise(own_keys[12], (D_STATE, BATCH, D_INNER), 1.0, 6.0, ((0, 4), (2, 64)), jnp.float32),
        "output_proj": noise(key_list[13], (D_INNER, D), D_INNER ** -0.5, 0.0625, ((0, 64), (1, 4))),
        "moe_norm": jnp.clip(1.0 + 0.18 * jax.random.normal(key_list[14], (D,), jnp.float32), 0.1, 1.9),
        "router_weight": noise(key_list[15], (D, EXPERTS), D ** -0.5, 0.125, (), jnp.float32),
        "expert_ids": draw_expert_ids(jax.random.fold_in(jax.random.fold_in(key_list[21], part), 71), part),
        "slot_ids": draw_slot_ids(jax.random.fold_in(jax.random.fold_in(key_list[21], part), 71), part),
        "gate_proj": noise(key_list[18], (EXP_ROWS, D, FF_PART), D ** -0.5, 0.125, ((0, 64), (2, 4))),
        "up_proj": noise(key_list[19], (EXP_ROWS, D, FF_PART), D ** -0.5, 0.125, ((0, 64), (2, 4))),
        "down_proj": noise(key_list[20], (EXP_ROWS, FF_PART, D), FF ** -0.5, 0.0625, ((0, 64), (1, 4))),
    }


def reference(tokens, mixer_norm, input_proj, conv_weight, conv_bias, conv_state, state_proj, step_gain, step_proj, step_bias, decay_log, skip_gain, ssm_state, output_proj, moe_norm, router_weight, expert_ids, slot_ids, gate_proj, up_proj, down_proj):
    tok_f32 = tokens.astype(jnp.float32)
    inv_first = lax.rsqrt(lax.optimization_barrier(jnp.mean(tok_f32 * tok_f32, axis=1, keepdims=True)) + 1e-05)
    normed = (tok_f32 * inv_first * mixer_norm).astype(jnp.bfloat16)
    conv_input = jnp.dot(normed, input_proj[0], preferred_element_type=jnp.float32)
    gate_branch = jnp.dot(normed, input_proj[1], preferred_element_type=jnp.float32)
    window = jnp.concatenate([conv_state, conv_input[None]], axis=0)
    conv_out = jax.nn.silu(lax.optimization_barrier(jnp.sum(conv_weight[:, None, :] * window, axis=0)) + conv_bias)
    new_conv = window[1:]
    projected = jnp.dot(conv_out.astype(jnp.bfloat16), state_proj, preferred_element_type=jnp.float32)
    step_low = projected[:, :DT_RANK]
    b_input = projected[:, DT_RANK:DT_RANK + D_STATE]
    c_output = projected[:, DT_RANK + D_STATE:]
    step_inv = lax.rsqrt(lax.optimization_barrier(jnp.mean(step_low * step_low, axis=1, keepdims=True)) + 1e-06)
    step_normed = (step_low * step_inv * step_gain).astype(jnp.bfloat16)
    step_size = jax.nn.softplus(jnp.dot(step_normed, step_proj, preferred_element_type=jnp.float32) + step_bias)
    decay_rate = jnp.exp(-step_size[None] * jnp.exp(decay_log)[:, None, :])
    new_state = decay_rate * ssm_state + step_size[None] * b_input.T[:, :, None] * conv_out[None]
    readout = lax.optimization_barrier(jnp.sum(c_output.T[:, :, None] * new_state, axis=0))
    mixer_act = ((readout + skip_gain * conv_out) * jax.nn.silu(gate_branch)).astype(jnp.bfloat16)
    residual = (tok_f32 + jnp.dot(mixer_act, output_proj, preferred_element_type=jnp.float32)).astype(jnp.bfloat16)
    resid_f32 = residual.astype(jnp.float32)
    inv_second = lax.rsqrt(lax.optimization_barrier(jnp.mean(resid_f32 * resid_f32, axis=1, keepdims=True)) + 1e-05)
    scaled = resid_f32 * moe_norm
    row_normed = (scaled * inv_second).astype(jnp.bfloat16)
    logits = inv_second * jnp.dot(scaled, router_weight, precision=lax.Precision.HIGHEST)
    expert_hit = expert_ids[:, :, None] == jnp.arange(EXPERTS, dtype=jnp.int32)[None, None, :]
    chosen = lax.optimization_barrier(jnp.sum(jnp.where(expert_hit, logits[:, None, :], 0.0), axis=2))
    gate_probs = jax.nn.sigmoid(chosen - chosen[:, ::-1])
    kept_mask = slot_ids < CAP
    mix_weight = jnp.where(kept_mask, gate_probs, 0.0)
    token_weight = lax.optimization_barrier(jnp.sum(jnp.where(expert_hit, mix_weight[:, :, None], 0.0), axis=1))
    gate_all = gate_proj.reshape(EXPERTS, SPLIT, D, FF_PART).transpose(0, 2, 1, 3).reshape(EXPERTS, D, SPLIT * FF_PART)
    up_all = up_proj.reshape(EXPERTS, SPLIT, D, FF_PART).transpose(0, 2, 1, 3).reshape(EXPERTS, D, SPLIT * FF_PART)
    down_all = down_proj.reshape(EXPERTS, SPLIT * FF_PART, D)

    def one_expert(carry, inputs):
        gate_one, up_one, down_one, weight_one = inputs
        gate_val = jnp.dot(row_normed, gate_one, preferred_element_type=jnp.float32)
        up_val = jnp.dot(row_normed, up_one, preferred_element_type=jnp.float32)
        hidden = (jax.nn.silu(gate_val) * up_val).astype(jnp.bfloat16)
        expert_value = jnp.dot(hidden, down_one, preferred_element_type=jnp.float32)
        return (carry + weight_one[:, None] * expert_value, None)
    expert_mix, _ = lax.scan(one_expert, jnp.zeros((BATCH, D), jnp.float32), (gate_all, up_all, down_all, token_weight.T))
    layer_out = (resid_f32 + expert_mix).astype(jnp.bfloat16)
    expert_load = lax.optimization_barrier(jnp.sum(jnp.where(expert_hit & kept_mask[:, :, None], 1.0, 0.0), axis=(0, 1))).astype(jnp.float32)
    mean_prob = lax.optimization_barrier(jnp.mean(jax.nn.sigmoid(logits), axis=0))
    aux_loss = (EXPERTS * jnp.sum(expert_load / (BATCH * TOPK) * mean_prob)).reshape(1)
    return (layer_out, new_conv, new_state, expert_load, aux_loss)
```

```python
import functools

import jax
import jax.numpy as jnp
from jax import lax
from jax.experimental import pallas as pl
from jax.experimental.pallas import tpu as pltpu
from jax.sharding import PartitionSpec as P

EXPERTS = 8
TOPK = 2
CAP = 2
LANES = 128
NORM_EPS = 1e-05
STEP_EPS = 1e-06
MESH = pl.DeviceIdType.MESH
F32 = jnp.float32
BF16 = jnp.bfloat16
HI = lax.Precision.HIGHEST


def div(a, n):
    assert n & (n - 1) == 0
    return lax.shift_right_logical(a, jnp.int32(n.bit_length() - 1)) if n > 1 else a


def mod(a, n):
    assert n & (n - 1) == 0
    return a & (n - 1)


def grid_of(rows, cols):
    return (
        lax.broadcasted_iota(jnp.int32, (rows, cols), 0),
        lax.broadcasted_iota(jnp.int32, (rows, cols), 1),
    )


def ones_where(cond, dtype=BF16):
    return jnp.where(cond, 1.0, 0.0).astype(dtype)


def mm(a, b, precision=None):
    return jnp.dot(a, b, preferred_element_type=F32, precision=precision)


def mm_nt(a, b, precision=None):
    return lax.dot_general(
        a, b, (((1,), (1,)), ((), ())), preferred_element_type=F32, precision=precision
    )


def silu(v):
    return v * jax.nn.sigmoid(v)


def softplus(v):
    return jnp.maximum(v, 0.0) + jnp.log1p(jnp.exp(-jnp.abs(v)))


def by_distance(n):
    return sorted(range(1, n), key=lambda k: -min(k, n - k))


STAGES = (
    "tok_far", "tok_near", "branch", "gate", "square", "proj_near", "proj_far", "low_near", "low_state",
    "read", "mix_near", "mix_far", "stat", "row_far", "row_near", "row_state", "out_state", "out_near",
    "out_far", "aux_near", "aux_far",
)
LOADS = ("win", "conv", "sproj", "tproj", "ssm", "oproj", "router", "gate", "up", "down")


def step_kernel(
    n,
    tok_ref, ids_ref, mixn_ref, win_hbm, cw_ref, cb_ref, cs_hbm, sp_hbm, sg_ref, tp_hbm, sb_ref,
    dl_ref, sk_ref, ssm_hbm, op_hbm, mn_ref, rw_hbm, gp_hbm, up_hbm, dn_hbm,
    lo_ref, cin_ref, ns_ref, aux_ref,
    win, cs, sp, tp, ssm, op, rw, gp, up, dn,
    pick, pick_row, G, XC, XG, XS, cob, P2, R2, F2, S2, XR, N3, R3, F3, Q3, ST, F4, G4, rows, rn,
    X5, Y5, N5, R5, F5, Q5, AN, AF,
    send_sem, recv_sem, load_sem,
):
    head = lax.axis_index("head")
    x = lax.axis_index("state")
    b = head // n.NM
    m = head % n.NM
    X, NB, NM, OWN, J, R, T, C, S = n.X, n.NB, n.NM, n.OWN, n.J, n.R, n.T, n.C, n.S

    far = {k: {"head": ((b + k) % NB) * NM + m} for k in range(1, NB)}
    near = {k: {"head": b * NM + (m + k) % NM} for k in range(1, NM)}
    side = {k: {"state": (x + k) % X} for k in range(1, X)}

    barrier = pltpu.get_barrier_semaphore()
    for group in (far, near, side):
        for k in group:
            pl.semaphore_signal(barrier, inc=1, device_id=group[k], device_id_type=MESH)

    loads = {}
    for k, (src, dst) in enumerate(
        (
            (win_hbm, win), (cs_hbm, cs), (sp_hbm, sp), (tp_hbm, tp), (ssm_hbm, ssm), (op_hbm, op),
            (rw_hbm.at[pl.ds(pl.multiple_of(x * n.Q, n.Q), n.Q), :], rw),
            (gp_hbm, gp), (up_hbm, up), (dn_hbm, dn),
        )
    ):
        loads[LOADS[k]] = pltpu.make_async_copy(src, dst, load_sem.at[k])
        loads[LOADS[k]].start()

    pending = []

    def exchange(stage, group, pair):
        at = STAGES.index(stage)
        copies = []
        for k in by_distance(len(group) + 1):
            src, dst = pair(k)
            copy = pltpu.make_async_remote_copy(
                src_ref=src, dst_ref=dst, send_sem=send_sem.at[at, k - 1], recv_sem=recv_sem.at[at, k - 1],
                device_id=group[k], device_id_type=MESH,
            )
            copy.start()
            copies.append(copy)
        pending.extend(copies)
        return copies

    def arrive(copies):
        for copy in copies:
            copy.wait_recv()

    tok_bf = tok_ref[...]
    G[m, b] = tok_bf
    pl.semaphore_wait(barrier, (NB - 1) + (NM - 1) + (X - 1))
    sent = exchange("tok_far", far, lambda k: (tok_ref, G.at[m, b]))

    r_i, c_i = grid_of(T, n.H * R)
    tok_of = (div(mod(c_i, NB * R), R) * NM + div(c_i, NB * R)) * OWN + mod(c_i, OWN)
    match = tok_of == r_i
    which = mod(div(c_i, OWN), J)
    for j in range(J):
        pick[j] = ones_where(match & (which == j))
    r_i, c_i = grid_of(n.SLOTS, n.SLOTS * J)
    match = div(c_i, J * CAP) * CAP + mod(c_i, CAP) == r_i
    which = mod(div(c_i, CAP), J)
    for j in range(J):
        pick_row[j] = ones_where(match & (which == j))

    arrive(sent)
    sent = exchange("tok_near", near, lambda k: (G.at[m], G.at[m]))
    loads["win"].wait()
    arrive(sent)

    gathered = G[...].reshape(n.H * R, LANES)
    conv_part = jnp.zeros((T, C), F32)
    gate_part = jnp.zeros((T, C), F32)
    squares = jnp.zeros((T, 1), F32)
    for j in range(J):
        tok_j = mm(pick[j], gathered)
        squares += jnp.sum(tok_j * tok_j, axis=1, keepdims=True)
        wide = (tok_j * mixn_ref[j : j + 1, :]).astype(BF16)
        conv_part += mm(wide, win[0, j * LANES : (j + 1) * LANES, :])
        gate_part += mm(wide, win[1, j * LANES : (j + 1) * LANES, :])
    XS[x] = jnp.broadcast_to(squares, (T, LANES)).T[:8, :]
    XC[x] = conv_part.astype(BF16)
    sent_sq = exchange("square", side, lambda k: (XS.at[x], XS.at[x]))
    sent = exchange("branch", side, lambda k: (XC.at[x], XC.at[x]))
    XG[x] = gate_part.astype(BF16)
    sent_gate = exchange("gate", side, lambda k: (XG.at[x], XG.at[x]))

    loads["conv"].wait()
    window = cb_ref[...] + sum(cw_ref[k : k + 1, :] * cs[k] for k in range(n.CONV - 1))
    loads["sproj"].wait()
    P2[...] = jnp.zeros_like(P2)
    arrive(sent_sq)
    total = XS[0]
    for k in range(1, X):
        total += XS[k]
    inv_first = lax.rsqrt(jnp.broadcast_to(total[:1, :], (LANES, T)).T[:, :1] / n.D + NORM_EPS)
    arrive(sent)
    conv_in = XC[0].astype(F32)
    for k in range(1, X):
        conv_in += XC[k].astype(F32)
    conv_in = conv_in * inv_first
    cin_ref[...] = conv_in
    conv_out = silu(window + cw_ref[n.CONV - 1 : n.CONV, :] * conv_in)
    cob[...] = conv_out.astype(BF16)

    quarter = T // X
    part = mm(cob[pl.ds(pl.multiple_of(x * quarter, quarter), quarter), :], sp[...])
    P2[:, :, : n.PROJ] = part.reshape(NM, n.TB, n.PROJ)
    R2[m] = P2[m]
    sent = exchange("proj_near", near, lambda k: (P2.at[(m + k) % NM], R2.at[m]))
    arrive(sent)
    total = R2[0]
    for k in range(1, NM):
        total += R2[k]
    F2[b] = total.astype(BF16)
    sent = exchange("proj_far", far, lambda k: (F2.at[b], F2.at[b]))
    for name in ("tproj", "ssm"):
        loads[name].wait()
    arrive(sent)
    total = F2[0].astype(F32)
    for k in range(1, NB):
        total += F2[k].astype(F32)
    S2[x, m] = total.astype(BF16)
    sent = exchange("low_near", near, lambda k: (S2.at[x, m], S2.at[x, m]))
    arrive(sent)
    sent = exchange("low_state", side, lambda k: (S2.at[x], S2.at[x]))
    arrive(sent_gate)
    gate = XG[0].astype(F32)
    for k in range(1, X):
        gate += XG[k].astype(F32)
    gate = silu(gate * inv_first)
    rates = [jnp.exp(dl_ref[k : k + 1, :]) for k in range(S)]
    arrive(sent)

    projected = S2[...].astype(F32).reshape(T, n.PW)
    low = projected[:, : n.RANK]
    step_inv = lax.rsqrt(jnp.mean(low * low, axis=1, keepdims=True) + STEP_EPS)
    step_normed = (low * step_inv * sg_ref[...]).astype(BF16)
    step_size = softplus(mm(step_normed, tp[...]) + sb_ref[...])
    vectors = projected[:, n.RANK :].astype(BF16)
    rows_i, _ = grid_of(LANES, C)
    driven = step_size * conv_out
    read = jnp.zeros((T, C), F32)
    for k in range(S):
        b_in = mm(vectors, ones_where(rows_i == x * S + k))
        c_out = mm(vectors, ones_where(rows_i == n.STATE + x * S + k))
        fresh = jnp.exp(-step_size * rates[k]) * ssm[k] + driven * b_in
        ns_ref[k] = fresh
        read += c_out * fresh
    XR[x] = read.astype(BF16)
    sent = exchange("read", side, lambda k: (XR.at[x], XR.at[x]))
    loads["oproj"].wait()
    r_i, c_i = grid_of(T, T)
    source = (div(mod(r_i, NB * OWN), OWN) * NM + div(r_i, NB * OWN)) * OWN + mod(r_i, OWN)
    by_member = ones_where(source == c_i)
    arrive(sent)
    read = XR[0].astype(F32)
    for k in range(1, X):
        read += XR[k].astype(F32)
    act = ((read + sk_ref[...] * conv_out) * gate).astype(BF16)
    act = mm(by_member, act).astype(BF16)
    N3[...] = mm(act, op[...]).astype(BF16).reshape(NM, NB * OWN, n.Q)
    R3[m] = N3[m]
    sent = exchange("mix_near", near, lambda k: (N3.at[(m + k) % NM], R3.at[m]))
    arrive(sent)
    total = R3[0].astype(F32)
    for k in range(1, NM):
        total += R3[k].astype(F32)
    total = total.astype(BF16)
    r_i, c_i = grid_of(NB * R, NB * OWN)
    match = div(r_i, R) * OWN + mod(r_i, OWN) == c_i
    which = mod(div(r_i, OWN), J)
    spread = jnp.zeros((NB * R, LANES), F32)
    for j in range(J):
        spread += mm(ones_where(match & (which == j)), total[:, j * LANES : (j + 1) * LANES])
    F3[...] = spread.astype(BF16).reshape(NB, R, LANES)
    Q3[b] = F3[b]
    sent = exchange("mix_far", far, lambda k: (F3.at[(b + k) % NB], Q3.at[b]))
    loads["router"].wait()
    arrive(sent)
    total = Q3[0].astype(F32)
    for k in range(1, NB):
        total += Q3[k].astype(F32)

    resid_bf = (tok_bf.astype(F32) + total).astype(BF16)
    resid = resid_bf.astype(F32)
    row_i, lane_i = grid_of(R, LANES)
    hits, kept, slots = [], [], []
    for k in range(TOPK):
        e_k, s_k = ids_ref[:, k : k + 1], ids_ref[:, TOPK + k : TOPK + k + 1]
        keep = s_k < CAP
        hits.append(lane_i == e_k)
        kept.append(keep)
        slots.append((lane_i == e_k * CAP + s_k) & keep)
    dispatch = sum(ones_where(s, F32) for s in slots).astype(BF16)
    d_i, q_i = grid_of(NB * J * CAP, LANES)
    slot_of = ones_where(q_i == div(d_i, J * CAP) * CAP + mod(d_i, CAP))
    d_i, c_i = grid_of(NB * J * CAP, R)
    chosen_rows = jnp.where(
        mod(div(d_i, CAP), J) == div(c_i, OWN), mm_nt(slot_of, dispatch), 0.0
    ).astype(BF16)
    F4[...] = mm(chosen_rows, resid_bf).reshape(NB, J * CAP, LANES).astype(BF16)
    G4[x, m, b] = F4[b]
    sent = exchange("row_far", far, lambda k: (F4.at[(b + k) % NB], G4.at[x, m, b]))

    gain = jnp.zeros((R, LANES), F32)
    for j in range(J):
        gain = jnp.where(div(row_i, OWN) == j, mn_ref[pl.ds(x * J + j, 1), :], gain)
    scaled = resid * gain
    raw = jnp.zeros((R, EXPERTS), F32)
    for j in range(J):
        raw += mm(
            jnp.where(div(row_i, OWN) == j, scaled, 0.0), rw[j * LANES : (j + 1) * LANES, :], HI
        )
    ST[x] = jnp.broadcast_to(jnp.sum(resid * resid, axis=1, keepdims=True), (R, LANES))
    ST[x, :, :EXPERTS] = raw
    sent_stat = exchange("stat", side, lambda k: (ST.at[x], ST.at[x]))
    arrive(sent_stat)
    total = ST[0]
    for k in range(1, X):
        total += ST[k]
    r_i, c_i = grid_of(R, R)
    total = mm(ones_where(mod(r_i, OWN) == mod(c_i, OWN), F32), total, HI)
    inv_second = lax.rsqrt(total[:, EXPERTS : EXPERTS + 1] / n.D + NORM_EPS)
    logits = inv_second * total
    chosen = [jnp.sum(jnp.where(hit, logits, 0.0), axis=1, keepdims=True) for hit in hits]
    mixing = jnp.zeros((R, LANES), F32)
    for k in range(TOPK):
        weight = jax.nn.sigmoid(chosen[k] - chosen[1 - k])
        mixing += jnp.where(slots[k], weight, 0.0)
    first = row_i < OWN
    load = sum(ones_where(hits[k] & kept[k] & first, F32) for k in range(TOPK))
    load = jnp.sum(load, axis=0, keepdims=True)
    prob = jnp.where(first & (lane_i < EXPERTS), jax.nn.sigmoid(logits), 0.0)
    prob = jnp.sum(prob, axis=0, keepdims=True)
    a_i, l_i = grid_of(8, LANES)
    AN[m] = jnp.where(a_i == 0, load, jnp.where(a_i == 1, prob, 0.0))
    sent_aux = exchange("aux_near", near, lambda k: (AN.at[m], AN.at[m]))
    d_i, q_i = grid_of(R, NB * J * CAP)
    combine = jnp.where(
        mod(div(q_i, CAP), J) == div(d_i, OWN), mm_nt(mixing, slot_of.astype(F32), HI), 0.0
    )
    for name in ("gate", "up", "down"):
        loads[name].wait()

    arrive(sent)
    sent = exchange("row_near", near, lambda k: (G4.at[x, m], G4.at[x, m]))
    arrive(sent_aux)
    total = AN[0]
    for k in range(1, NM):
        total += AN[k]
    AF[b] = total
    sent_aux = exchange("aux_far", far, lambda k: (AF.at[b], AF.at[b]))
    arrive(sent)
    sent = exchange("row_state", side, lambda k: (G4.at[x], G4.at[x]))
    arrive(sent)

    squares = jnp.zeros((n.SLOTS, 1), F32)
    for k in range(X):
        source = G4[k].astype(F32).reshape(n.SLOTS * J, LANES).astype(BF16)
        for j in range(J):
            at = k * J + j
            block = mm(pick_row[j], source)
            squares += jnp.sum(block * block, axis=1, keepdims=True)
            rows[:, at * LANES : (at + 1) * LANES] = block * mn_ref[at : at + 1, :]
    inv_rows = lax.rsqrt(squares / n.D + NORM_EPS)
    rn[...] = (rows[...] * inv_rows).astype(BF16)
    normed = rn[...]
    hidden = (silu(mm(normed, gp[0])) * mm(normed, up[0])).astype(BF16)
    for k in range(X):
        X5[k] = mm(hidden, dn[0, :, k * n.Q : (k + 1) * n.Q]).astype(BF16)
    Y5[x] = X5[x]
    sent = exchange("out_state", side, lambda k: (X5.at[(x + k) % X], Y5.at[x]))
    arrive(sent)
    total = Y5[0].astype(F32)
    for k in range(1, X):
        total += Y5[k].astype(F32)
    N5[...] = total.reshape(NM, NB * CAP, n.Q).astype(BF16)
    R5[m] = N5[m]
    sent = exchange("out_near", near, lambda k: (N5.at[(m + k) % NM], R5.at[m]))
    arrive(sent)
    total = R5[0].astype(F32)
    for k in range(1, NM):
        total += R5[k].astype(F32)
    total = total.astype(BF16)
    r_i, c_i = grid_of(NB * J * CAP, NB * CAP)
    match = div(r_i, J * CAP) * CAP + mod(r_i, CAP) == c_i
    which = mod(div(r_i, CAP), J)
    spread = jnp.zeros((NB * J * CAP, LANES), F32)
    for j in range(J):
        spread += mm(ones_where(match & (which == j)), total[:, j * LANES : (j + 1) * LANES])
    F5[...] = spread.reshape(NB, J * CAP, LANES).astype(BF16)
    Q5[b] = F5[b]
    sent = exchange("out_far", far, lambda k: (F5.at[(b + k) % NB], Q5.at[b]))
    arrive(sent_aux)
    total = AF[0]
    for k in range(1, NB):
        total += AF[k]
    share = total[0:1, :] / (T * TOPK) * (total[1:2, :] / T)
    loss = EXPERTS * jnp.sum(jnp.where(l_i[:1] < EXPERTS, share, 0.0), axis=1, keepdims=True)
    aux_ref[...] = jnp.where(a_i == 0, total[0:1, :], loss)
    arrive(sent)
    back = Q5[...].astype(F32).reshape(NB * J * CAP, LANES)
    lo_ref[...] = (resid + mm(combine, back, HI)).astype(BF16)
    for copy in pending:
        copy.wait_send()


class Sizes:
    pass


def per_device(
    head_count, state_count,
    tokens, mixer_norm, input_proj, conv_weight, conv_bias, conv_state, state_proj, step_gain, step_proj,
    step_bias, decay_log, skip_gain, ssm_state, output_proj, moe_norm, router_weight, expert_ids, slot_ids,
    gate_proj, up_proj, down_proj,
):
    n = Sizes()
    n.H, n.X, n.NB = head_count, state_count, EXPERTS
    n.NM = n.H // n.NB
    n.OWN, n.Q = tokens.shape
    n.J = n.Q // LANES
    n.R = n.OWN * n.J
    n.D = n.Q * n.X
    n.CONV = conv_weight.shape[0]
    _, n.T, n.C = conv_state.shape
    n.S = decay_log.shape[0]
    n.STATE = n.S * n.X
    n.RANK, n.PROJ = step_proj.shape[0], state_proj.shape[1]
    n.PW = -(-n.PROJ // LANES) * LANES
    n.TB = n.T // n.X // n.NM
    n.SLOTS = n.NM * n.NB * CAP
    n.FF = gate_proj.shape[2]

    tok = tokens.reshape(n.OWN, n.J, LANES).transpose(1, 0, 2).reshape(n.R, LANES)
    ids = jnp.tile(jnp.concatenate([expert_ids, slot_ids], axis=1), (n.J, 1))
    vm = pl.BlockSpec(memory_space=pltpu.VMEM)
    hbm = pl.BlockSpec(memory_space=pl.ANY)
    V = pltpu.VMEM
    operands = (
        (tok, vm), (ids, vm), (mixer_norm.reshape(n.J, LANES), vm), (input_proj, hbm), (conv_weight, vm),
        (conv_bias.reshape(1, -1), vm), (conv_state, hbm), (state_proj, hbm), (step_gain.reshape(1, -1), vm),
        (step_proj, hbm), (step_bias.reshape(1, -1), vm), (decay_log, vm), (skip_gain.reshape(1, -1), vm),
        (ssm_state, hbm), (output_proj, hbm), (moe_norm.reshape(-1, LANES), vm), (router_weight, hbm),
        (gate_proj, hbm), (up_proj, hbm), (down_proj, hbm),
    )
    wide = n.J * CAP
    scratch = [
        V(input_proj.shape, BF16), V(conv_state.shape, F32), V(state_proj.shape, BF16), V(step_proj.shape, BF16),
        V(ssm_state.shape, F32), V(output_proj.shape, BF16), V((n.Q, EXPERTS), F32), V(gate_proj.shape, BF16),
        V(up_proj.shape, BF16), V(down_proj.shape, BF16),
        V((n.J, n.T, n.H * n.R), BF16),
        V((n.J, n.SLOTS, n.SLOTS * n.J), BF16),
        V((n.NM, n.NB, n.R, LANES), BF16),
        V((n.X, n.T, n.C), BF16), V((n.X, n.T, n.C), BF16),
        V((n.X, 8, n.T), F32),
        V((n.T, n.C), BF16),
        V((n.NM, n.TB, n.PW), F32), V((n.NM, n.TB, n.PW), F32),
        V((n.NB, n.TB, n.PW), BF16), V((n.X, n.NM, n.TB, n.PW), BF16),
        V((n.X, n.T, n.C), BF16),
        V((n.NM, n.NB * n.OWN, n.Q), BF16), V((n.NM, n.NB * n.OWN, n.Q), BF16),
        V((n.NB, n.R, LANES), BF16), V((n.NB, n.R, LANES), BF16),
        V((n.X, n.R, LANES), F32),
        V((n.NB, wide, LANES), BF16), V((n.X, n.NM, n.NB, wide, LANES), BF16),
        V((n.SLOTS, n.D), F32), V((n.SLOTS, n.D), BF16),
        V((n.X, n.SLOTS, n.Q), BF16), V((n.X, n.SLOTS, n.Q), BF16),
        V((n.NM, n.NB * CAP, n.Q), BF16), V((n.NM, n.NB * CAP, n.Q), BF16),
        V((n.NB, wide, LANES), BF16), V((n.NB, wide, LANES), BF16),
        V((n.NM, 8, LANES), F32), V((n.NB, 8, LANES), F32),
    ]
    most = max(n.NM, n.NB, n.X) - 1
    scratch += [
        pltpu.SemaphoreType.DMA((len(STAGES), most)), pltpu.SemaphoreType.DMA((len(STAGES), most)),
        pltpu.SemaphoreType.DMA((len(LOADS),)),
    ]
    out, conv_in, new_state, aux = pl.pallas_call(
        functools.partial(step_kernel, n),
        out_shape=(
            jax.ShapeDtypeStruct((n.R, LANES), BF16),
            jax.ShapeDtypeStruct((n.T, n.C), F32),
            jax.ShapeDtypeStruct(ssm_state.shape, F32),
            jax.ShapeDtypeStruct((8, LANES), F32),
        ),
        in_specs=[spec for _, spec in operands],
        out_specs=(vm, vm, vm, vm),
        scratch_shapes=scratch,
        compiler_params=pltpu.CompilerParams(
            collective_id=0, has_side_effects=True, vmem_limit_bytes=48 * 1024 * 1024
        ),
        name="mixer_moe_step",
    )(*[a for a, _ in operands])
    layer_out = out.reshape(n.J, n.OWN, LANES).transpose(1, 0, 2).reshape(n.OWN, n.Q)
    new_conv = jnp.concatenate([conv_state[1:], conv_in[None]], axis=0)
    return layer_out, new_conv, new_state, aux[0, :EXPERTS], aux[1, :1]


def solution(mesh):
    in_specs = (
        P(("groups", "head"), "state"),
        P("state"),
        P(None, "state", "head"),
        P(None, "head"),
        P("head"),
        P(None, "groups", "head"),
        P("head", None),
        P(),
        P(None, "head"),
        P("head"),
        P("state", "head"),
        P("head"),
        P("state", "groups", "head"),
        P("head", "state"),
        P(),
        P(),
        P(("groups", "head"), None),
        P(("groups", "head"), None),
        P("head", None, "state"),
        P("head", None, "state"),
        P("head", "state", None),
    )
    out_specs = (
        P(("groups", "head"), "state"),
        P(None, "groups", "head"),
        P("state", "groups", "head"),
        P("groups"),
        P("groups"),
    )
    return jax.shard_map(
        functools.partial(per_device, mesh.shape["head"], mesh.shape["state"]),
        mesh=mesh, in_specs=in_specs, out_specs=out_specs, check_vma=False,
    )
```

```python
import functools

import jax
import jax.numpy as jnp
from jax import lax
from jax.experimental import pallas as pl
from jax.experimental.pallas import tpu as pltpu
from jax.sharding import PartitionSpec as P

EXPERTS = 8
TOPK = 2
CAP = 2
LANES = 128
NORM_EPS = 1e-05
STEP_EPS = 1e-06
MESH = pl.DeviceIdType.MESH
F32 = jnp.float32
BF16 = jnp.bfloat16
HI = lax.Precision.HIGHEST


def div(a, n):
    assert n & (n - 1) == 0
    return lax.shift_right_logical(a, jnp.int32(n.bit_length() - 1)) if n > 1 else a


def mod(a, n):
    assert n & (n - 1) == 0
    return a & (n - 1)


def grid_of(rows, cols):
    return (
        lax.broadcasted_iota(jnp.int32, (rows, cols), 0),
        lax.broadcasted_iota(jnp.int32, (rows, cols), 1),
    )


def ones_where(cond, dtype=BF16):
    return jnp.where(cond, 1.0, 0.0).astype(dtype)


def mm(a, b, precision=None):
    return jnp.dot(a, b, preferred_element_type=F32, precision=precision)


def mm_nt(a, b, precision=None):
    return lax.dot_general(
        a, b, (((1,), (1,)), ((), ())), preferred_element_type=F32, precision=precision
    )


def silu(v):
    return v * jax.nn.sigmoid(v)


def softplus(v):
    return jnp.maximum(v, 0.0) + jnp.log1p(jnp.exp(-jnp.abs(v)))


def by_distance(n):
    return sorted(range(1, n), key=lambda k: -min(k, n - k))


STAGES = (
    "tok_far", "tok_near", "branch", "gate", "square", "proj_near", "proj_far", "low_near", "low_state",
    "read", "mix_near", "mix_far", "stat", "row_far", "row_near", "out_state", "out_near",
    "out_far", "aux_near", "aux_far",
)
OPERANDS = (
    "mixn", "win", "cw", "cb", "sp", "sg", "tp", "sb", "dl", "sk", "ssm", "op", "mn", "eid", "sid", "gp",
    "up", "dn",
)


def step_kernel(n, tok_hbm, cs_hbm, rw_hbm, *refs):
    count = len(OPERANDS)
    sources = refs[:count]
    lo_ref, nc_ref, ns_ref, load_ref, loss_ref = refs[count : count + 5]
    held = dict(zip(OPERANDS, refs[count + 5 : 2 * count + 5]))
    (
        cs, rw, pick, pick_row, G, XC, XG, XS, cob, P2, R2, F2, S2, XR, N3, R3, F3, Q3, ST, F4, G4, rows,
        rn, X5, Y5, N5, R5, F5, Q5, AN, AF, send_sem, recv_sem, row_send, row_recv, load_sem,
    ) = refs[2 * count + 5 :]
    head = lax.axis_index("head")
    x = lax.axis_index("state")
    b = head // n.NM
    m = head % n.NM
    X, NB, NM, OWN, J, R, T, C, S = n.X, n.NB, n.NM, n.OWN, n.J, n.R, n.T, n.C, n.S

    def offset(k):
        return k if 2 * k <= NM else k - NM

    far = {k: {"head": ((b + k) % NB) * NM + m} for k in range(1, NB)}
    near = {k: {"head": (head + n.H + offset(k)) % n.H} for k in range(1, NM)}
    block = {k: {"head": b * NM + (m + k) % NM} for k in range(1, NM)}
    side = {k: {"state": (x + k) % X} for k in range(1, X)}

    barrier = pltpu.get_barrier_semaphore()
    behind = {k: {"head": (head + n.H - offset(k)) % n.H} for k in near}
    for group in (side, behind, block, far):
        for k in group:
            pl.semaphore_signal(barrier, inc=1, device_id=group[k], device_id_type=MESH)

    loads = {}

    def load(name, src, dst):
        loads[name] = pltpu.make_async_copy(src, dst, load_sem.at[len(loads)])
        loads[name].start()

    load("tok", tok_hbm, G.at[m, b])
    for name, src in zip(OPERANDS, sources):
        load(name, src, held[name])
    load("conv", cs_hbm.at[0], cs)
    load("keep", cs_hbm.at[1 : n.CONV - 1], nc_ref.at[0 : n.CONV - 2])
    load("router", rw_hbm.at[:, pl.ds(pl.multiple_of(x * n.Q, n.Q), n.Q)], rw)
    mixn_ref, win, cw_ref, cb_ref = held["mixn"], held["win"], held["cw"], held["cb"]
    sp, sg_ref, tp, sb_ref, dl_ref = held["sp"], held["sg"], held["tp"], held["sb"], held["dl"]
    sk_ref, ssm, op, mn_ref = held["sk"], held["ssm"], held["op"], held["mn"]

    def loaded(*names):
        for name in names:
            loads[name].wait()

    pending = []

    def exchange(stage, group, pair):
        at = STAGES.index(stage)
        copies = []
        for k in by_distance(len(group) + 1):
            src, dst = pair(k)
            copy = pltpu.make_async_remote_copy(
                src_ref=src, dst_ref=dst, send_sem=send_sem.at[at, k - 1], recv_sem=recv_sem.at[at, k - 1],
                device_id=group[k], device_id_type=MESH,
            )
            copy.start()
            copies.append(copy)
        pending.extend(copies)
        return copies

    def arrive(copies):
        for copy in copies:
            copy.wait_recv()

    loaded("tok")
    pl.semaphore_wait(barrier, (NB - 1) + 2 * (NM - 1) + (X - 1))
    sent = exchange("tok_far", far, lambda k: (G.at[m, b], G.at[m, b]))
    tok_bf = G[m, b]

    r_i, c_i = grid_of(T, n.H * R)
    tok_of = (div(mod(c_i, NB * R), R) * NM + div(c_i, NB * R)) * OWN + mod(c_i, OWN)
    match = tok_of == r_i
    which = mod(div(c_i, OWN), J)
    for j in range(J):
        pick[j] = ones_where(match & (which == j))
    r_i, c_i = grid_of(n.SLOTS, n.SLOTS * J)
    match = div(c_i, J * CAP) * CAP + mod(c_i, CAP) == r_i
    which = mod(div(c_i, CAP), J)
    for j in range(J):
        pick_row[j] = ones_where(match & (which == j))

    arrive(sent)
    sent = exchange("tok_near", near, lambda k: (G.at[m], G.at[m]))
    loaded("win", "mixn")
    arrive(sent)

    gathered = G[...].reshape(n.H * R, LANES)
    conv_part = jnp.zeros((T, C), F32)
    gate_part = jnp.zeros((T, C), F32)
    squares = jnp.zeros((T, 1), F32)
    for j in range(J):
        tok_j = mm(pick[j], gathered)
        squares += jnp.sum(tok_j * tok_j, axis=1, keepdims=True)
        wide = (tok_j * mixn_ref[j : j + 1, :]).astype(BF16)
        conv_part += mm(wide, win[0, j * LANES : (j + 1) * LANES, :])
        gate_part += mm(wide, win[1, j * LANES : (j + 1) * LANES, :])
    XS[x] = jnp.broadcast_to(squares, (T, LANES)).T[:8, :]
    XC[x] = conv_part.astype(BF16)
    sent_sq = exchange("square", side, lambda k: (XS.at[x], XS.at[x]))
    sent = exchange("branch", side, lambda k: (XC.at[x], XC.at[x]))
    XG[x] = gate_part.astype(BF16)
    sent_gate = exchange("gate", side, lambda k: (XG.at[x], XG.at[x]))

    loaded("conv", "keep", "cw", "cb", "sp")
    window = cb_ref[...] + cw_ref[0:1, :] * cs[...]
    for k in range(n.CONV - 2):
        window += cw_ref[k + 1 : k + 2, :] * nc_ref[k]
    P2[...] = jnp.zeros_like(P2)
    arrive(sent_sq)
    total = XS[0]
    for k in range(1, X):
        total += XS[k]
    inv_first = lax.rsqrt(jnp.broadcast_to(total[:1, :], (LANES, T)).T[:, :1] / n.D + NORM_EPS)
    arrive(sent)
    conv_in = XC[0].astype(F32)
    for k in range(1, X):
        conv_in += XC[k].astype(F32)
    conv_in = conv_in * inv_first
    nc_ref[n.CONV - 2] = conv_in
    conv_out = silu(window + cw_ref[n.CONV - 1 : n.CONV, :] * conv_in)
    cob[...] = conv_out.astype(BF16)

    quarter = T // X
    part = mm_nt(cob[pl.ds(pl.multiple_of(x * quarter, quarter), quarter), :], sp[...])
    P2[:, :, : n.PROJ] = part.reshape(NM, n.TB, n.PROJ)
    R2[m] = P2[m]
    sent = exchange("proj_near", near, lambda k: (P2.at[(m + k) % NM], R2.at[m]))
    arrive(sent)
    total = R2[0]
    for k in range(1, NM):
        total += R2[k]
    F2[b] = total.astype(BF16)
    sent = exchange("proj_far", far, lambda k: (F2.at[b], F2.at[b]))
    loaded("tp", "ssm", "sg", "sb", "dl")
    arrive(sent)
    total = F2[0].astype(F32)
    for k in range(1, NB):
        total += F2[k].astype(F32)
    S2[x, m] = total.astype(BF16)
    sent = exchange("low_near", near, lambda k: (S2.at[x, m], S2.at[x, m]))
    arrive(sent)
    sent = exchange("low_state", side, lambda k: (S2.at[x], S2.at[x]))
    arrive(sent_gate)
    gate = XG[0].astype(F32)
    for k in range(1, X):
        gate += XG[k].astype(F32)
    gate = silu(gate * inv_first)
    rates = [jnp.exp(dl_ref[k : k + 1, :]) for k in range(S)]
    arrive(sent)

    projected = S2[...].astype(F32).reshape(T, n.PW)
    low = projected[:, : n.RANK]
    step_inv = lax.rsqrt(jnp.mean(low * low, axis=1, keepdims=True) + STEP_EPS)
    step_normed = (low * step_inv * sg_ref[...]).astype(BF16)
    step_size = softplus(mm(step_normed, tp[...]) + sb_ref[...])
    vectors = projected[:, n.RANK :].astype(BF16)
    rows_i, _ = grid_of(LANES, C)
    driven = step_size * conv_out
    read = jnp.zeros((T, C), F32)
    for k in range(S):
        b_in = mm(vectors, ones_where(rows_i == x * S + k))
        c_out = mm(vectors, ones_where(rows_i == n.STATE + x * S + k))
        fresh = jnp.exp(-step_size * rates[k]) * ssm[k] + driven * b_in
        ns_ref[k] = fresh
        read += c_out * fresh
    XR[x] = read.astype(BF16)
    sent = exchange("read", side, lambda k: (XR.at[x], XR.at[x]))
    loaded("op", "sk")
    r_i, c_i = grid_of(T, T)
    source = (div(mod(r_i, NB * OWN), OWN) * NM + div(r_i, NB * OWN)) * OWN + mod(r_i, OWN)
    by_member = ones_where(source == c_i)
    arrive(sent)
    read = XR[0].astype(F32)
    for k in range(1, X):
        read += XR[k].astype(F32)
    act = ((read + sk_ref[...] * conv_out) * gate).astype(BF16)
    act = mm(by_member, act).astype(BF16)
    N3[...] = mm(act, op[...]).astype(BF16).reshape(NM, NB * OWN, n.Q)
    R3[m] = N3[m]
    sent = exchange("mix_near", near, lambda k: (N3.at[(m + k) % NM], R3.at[m]))
    arrive(sent)
    total = R3[0].astype(F32)
    for k in range(1, NM):
        total += R3[k].astype(F32)
    total = total.astype(BF16)
    r_i, c_i = grid_of(NB * R, NB * OWN)
    match = div(r_i, R) * OWN + mod(r_i, OWN) == c_i
    which = mod(div(r_i, OWN), J)
    spread = jnp.zeros((NB * R, LANES), F32)
    for j in range(J):
        spread += mm(ones_where(match & (which == j)), total[:, j * LANES : (j + 1) * LANES])
    F3[...] = spread.astype(BF16).reshape(NB, R, LANES)
    Q3[b] = F3[b]
    sent = exchange("mix_far", far, lambda k: (F3.at[(b + k) % NB], Q3.at[b]))
    loaded("router", "mn", "eid", "sid")
    arrive(sent)
    total = Q3[0].astype(F32)
    for k in range(1, NB):
        total += Q3[k].astype(F32)

    resid_bf = (tok_bf.astype(F32) + total).astype(BF16)
    resid = resid_bf.astype(F32)
    row_i, lane_i = grid_of(R, LANES)
    hits, kept, slots = [], [], []
    i_i, t_i = grid_of(R, OWN)

    def by_row(ref, k):
        wide = jnp.broadcast_to(ref[k : k + 1, :], (R, OWN)).astype(F32)
        return jnp.sum(jnp.where(mod(i_i, OWN) == t_i, wide, 0.0), axis=1, keepdims=True).astype(jnp.int32)

    for k in range(TOPK):
        e_k, s_k = by_row(held["eid"], k), by_row(held["sid"], k)
        keep = s_k < CAP
        hits.append(lane_i == e_k)
        kept.append(keep)
        slots.append((lane_i == e_k * CAP + s_k) & keep)
    dispatch = sum(ones_where(s, F32) for s in slots).astype(BF16)
    d_i, q_i = grid_of(NB * J * CAP, LANES)
    slot_of = ones_where(q_i == div(d_i, J * CAP) * CAP + mod(d_i, CAP))
    d_i, c_i = grid_of(NB * J * CAP, R)
    chosen_rows = jnp.where(
        mod(div(d_i, CAP), J) == div(c_i, OWN), mm_nt(slot_of, dispatch), 0.0
    ).astype(BF16)
    F4[...] = mm(chosen_rows, resid_bf).reshape(NB, J * CAP, LANES).astype(BF16)
    G4[x, m, b] = F4[b]
    sent = exchange("row_far", far, lambda k: (F4.at[(b + k) % NB], G4.at[x, m, b]))

    gain = jnp.zeros((R, LANES), F32)
    for j in range(J):
        gain = jnp.where(div(row_i, OWN) == j, mn_ref[pl.ds(x * J + j, 1), :], gain)
    scaled = resid * gain
    raw = jnp.zeros((R, EXPERTS), F32)
    for j in range(J):
        raw += mm_nt(
            jnp.where(div(row_i, OWN) == j, scaled, 0.0), rw[:, j * LANES : (j + 1) * LANES], HI
        )
    ST[x] = jnp.broadcast_to(jnp.sum(resid * resid, axis=1, keepdims=True), (R, LANES))
    ST[x, :, :EXPERTS] = raw
    sent_stat = exchange("stat", side, lambda k: (ST.at[x], ST.at[x]))
    arrive(sent_stat)
    total = ST[0]
    for k in range(1, X):
        total += ST[k]
    r_i, c_i = grid_of(R, R)
    total = mm(ones_where(mod(r_i, OWN) == mod(c_i, OWN), F32), total, HI)
    inv_second = lax.rsqrt(total[:, EXPERTS : EXPERTS + 1] / n.D + NORM_EPS)
    logits = inv_second * total
    chosen = [jnp.sum(jnp.where(hit, logits, 0.0), axis=1, keepdims=True) for hit in hits]
    mixing = jnp.zeros((R, LANES), F32)
    for k in range(TOPK):
        weight = jax.nn.sigmoid(chosen[k] - chosen[1 - k])
        mixing += jnp.where(slots[k], weight, 0.0)
    first = row_i < OWN
    load = sum(ones_where(hits[k] & kept[k] & first, F32) for k in range(TOPK))
    load = jnp.sum(load, axis=0, keepdims=True)
    prob = jnp.where(first & (lane_i < EXPERTS), jax.nn.sigmoid(logits), 0.0)
    prob = jnp.sum(prob, axis=0, keepdims=True)
    a_i, l_i = grid_of(8, LANES)
    AN[m] = jnp.where(a_i == 0, load, jnp.where(a_i == 1, prob, 0.0))
    sent_aux = exchange("aux_near", block, lambda k: (AN.at[m], AN.at[m]))
    d_i, q_i = grid_of(R, NB * J * CAP)
    combine = jnp.where(
        mod(div(q_i, CAP), J) == div(d_i, OWN), mm_nt(mixing, slot_of.astype(F32), HI), 0.0
    )
    loaded("gp", "up", "dn")

    arrive(sent)

    def to_side(piece, at):
        copies = []
        for k in by_distance(X):
            copy = pltpu.make_async_remote_copy(
                src_ref=G4.at[x, piece], dst_ref=G4.at[x, piece], send_sem=row_send.at[at, k - 1],
                recv_sem=row_recv.at[at, k - 1], device_id=side[k], device_id_type=MESH,
            )
            copy.start()
            copies.append(copy)
        pending.extend(copies)
        return copies

    sent = exchange("row_near", block, lambda k: (G4.at[x, m], G4.at[x, m]))
    sideways = to_side(m, 0)
    for copy, k in reversed(list(zip(sent, by_distance(NM)))):
        arrive([copy])
        sideways += to_side((m + NM - k) % NM, k)
    arrive(sent_aux)
    total = AN[0]
    for k in range(1, NM):
        total += AN[k]
    AF[b] = total
    sent_aux = exchange("aux_far", far, lambda k: (AF.at[b], AF.at[b]))
    arrive(sideways)

    squares = jnp.zeros((n.SLOTS, 1), F32)
    for k in range(X):
        source = G4[k].astype(F32).reshape(n.SLOTS * J, LANES).astype(BF16)
        for j in range(J):
            at = k * J + j
            part = mm(pick_row[j], source)
            squares += jnp.sum(part * part, axis=1, keepdims=True)
            rows[:, at * LANES : (at + 1) * LANES] = part * mn_ref[at : at + 1, :]
    inv_rows = lax.rsqrt(squares / n.D + NORM_EPS)
    rn[...] = (rows[...] * inv_rows).astype(BF16)
    normed = rn[...]
    hidden = (silu(mm_nt(normed, held["gp"][0])) * mm_nt(normed, held["up"][0])).astype(BF16)
    for k in range(X):
        X5[k] = mm(hidden, held["dn"][0, :, k * n.Q : (k + 1) * n.Q]).astype(BF16)
    sent = exchange("out_state", side, lambda k: (X5.at[(x + k) % X], Y5.at[x]))
    Y5[x] = X5[x]
    arrive(sent)
    total = Y5[0].astype(F32)
    for k in range(1, X):
        total += Y5[k].astype(F32)
    N5[...] = total.reshape(NM, NB * CAP, n.Q).astype(BF16)
    R5[m] = N5[m]
    sent = exchange("out_near", block, lambda k: (N5.at[(m + k) % NM], R5.at[m]))
    arrive(sent)
    total = R5[0].astype(F32)
    for k in range(1, NM):
        total += R5[k].astype(F32)
    total = total.astype(BF16)
    r_i, c_i = grid_of(NB * J * CAP, NB * CAP)
    match = div(r_i, J * CAP) * CAP + mod(r_i, CAP) == c_i
    which = mod(div(r_i, CAP), J)
    spread = jnp.zeros((NB * J * CAP, LANES), F32)
    for j in range(J):
        spread += mm(ones_where(match & (which == j)), total[:, j * LANES : (j + 1) * LANES])
    F5[...] = spread.reshape(NB, J * CAP, LANES).astype(BF16)
    Q5[b] = F5[b]
    sent = exchange("out_far", far, lambda k: (F5.at[(b + k) % NB], Q5.at[b]))
    arrive(sent_aux)
    total = AF[0]
    for k in range(1, NB):
        total += AF[k]
    share = total[0:1, :] / (T * TOPK) * (total[1:2, :] / T)
    loss = EXPERTS * jnp.sum(jnp.where(l_i[:1] < EXPERTS, share, 0.0), axis=1, keepdims=True)
    load_ref[...] = total[0:1, :EXPERTS]
    loss_ref[...] = loss
    arrive(sent)
    back = Q5[...].astype(F32).reshape(NB * J * CAP, LANES)
    lo_ref[...] = (resid + mm(combine, back, HI)).astype(BF16)
    for copy in pending:
        copy.wait_send()


def finish_kernel(*refs):
    count = len(refs) // 2
    copies = [
        pltpu.make_async_copy(refs[k], refs[count + k], refs[-1].at[k]) for k in range(count)
    ]
    for copy in copies:
        copy.start()
    for copy in copies:
        copy.wait()


class Sizes:
    pass


def per_device(
    head_count, state_count,
    tokens, mixer_norm, input_proj, conv_weight, conv_bias, conv_state, state_proj, step_gain, step_proj,
    step_bias, decay_log, skip_gain, ssm_state, output_proj, moe_norm, router_weight, expert_ids, slot_ids,
    gate_proj, up_proj, down_proj,
):
    n = Sizes()
    n.H, n.X, n.NB = head_count, state_count, EXPERTS
    n.NM = n.H // n.NB
    n.OWN, n.Q = tokens.shape
    n.J = n.Q // LANES
    n.R = n.OWN * n.J
    n.D = n.Q * n.X
    n.CONV = conv_weight.shape[0]
    _, n.T, n.C = conv_state.shape
    n.S = decay_log.shape[0]
    n.STATE = n.S * n.X
    n.RANK, n.PROJ = step_proj.shape[0], state_proj.shape[1]
    n.PW = -(-n.PROJ // LANES) * LANES
    n.TB = n.T // n.X // n.NM
    n.SLOTS = n.NM * n.NB * CAP
    n.FF = gate_proj.shape[2]

    tok = tokens.reshape(n.OWN, n.J, LANES).transpose(1, 0, 2).reshape(n.R, LANES)
    V = pltpu.VMEM
    operands = (
        mixer_norm.reshape(n.J, LANES), input_proj, conv_weight, conv_bias.reshape(1, -1), state_proj.T,
        step_gain.reshape(1, -1), step_proj, step_bias.reshape(1, -1), decay_log, skip_gain.reshape(1, -1),
        ssm_state, output_proj, moe_norm.reshape(-1, LANES), expert_ids.T, slot_ids.T,
        gate_proj.transpose(0, 2, 1), up_proj.transpose(0, 2, 1), down_proj,
    )
    vm = pl.BlockSpec(memory_space=pltpu.VMEM)
    hbm = pl.BlockSpec(memory_space=pltpu.HBM)
    wide = n.J * CAP
    scratch = [V(a.shape, a.dtype) for a in operands]
    scratch += [
        V(conv_state.shape[1:], F32), V((EXPERTS, n.Q), F32),
        V((n.J, n.T, n.H * n.R), BF16),
        V((n.J, n.SLOTS, n.SLOTS * n.J), BF16),
        V((n.NM, n.NB, n.R, LANES), BF16),
        V((n.X, n.T, n.C), BF16), V((n.X, n.T, n.C), BF16),
        V((n.X, 8, n.T), F32),
        V((n.T, n.C), BF16),
        V((n.NM, n.TB, n.PW), F32), V((n.NM, n.TB, n.PW), F32),
        V((n.NB, n.TB, n.PW), BF16), V((n.X, n.NM, n.TB, n.PW), BF16),
        V((n.X, n.T, n.C), BF16),
        V((n.NM, n.NB * n.OWN, n.Q), BF16), V((n.NM, n.NB * n.OWN, n.Q), BF16),
        V((n.NB, n.R, LANES), BF16), V((n.NB, n.R, LANES), BF16),
        V((n.X, n.R, LANES), F32),
        V((n.NB, wide, LANES), BF16), V((n.X, n.NM, n.NB, wide, LANES), BF16),
        V((n.SLOTS, n.D), F32), V((n.SLOTS, n.D), BF16),
        V((n.X, n.SLOTS, n.Q), BF16), V((n.X, n.SLOTS, n.Q), BF16),
        V((n.NM, n.NB * CAP, n.Q), BF16), V((n.NM, n.NB * CAP, n.Q), BF16),
        V((n.NB, wide, LANES), BF16), V((n.NB, wide, LANES), BF16),
        V((n.NM, 8, LANES), F32), V((n.NB, 8, LANES), F32),
    ]
    most = max(n.NM, n.NB, n.X) - 1
    dma = pltpu.SemaphoreType.DMA
    scratch += [
        dma((len(STAGES), most)), dma((len(STAGES), most)), dma((n.NM, n.X - 1)), dma((n.NM, n.X - 1)),
        dma((len(OPERANDS) + 4,)),
    ]
    shapes = (
        jax.ShapeDtypeStruct((n.R, LANES), BF16),
        jax.ShapeDtypeStruct(conv_state.shape, F32),
        jax.ShapeDtypeStruct(ssm_state.shape, F32),
        jax.ShapeDtypeStruct((1, EXPERTS), F32),
        jax.ShapeDtypeStruct((1, 1), F32),
    )
    results = pl.pallas_call(
        functools.partial(step_kernel, n),
        out_shape=shapes,
        in_specs=[hbm] * (len(operands) + 3),
        out_specs=(vm,) * len(shapes),
        scratch_shapes=scratch,
        compiler_params=pltpu.CompilerParams(
            collective_id=0, has_side_effects=True, vmem_limit_bytes=48 * 1024 * 1024
        ),
        name="mixer_moe_step",
    )(*[pltpu.with_memory_space_constraint(a, pltpu.HBM) for a in (tok, conv_state, router_weight.T, *operands)])
    out, new_conv, new_state, load, loss = pl.pallas_call(
        finish_kernel,
        out_shape=shapes,
        in_specs=[vm] * len(shapes),
        out_specs=(hbm,) * len(shapes),
        scratch_shapes=[dma((len(shapes),))],
        compiler_params=pltpu.CompilerParams(vmem_limit_bytes=1024 * 1024),
        name="finish",
    )(*results)
    layer_out = out.reshape(n.J, n.OWN, LANES).transpose(1, 0, 2).reshape(n.OWN, n.Q)
    return layer_out, new_conv, new_state, load.reshape(-1), loss.reshape(1)


def solution(mesh):
    in_specs = (
        P(("groups", "head"), "state"),
        P("state"),
        P(None, "state", "head"),
        P(None, "head"),
        P("head"),
        P(None, "groups", "head"),
        P("head", None),
        P(),
        P(None, "head"),
        P("head"),
        P("state", "head"),
        P("head"),
        P("state", "groups", "head"),
        P("head", "state"),
        P(),
        P(),
        P(("groups", "head"), None),
        P(("groups", "head"), None),
        P("head", None, "state"),
        P("head", None, "state"),
        P("head", "state", None),
    )
    out_specs = (
        P(("groups", "head"), "state"),
        P(None, "groups", "head"),
        P("state", "groups", "head"),
        P("groups"),
        P("groups"),
    )
    return jax.shard_map(
        functools.partial(per_device, mesh.shape["head"], mesh.shape["state"]),
        mesh=mesh, in_specs=in_specs, out_specs=out_specs, check_vma=False,
    )
```

```python
import functools

import jax
import jax.numpy as jnp
from jax import lax
from jax.experimental import pallas as pl
from jax.experimental.pallas import tpu as pltpu
from jax.sharding import PartitionSpec as P

EXPERTS = 8
TOPK = 2
CAP = 2
LANES = 128
NORM_EPS = 1e-05
STEP_EPS = 1e-06
MESH = pl.DeviceIdType.MESH
F32 = jnp.float32
BF16 = jnp.bfloat16
HI = lax.Precision.HIGHEST


def div(a, n):
    assert n & (n - 1) == 0
    return lax.shift_right_logical(a, jnp.int32(n.bit_length() - 1)) if n > 1 else a


def mod(a, n):
    assert n & (n - 1) == 0
    return a & (n - 1)


def grid_of(rows, cols):
    return (
        lax.broadcasted_iota(jnp.int32, (rows, cols), 0),
        lax.broadcasted_iota(jnp.int32, (rows, cols), 1),
    )


def ones_where(cond, dtype=BF16):
    return jnp.where(cond, 1.0, 0.0).astype(dtype)


def mm(a, b, precision=None):
    return jnp.dot(a, b, preferred_element_type=F32, precision=precision)


def mm_nt(a, b, precision=None):
    return lax.dot_general(
        a, b, (((1,), (1,)), ((), ())), preferred_element_type=F32, precision=precision
    )


def silu(v):
    return v * jax.nn.sigmoid(v)


def softplus(v):
    return jnp.maximum(v, 0.0) + jnp.log1p(jnp.exp(-jnp.abs(v)))


def by_distance(n):
    return sorted(range(1, n), key=lambda k: -min(k, n - k))


STAGES = (
    "tok_near", "tok_last", "branch", "gate", "square", "proj_near", "proj_far", "low_near", "low_state",
    "read", "mix_near", "mix_far", "stat", "row_far", "row_near", "row_state", "out_state", "out_near",
    "out_far", "aux_near", "aux_far",
)
OPERANDS = (
    "mixn", "win", "cw", "cb", "sp", "sg", "tp", "sb", "dl", "sk", "ssm", "op", "mn", "eid", "sid", "gp",
    "up", "dn",
)


def step_kernel(n, tok_hbm, cs_hbm, rw_hbm, *refs):
    count = len(OPERANDS)
    sources = refs[:count]
    lo_ref, nc_ref, ns_ref, load_ref, loss_ref = refs[count : count + 5]
    held = dict(zip(OPERANDS, refs[count + 5 : 2 * count + 5]))
    (
        cs, rw, pick, pick_row, G, XC, XG, XS, cob, P2, R2, F2, S2, XR, N3, R3, F3, Q3, ST, F4, G4, rows,
        rn, X5, Y5, N5, R5, F5, Q5, AN, AF, send_sem, recv_sem, piece_sem, up_send, up_recv, down_send,
        down_recv, ready_up, ready_near, load_sem,
    ) = refs[2 * count + 5 :]
    head = lax.axis_index("head")
    x = lax.axis_index("state")
    b = head // n.NM
    m = head % n.NM
    X, NB, NM, OWN, J, R, T, C, S = n.X, n.NB, n.NM, n.OWN, n.J, n.R, n.T, n.C, n.S

    def offset(k):
        return k if 2 * k <= NM else k - NM

    far = {k: {"head": ((b + k) % NB) * NM + m} for k in range(1, NB)}
    near = {k: {"head": (head + n.H + offset(k)) % n.H} for k in range(1, NM)}
    block = {k: {"head": b * NM + (m + k) % NM} for k in range(1, NM)}
    side = {k: {"state": (x + k) % X} for k in range(1, X)}

    barrier = pltpu.get_barrier_semaphore()
    around = [(head + n.H + o) % n.H for o in range(-(NM // 2), NM // 2 + 1) if o]

    def greet(partner):
        pl.semaphore_signal(barrier, inc=1, device_id=partner, device_id_type=MESH)

    for k in side:
        greet(side[k])
    for other in around:
        pl.when(other > head)(functools.partial(greet, {"head": other}))
    for k in range(1, NB):
        pl.when(b + k < NB)(functools.partial(greet, {"head": (b + k) * NM + m}))
    expected = b + (X - 1)
    for other in around:
        expected += jnp.where(other < head, 1, 0)

    loads = {}

    def load(name, src, dst):
        loads[name] = pltpu.make_async_copy(src, dst, load_sem.at[len(loads)])
        loads[name].start()

    load("tok", tok_hbm, G.at[m, b])
    for name, src in zip(OPERANDS, sources):
        load(name, src, held[name])
    load("conv", cs_hbm.at[0], cs)
    load("keep", cs_hbm.at[1 : n.CONV - 1], nc_ref.at[0 : n.CONV - 2])
    load("router", rw_hbm.at[:, pl.ds(pl.multiple_of(x * n.Q, n.Q), n.Q)], rw)
    mixn_ref, win, cw_ref, cb_ref = held["mixn"], held["win"], held["cw"], held["cb"]
    sp, sg_ref, tp, sb_ref, dl_ref = held["sp"], held["sg"], held["tp"], held["sb"], held["dl"]
    sk_ref, ssm, op, mn_ref = held["sk"], held["ssm"], held["op"], held["mn"]

    def loaded(*names):
        for name in names:
            loads[name].wait()

    pending = []

    def remote(src, dst, send, recv, partner):
        return pltpu.make_async_remote_copy(
            src_ref=src, dst_ref=dst, send_sem=send, recv_sem=recv, device_id=partner, device_id_type=MESH
        )

    def exchange(stage, group, pair, landing, first=None):
        at = STAGES.index(stage)
        for k in by_distance(len(group) + 1):
            if first is not None:
                first(k)
            src, dst = pair(k)
            remote(src, dst, send_sem.at[at], recv_sem.at[at], group[k]).start()
        pending.append(pltpu.make_async_copy(landing, landing, send_sem.at[at]))
        return pltpu.make_async_copy(landing, landing, recv_sem.at[at])

    def arrive(copy):
        copy.wait()

    def by_pieces(name, group, ref, at):
        near_at, side_at = STAGES.index(name + "_near"), STAGES.index(name + "_state")
        sent = {}
        order = by_distance(NM)
        for k in order:
            sent[k] = remote(
                ref.at[x, m], ref.at[x, m], send_sem.at[near_at], piece_sem.at[at, k - 1], group[k]
            )
            sent[k].start()
        for step in [0] + order[::-1]:
            piece = (m + NM - step) % NM
            if step:
                sent[step].wait_recv()
            for k in by_distance(X):
                remote(
                    ref.at[x, piece], ref.at[x, piece], send_sem.at[side_at], recv_sem.at[side_at], side[k]
                ).start()
        landing = ref.at[0, 0 : NM - 1]
        pending.append(pltpu.make_async_copy(landing, landing, send_sem.at[near_at]))
        landing = ref.at[0 : X - 1]
        pending.append(pltpu.make_async_copy(landing, landing, send_sem.at[side_at]))
        return pltpu.make_async_copy(landing, landing, recv_sem.at[side_at])

    loaded("tok")
    pl.semaphore_wait(barrier, expected)

    @pl.when(b > 0)
    def _():
        pl.semaphore_signal(ready_up, inc=1, device_id={"head": head - NM}, device_id_type=MESH)

    for k in near:
        source = (head + n.H - offset(k)) % n.H

        @pl.when(source < head)
        def _(k=k, source=source):
            pl.semaphore_signal(
                ready_near.at[k - 1], inc=1, device_id={"head": source}, device_id_type=MESH
            )

    own = G.at[m, b]
    downs = []
    for k in by_distance(NB):
        copy = remote(own, own, down_send.at[k - 1], down_recv.at[k - 1], {"head": head - k * NM})
        pl.when(b >= k)(copy.start)
        downs.append((k, copy))
    climbing = b < NB - 1
    ups = [
        remote(G.at[m, k], G.at[m, k], up_send.at[k], up_recv.at[k], {"head": head + NM})
        for k in range(NB - 1)
    ]

    @pl.when(climbing)
    def _():
        pl.semaphore_wait(ready_up, 1)

    for k in range(NB - 2, -1, -1):
        pl.when(k < b)(ups[k].wait_recv)
        pl.when((k <= b) & climbing)(ups[k].start)

    def from_above(last):
        for k, copy in sorted(downs, key=lambda t: t[0]):
            pl.when((b + k == NB - 1) if last else (b + k < NB - 1))(copy.wait_recv)

    def near_ready(k):
        target = (head + n.H + offset(k)) % n.H

        @pl.when(target > head)
        def _():
            pl.semaphore_wait(ready_near.at[k - 1], 1)

    from_above(False)
    early = G.at[m, 0 : NB - 1]
    sent_early = exchange(
        "tok_near", near, lambda k: (early, early), G.at[0 : NM - 1, 0 : NB - 1], near_ready
    )
    tok_bf = G[m, b]

    r_i, c_i = grid_of(T, n.H * R)
    tok_of = (div(mod(c_i, NB * R), R) * NM + div(c_i, NB * R)) * OWN + mod(c_i, OWN)
    match = tok_of == r_i
    which = mod(div(c_i, OWN), J)
    for j in range(J):
        pick[j] = ones_where(match & (which == j))
    r_i, c_i = grid_of(n.SLOTS, n.SLOTS * J)
    match = div(c_i, J * CAP) * CAP + mod(c_i, CAP) == r_i
    which = mod(div(c_i, CAP), J)
    for j in range(J):
        pick_row[j] = ones_where(match & (which == j))

    from_above(True)
    final = G.at[m, NB - 1]
    sent = exchange("tok_last", near, lambda k: (final, final), G.at[0, 0 : NM - 1])
    loaded("win", "mixn")
    arrive(sent_early)
    arrive(sent)

    gathered = G[...].reshape(n.H * R, LANES)
    conv_part = jnp.zeros((T, C), F32)
    gate_part = jnp.zeros((T, C), F32)
    squares = jnp.zeros((T, 1), F32)
    for j in range(J):
        tok_j = mm(pick[j], gathered)
        squares += jnp.sum(tok_j * tok_j, axis=1, keepdims=True)
        wide = tok_j * mixn_ref[j : j + 1, :]
        high = wide.astype(BF16)
        for half in (high, (wide - high.astype(F32)).astype(BF16)):
            conv_part += mm(half, win[0, j * LANES : (j + 1) * LANES, :])
            gate_part += mm(half, win[1, j * LANES : (j + 1) * LANES, :])
    XS[x] = jnp.broadcast_to(squares, (T, LANES)).T[:8, :]
    XC[x] = conv_part.astype(BF16)
    sent_sq = exchange("square", side, lambda k: (XS.at[x], XS.at[x]), XS.at[0 : X - 1])
    sent = exchange("branch", side, lambda k: (XC.at[x], XC.at[x]), XC.at[0 : X - 1])
    XG[x] = gate_part.astype(BF16)
    sent_gate = exchange("gate", side, lambda k: (XG.at[x], XG.at[x]), XG.at[0 : X - 1])

    loaded("conv", "keep", "cw", "cb", "sp")
    window = cb_ref[...] + cw_ref[0:1, :] * cs[...]
    for k in range(n.CONV - 2):
        window += cw_ref[k + 1 : k + 2, :] * nc_ref[k]
    P2[...] = jnp.zeros_like(P2)
    arrive(sent_sq)
    total = XS[0]
    for k in range(1, X):
        total += XS[k]
    inv_first = lax.rsqrt(jnp.broadcast_to(total[:1, :], (LANES, T)).T[:, :1] / n.D + NORM_EPS)
    arrive(sent)
    conv_in = XC[0].astype(F32)
    for k in range(1, X):
        conv_in += XC[k].astype(F32)
    conv_in = conv_in * inv_first
    nc_ref[n.CONV - 2] = conv_in
    conv_out = silu(window + cw_ref[n.CONV - 1 : n.CONV, :] * conv_in)
    cob[...] = conv_out.astype(BF16)

    quarter = T // X
    spare = n.PROJ - n.RANK

    def in_halves(wide):
        low, vectors = wide[:, : n.RANK], wide[:, n.RANK :]
        high = vectors.astype(BF16).astype(F32)
        rest = pltpu.roll(vectors - high, spare, 1)
        return jnp.concatenate([low, high + rest], axis=1).astype(BF16)

    part = mm_nt(cob[pl.ds(pl.multiple_of(x * quarter, quarter), quarter), :], sp[...])
    P2[:, :, : n.PROJ] = part.reshape(NM, n.TB, n.PROJ)
    R2[m] = P2[m]
    sent = exchange("proj_near", near, lambda k: (P2.at[(m + k) % NM], R2.at[m]), R2.at[0 : NM - 1])
    arrive(sent)
    total = R2[0]
    for k in range(1, NM):
        total += R2[k]
    F2[b] = in_halves(total)
    sent = exchange("proj_far", far, lambda k: (F2.at[b], F2.at[b]), F2.at[0 : NB - 1])
    loaded("tp", "ssm", "sg", "sb", "dl")
    arrive(sent)
    total = F2[0].astype(F32)
    for k in range(1, NB):
        total += F2[k].astype(F32)
    low, vectors = total[:, : n.RANK], total[:, n.RANK :]
    step_inv = lax.rsqrt(jnp.mean(low * low, axis=1, keepdims=True) + STEP_EPS)
    vectors = vectors + pltpu.roll(vectors, LANES - spare, 1)
    _, l_i = grid_of(n.TB, LANES)
    vectors = jnp.where(l_i < spare, vectors, 0.0)
    S2[x, m] = in_halves(jnp.concatenate([low * step_inv * sg_ref[...], vectors], axis=1))
    sent = by_pieces("low", near, S2, 0)
    arrive(sent_gate)
    gate = gate_part
    for k in range(1, X):
        gate += XG[(x + k) % X].astype(F32)
    gate = silu(gate * inv_first)
    rates = [jnp.exp(dl_ref[k : k + 1, :]) for k in range(S)]
    arrive(sent)

    projected = S2[...].astype(F32).reshape(T, n.PW)
    step_normed = projected[:, : n.RANK].astype(BF16)
    step_size = softplus(mm(step_normed, tp[...]) + sb_ref[...])
    vectors = projected[:, n.RANK :].astype(BF16)
    rows_i, _ = grid_of(LANES, C)
    driven = step_size * conv_out
    read = jnp.zeros((T, C), F32)
    for k in range(S):
        at = x * S + k
        b_in = mm(vectors, ones_where((rows_i == at) | (rows_i == spare + at)))
        at = at + n.STATE
        c_out = mm(vectors, ones_where((rows_i == at) | (rows_i == spare + at)))
        fresh = jnp.exp(-step_size * rates[k]) * ssm[k] + driven * b_in
        ns_ref[k] = fresh
        read += c_out * fresh
    XR[x] = read.astype(BF16)
    sent = exchange("read", side, lambda k: (XR.at[x], XR.at[x]), XR.at[0 : X - 1])
    loaded("op", "sk")
    r_i, c_i = grid_of(T, T)
    source = (div(mod(r_i, NB * OWN), OWN) * NM + div(r_i, NB * OWN)) * OWN + mod(r_i, OWN)
    by_member = ones_where(source == c_i)
    arrive(sent)
    for k in range(1, X):
        read += XR[(x + k) % X].astype(F32)
    act = ((read + sk_ref[...] * conv_out) * gate).astype(BF16)
    act = mm(by_member, act).astype(BF16)
    N3[...] = mm(act, op[...]).astype(BF16).reshape(NM, NB * OWN, n.Q)
    R3[m] = N3[m]
    sent = exchange("mix_near", near, lambda k: (N3.at[(m + k) % NM], R3.at[m]), R3.at[0 : NM - 1])
    arrive(sent)
    total = R3[0].astype(F32)
    for k in range(1, NM):
        total += R3[k].astype(F32)
    total = total.astype(BF16)
    r_i, c_i = grid_of(NB * R, NB * OWN)
    match = div(r_i, R) * OWN + mod(r_i, OWN) == c_i
    which = mod(div(r_i, OWN), J)
    spread = jnp.zeros((NB * R, LANES), F32)
    for j in range(J):
        spread += mm(ones_where(match & (which == j)), total[:, j * LANES : (j + 1) * LANES])
    F3[...] = spread.astype(BF16).reshape(NB, R, LANES)
    Q3[b] = F3[b]
    sent = exchange("mix_far", far, lambda k: (F3.at[(b + k) % NB], Q3.at[b]), Q3.at[0 : NB - 1])
    loaded("router", "mn", "eid", "sid")
    arrive(sent)
    total = Q3[0].astype(F32)
    for k in range(1, NB):
        total += Q3[k].astype(F32)

    resid_bf = (tok_bf.astype(F32) + total).astype(BF16)
    resid = resid_bf.astype(F32)
    row_i, lane_i = grid_of(R, LANES)
    hits, kept, slots = [], [], []
    i_i, t_i = grid_of(R, OWN)

    def by_row(ref, k):
        wide = jnp.broadcast_to(ref[k : k + 1, :], (R, OWN)).astype(F32)
        return jnp.sum(jnp.where(mod(i_i, OWN) == t_i, wide, 0.0), axis=1, keepdims=True).astype(jnp.int32)

    for k in range(TOPK):
        e_k, s_k = by_row(held["eid"], k), by_row(held["sid"], k)
        keep = s_k < CAP
        hits.append(lane_i == e_k)
        kept.append(keep)
        slots.append((lane_i == e_k * CAP + s_k) & keep)
    dispatch = sum(ones_where(s, F32) for s in slots).astype(BF16)
    d_i, q_i = grid_of(NB * J * CAP, LANES)
    slot_of = ones_where(q_i == div(d_i, J * CAP) * CAP + mod(d_i, CAP))
    d_i, c_i = grid_of(NB * J * CAP, R)
    chosen_rows = jnp.where(
        mod(div(d_i, CAP), J) == div(c_i, OWN), mm_nt(slot_of, dispatch), 0.0
    ).astype(BF16)
    F4[...] = mm(chosen_rows, resid_bf).reshape(NB, J * CAP, LANES).astype(BF16)
    G4[x, m, b] = F4[b]
    sent = exchange(
        "row_far", far, lambda k: (F4.at[(b + k) % NB], G4.at[x, m, b]), G4.at[x, m, 0 : NB - 1]
    )

    gain = jnp.zeros((R, LANES), F32)
    for j in range(J):
        gain = jnp.where(div(row_i, OWN) == j, mn_ref[pl.ds(x * J + j, 1), :], gain)
    scaled = resid * gain
    raw = jnp.zeros((R, EXPERTS), F32)
    for j in range(J):
        raw += mm_nt(
            jnp.where(div(row_i, OWN) == j, scaled, 0.0), rw[:, j * LANES : (j + 1) * LANES], HI
        )
    ST[x] = jnp.broadcast_to(jnp.sum(resid * resid, axis=1, keepdims=True), (R, LANES))
    ST[x, :, :EXPERTS] = raw
    sent_stat = exchange("stat", side, lambda k: (ST.at[x], ST.at[x]), ST.at[0 : X - 1])
    arrive(sent_stat)
    total = ST[0]
    for k in range(1, X):
        total += ST[k]
    r_i, c_i = grid_of(R, R)
    total = mm(ones_where(mod(r_i, OWN) == mod(c_i, OWN), F32), total, HI)
    inv_second = lax.rsqrt(total[:, EXPERTS : EXPERTS + 1] / n.D + NORM_EPS)
    logits = inv_second * total
    chosen = [jnp.sum(jnp.where(hit, logits, 0.0), axis=1, keepdims=True) for hit in hits]
    mixing = jnp.zeros((R, LANES), F32)
    for k in range(TOPK):
        weight = jax.nn.sigmoid(chosen[k] - chosen[1 - k])
        mixing += jnp.where(slots[k], weight, 0.0)
    first = row_i < OWN
    load = sum(ones_where(hits[k] & kept[k] & first, F32) for k in range(TOPK))
    load = jnp.sum(load, axis=0, keepdims=True)
    prob = jnp.where(first & (lane_i < EXPERTS), jax.nn.sigmoid(logits), 0.0)
    prob = jnp.sum(prob, axis=0, keepdims=True)
    a_i, l_i = grid_of(8, LANES)
    AN[m] = jnp.where(a_i == 0, load, jnp.where(a_i == 1, prob, 0.0))
    sent_aux = exchange("aux_near", block, lambda k: (AN.at[m], AN.at[m]), AN.at[0 : NM - 1])
    d_i, q_i = grid_of(R, NB * J * CAP)
    combine = jnp.where(
        mod(div(q_i, CAP), J) == div(d_i, OWN), mm_nt(mixing, slot_of.astype(F32), HI), 0.0
    )
    loaded("gp", "up", "dn")

    arrive(sent)

    sideways = by_pieces("row", block, G4, 1)
    arrive(sent_aux)
    total = AN[0]
    for k in range(1, NM):
        total += AN[k]
    AF[b] = total
    sent_aux = exchange("aux_far", far, lambda k: (AF.at[b], AF.at[b]), AF.at[0 : NB - 1])
    arrive(sideways)

    squares = jnp.zeros((n.SLOTS, 1), F32)
    for k in range(X):
        source = G4[k].astype(F32).reshape(n.SLOTS * J, LANES).astype(BF16)
        for j in range(J):
            at = k * J + j
            part = mm(pick_row[j], source)
            squares += jnp.sum(part * part, axis=1, keepdims=True)
            rows[:, at * LANES : (at + 1) * LANES] = part * mn_ref[at : at + 1, :]
    inv_rows = lax.rsqrt(squares / n.D + NORM_EPS)
    rn[...] = (rows[...] * inv_rows).astype(BF16)
    normed = rn[...]
    hidden = (silu(mm_nt(normed, held["gp"][0])) * mm_nt(normed, held["up"][0])).astype(BF16)
    for k in range(X):
        X5[k] = mm(hidden, held["dn"][0, :, k * n.Q : (k + 1) * n.Q]).astype(BF16)
    sent = exchange("out_state", side, lambda k: (X5.at[(x + k) % X], Y5.at[x]), Y5.at[0 : X - 1])
    Y5[x] = X5[x]
    arrive(sent)
    total = Y5[0].astype(F32)
    for k in range(1, X):
        total += Y5[k].astype(F32)
    N5[...] = total.reshape(NM, NB * CAP, n.Q).astype(BF16)
    R5[m] = N5[m]
    sent = exchange("out_near", block, lambda k: (N5.at[(m + k) % NM], R5.at[m]), R5.at[0 : NM - 1])
    arrive(sent)
    total = R5[0].astype(F32)
    for k in range(1, NM):
        total += R5[k].astype(F32)
    total = total.astype(BF16)
    r_i, c_i = grid_of(NB * J * CAP, NB * CAP)
    match = div(r_i, J * CAP) * CAP + mod(r_i, CAP) == c_i
    which = mod(div(r_i, CAP), J)
    spread = jnp.zeros((NB * J * CAP, LANES), F32)
    for j in range(J):
        spread += mm(ones_where(match & (which == j)), total[:, j * LANES : (j + 1) * LANES])
    F5[...] = spread.reshape(NB, J * CAP, LANES).astype(BF16)
    Q5[b] = F5[b]
    sent = exchange("out_far", far, lambda k: (F5.at[(b + k) % NB], Q5.at[b]), Q5.at[0 : NB - 1])
    arrive(sent_aux)
    total = AF[0]
    for k in range(1, NB):
        total += AF[k]
    share = total[0:1, :] / (T * TOPK) * (total[1:2, :] / T)
    loss = EXPERTS * jnp.sum(jnp.where(l_i[:1] < EXPERTS, share, 0.0), axis=1, keepdims=True)
    load_ref[...] = total[0:1, :EXPERTS]
    loss_ref[...] = loss
    arrive(sent)
    back = Q5[...].astype(F32).reshape(NB * J * CAP, LANES)
    lo_ref[...] = (resid + mm(combine, back, HI)).astype(BF16)
    for copy in pending:
        copy.wait()
    for k, copy in downs:
        pl.when(b >= k)(copy.wait_send)
    for k in range(NB - 1):
        pl.when((k <= b) & climbing)(ups[k].wait_send)


def finish_kernel(*refs):
    count = len(refs) // 2
    copies = [
        pltpu.make_async_copy(refs[k], refs[count + k], refs[-1].at[k]) for k in range(count)
    ]
    for copy in copies:
        copy.start()
    for copy in copies:
        copy.wait()


class Sizes:
    pass


def per_device(
    head_count, state_count,
    tokens, mixer_norm, input_proj, conv_weight, conv_bias, conv_state, state_proj, step_gain, step_proj,
    step_bias, decay_log, skip_gain, ssm_state, output_proj, moe_norm, router_weight, expert_ids, slot_ids,
    gate_proj, up_proj, down_proj,
):
    n = Sizes()
    n.H, n.X, n.NB = head_count, state_count, EXPERTS
    n.NM = n.H // n.NB
    n.OWN, n.Q = tokens.shape
    n.J = n.Q // LANES
    n.R = n.OWN * n.J
    n.D = n.Q * n.X
    n.CONV = conv_weight.shape[0]
    _, n.T, n.C = conv_state.shape
    n.S = decay_log.shape[0]
    n.STATE = n.S * n.X
    n.RANK, n.PROJ = step_proj.shape[0], state_proj.shape[1]
    n.PW = -(-n.PROJ // LANES) * LANES
    n.TB = n.T // n.X // n.NM
    n.SLOTS = n.NM * n.NB * CAP
    n.FF = gate_proj.shape[2]

    tok = tokens.reshape(n.OWN, n.J, LANES).transpose(1, 0, 2).reshape(n.R, LANES)
    V = pltpu.VMEM
    operands = (
        mixer_norm.reshape(n.J, LANES), input_proj, conv_weight, conv_bias.reshape(1, -1), state_proj.T,
        step_gain.reshape(1, -1), step_proj, step_bias.reshape(1, -1), decay_log, skip_gain.reshape(1, -1),
        ssm_state, output_proj, moe_norm.reshape(-1, LANES), expert_ids.T, slot_ids.T,
        gate_proj.transpose(0, 2, 1), up_proj.transpose(0, 2, 1), down_proj,
    )
    vm = pl.BlockSpec(memory_space=pltpu.VMEM)
    hbm = pl.BlockSpec(memory_space=pltpu.HBM)
    wide = n.J * CAP
    scratch = [V(a.shape, a.dtype) for a in operands]
    scratch += [
        V(conv_state.shape[1:], F32), V((EXPERTS, n.Q), F32),
        V((n.J, n.T, n.H * n.R), BF16),
        V((n.J, n.SLOTS, n.SLOTS * n.J), BF16),
        V((n.NM, n.NB, n.R, LANES), BF16),
        V((n.X, n.T, n.C), BF16), V((n.X, n.T, n.C), BF16),
        V((n.X, 8, n.T), F32),
        V((n.T, n.C), BF16),
        V((n.NM, n.TB, n.PW), F32), V((n.NM, n.TB, n.PW), F32),
        V((n.NB, n.TB, n.PW), BF16), V((n.X, n.NM, n.TB, n.PW), BF16),
        V((n.X, n.T, n.C), BF16),
        V((n.NM, n.NB * n.OWN, n.Q), BF16), V((n.NM, n.NB * n.OWN, n.Q), BF16),
        V((n.NB, n.R, LANES), BF16), V((n.NB, n.R, LANES), BF16),
        V((n.X, n.R, LANES), F32),
        V((n.NB, wide, LANES), BF16), V((n.X, n.NM, n.NB, wide, LANES), BF16),
        V((n.SLOTS, n.D), F32), V((n.SLOTS, n.D), BF16),
        V((n.X, n.SLOTS, n.Q), BF16), V((n.X, n.SLOTS, n.Q), BF16),
        V((n.NM, n.NB * CAP, n.Q), BF16), V((n.NM, n.NB * CAP, n.Q), BF16),
        V((n.NB, wide, LANES), BF16), V((n.NB, wide, LANES), BF16),
        V((n.NM, 8, LANES), F32), V((n.NB, 8, LANES), F32),
    ]
    dma, regular = pltpu.SemaphoreType.DMA, pltpu.SemaphoreType.REGULAR
    climb = dma((n.NB - 1,))
    scratch += [
        dma((len(STAGES),)), dma((len(STAGES),)), dma((2, n.NM - 1)), climb, climb, climb, climb,
        regular, regular((n.NM - 1,)), dma((len(OPERANDS) + 4,)),
    ]
    shapes = (
        jax.ShapeDtypeStruct((n.R, LANES), BF16),
        jax.ShapeDtypeStruct(conv_state.shape, F32),
        jax.ShapeDtypeStruct(ssm_state.shape, F32),
        jax.ShapeDtypeStruct((1, EXPERTS), F32),
        jax.ShapeDtypeStruct((1, 1), F32),
    )
    results = pl.pallas_call(
        functools.partial(step_kernel, n),
        out_shape=shapes,
        in_specs=[hbm] * (len(operands) + 3),
        out_specs=(vm,) * len(shapes),
        scratch_shapes=scratch,
        compiler_params=pltpu.CompilerParams(
            collective_id=0, has_side_effects=True, vmem_limit_bytes=48 * 1024 * 1024
        ),
        name="mixer_moe_step",
    )(*[pltpu.with_memory_space_constraint(a, pltpu.HBM) for a in (tok, conv_state, router_weight.T, *operands)])
    out, new_conv, new_state, load, loss = pl.pallas_call(
        finish_kernel,
        out_shape=shapes,
        in_specs=[vm] * len(shapes),
        out_specs=(hbm,) * len(shapes),
        scratch_shapes=[dma((len(shapes),))],
        compiler_params=pltpu.CompilerParams(vmem_limit_bytes=1024 * 1024),
        name="finish",
    )(*results)
    layer_out = out.reshape(n.J, n.OWN, LANES).transpose(1, 0, 2).reshape(n.OWN, n.Q)
    return layer_out, new_conv, new_state, load.reshape(-1), loss.reshape(1)


def solution(mesh):
    in_specs = (
        P(("groups", "head"), "state"),
        P("state"),
        P(None, "state", "head"),
        P(None, "head"),
        P("head"),
        P(None, "groups", "head"),
        P("head", None),
        P(),
        P(None, "head"),
        P("head"),
        P("state", "head"),
        P("head"),
        P("state", "groups", "head"),
        P("head", "state"),
        P(),
        P(),
        P(("groups", "head"), None),
        P(("groups", "head"), None),
        P("head", None, "state"),
        P("head", None, "state"),
        P("head", "state", None),
    )
    out_specs = (
        P(("groups", "head"), "state"),
        P(None, "groups", "head"),
        P("state", "groups", "head"),
        P("groups"),
        P("groups"),
    )
    return jax.shard_map(
        functools.partial(per_device, mesh.shape["head"], mesh.shape["state"]),
        mesh=mesh, in_specs=in_specs, out_specs=out_specs, check_vma=False,
    )
```

```python
import functools

import jax
import jax.numpy as jnp
from jax import lax
from jax.experimental import pallas as pl
from jax.experimental.pallas import tpu as pltpu
from jax.sharding import PartitionSpec as P

EXPERTS = 8
TOPK = 2
CAP = 2
LANES = 128
NORM_EPS = 1e-05
STEP_EPS = 1e-06
MESH = pl.DeviceIdType.MESH
F32 = jnp.float32
BF16 = jnp.bfloat16
HI = lax.Precision.HIGHEST


def div(a, n):
    assert n & (n - 1) == 0
    return lax.shift_right_logical(a, jnp.int32(n.bit_length() - 1)) if n > 1 else a


def mod(a, n):
    assert n & (n - 1) == 0
    return a & (n - 1)


def grid_of(rows, cols):
    return (
        lax.broadcasted_iota(jnp.int32, (rows, cols), 0),
        lax.broadcasted_iota(jnp.int32, (rows, cols), 1),
    )


def ones_where(cond, dtype=BF16):
    return jnp.where(cond, 1.0, 0.0).astype(dtype)


def mm(a, b, precision=None):
    return jnp.dot(a, b, preferred_element_type=F32, precision=precision)


def mm_nt(a, b, precision=None):
    return lax.dot_general(
        a, b, (((1,), (1,)), ((), ())), preferred_element_type=F32, precision=precision
    )


def silu(v):
    return v * jax.nn.sigmoid(v)


def softplus(v):
    return jnp.maximum(v, 0.0) + jnp.log1p(jnp.exp(-jnp.abs(v)))


def by_distance(n):
    return sorted(range(1, n), key=lambda k: -min(k, n - k))


STAGES = (
    "tok_near", "tok_last", "branch", "gate", "square", "proj_near", "proj_far", "low_near", "low_state",
    "read", "mix_near", "mix_far", "stat", "row_far", "row_near", "row_state", "out_state", "out_near",
    "out_far", "aux_near", "aux_far",
)
OPERANDS = (
    "mixn", "win", "cw", "cb", "sp", "sg", "tp", "sb", "dl", "sk", "ssm", "op", "mn", "eid", "sid", "gp",
    "up", "dn",
)


def step_kernel(n, tok_hbm, cs_hbm, rw_hbm, *refs):
    count = len(OPERANDS)
    sources = refs[:count]
    lo_ref, nc_ref, ns_ref, load_ref, loss_ref = refs[count : count + 5]
    held = dict(zip(OPERANDS, refs[count + 5 : 2 * count + 5]))
    (
        cs, rw, pick, pick_row, G, XC, XG, XS, cob, P2, R2, F2, S2, XR, N3, R3, F3, Q3, ST, F4, G4, rows,
        rn, X5, Y5, N5, R5, F5, Q5, AN, AF, send_sem, recv_sem, piece_sem, up_send, up_recv, down_send,
        down_recv, wrap_sem, ready_up, ready_wrap, ready_near, load_sem,
    ) = refs[2 * count + 5 :]
    head = lax.axis_index("head")
    x = lax.axis_index("state")
    b = head // n.NM
    m = head % n.NM
    X, NB, NM, OWN, J, R, T, C, S = n.X, n.NB, n.NM, n.OWN, n.J, n.R, n.T, n.C, n.S

    def offset(k):
        return k if 2 * k <= NM else k - NM

    far = {k: {"head": ((b + k) % NB) * NM + m} for k in range(1, NB)}
    near = {k: {"head": (head + n.H + offset(k)) % n.H} for k in range(1, NM)}
    block = {k: {"head": b * NM + (m + k) % NM} for k in range(1, NM)}
    side = {k: {"state": (x + k) % X} for k in range(1, X)}

    barrier = pltpu.get_barrier_semaphore()
    around = [(head + n.H + o) % n.H for o in range(-(NM // 2), NM // 2 + 1) if o]

    def greet(partner):
        pl.semaphore_signal(barrier, inc=1, device_id=partner, device_id_type=MESH)

    for k in side:
        greet(side[k])
    for other in around:
        pl.when(other > head)(functools.partial(greet, {"head": other}))
    for k in range(1, NB):
        pl.when(b + k < NB)(functools.partial(greet, {"head": (b + k) * NM + m}))
    expected = b + (X - 1)
    for other in around:
        expected += jnp.where(other < head, 1, 0)

    loads = {}

    def load(name, src, dst):
        loads[name] = pltpu.make_async_copy(src, dst, load_sem.at[len(loads)])
        loads[name].start()

    load("tok", tok_hbm, G.at[m, b])
    for name, src in zip(OPERANDS, sources):
        load(name, src, held[name])
    load("conv", cs_hbm.at[0], cs)
    load("keep", cs_hbm.at[1 : n.CONV - 1], nc_ref.at[0 : n.CONV - 2])
    load("router", rw_hbm.at[:, pl.ds(pl.multiple_of(x * n.Q, n.Q), n.Q)], rw)
    mixn_ref, win, cw_ref, cb_ref = held["mixn"], held["win"], held["cw"], held["cb"]
    sp, sg_ref, tp, sb_ref, dl_ref = held["sp"], held["sg"], held["tp"], held["sb"], held["dl"]
    sk_ref, ssm, op, mn_ref = held["sk"], held["ssm"], held["op"], held["mn"]

    def loaded(*names):
        for name in names:
            loads[name].wait()

    pending = []

    def remote(src, dst, send, recv, partner):
        return pltpu.make_async_remote_copy(
            src_ref=src, dst_ref=dst, send_sem=send, recv_sem=recv, device_id=partner, device_id_type=MESH
        )

    def exchange(stage, group, pair, landing, first=None):
        at = STAGES.index(stage)
        for k in by_distance(len(group) + 1):
            if first is not None:
                first(k)
            src, dst = pair(k)
            remote(src, dst, send_sem.at[at], recv_sem.at[at], group[k]).start()
        pending.append(pltpu.make_async_copy(landing, landing, send_sem.at[at]))
        return pltpu.make_async_copy(landing, landing, recv_sem.at[at])

    def arrive(copy):
        copy.wait()

    def by_pieces(name, group, ref, at):
        near_at, side_at = STAGES.index(name + "_near"), STAGES.index(name + "_state")
        sent = {}
        order = by_distance(NM)
        for k in order:
            sent[k] = remote(
                ref.at[x, m], ref.at[x, m], send_sem.at[near_at], piece_sem.at[at, k - 1], group[k]
            )
            sent[k].start()
        for step in [0] + order[::-1]:
            piece = (m + NM - step) % NM
            if step:
                sent[step].wait_recv()
            for k in by_distance(X):
                remote(
                    ref.at[x, piece], ref.at[x, piece], send_sem.at[side_at], recv_sem.at[side_at], side[k]
                ).start()
        landing = ref.at[0, 0 : NM - 1]
        pending.append(pltpu.make_async_copy(landing, landing, send_sem.at[near_at]))
        landing = ref.at[0 : X - 1]
        pending.append(pltpu.make_async_copy(landing, landing, send_sem.at[side_at]))
        return pltpu.make_async_copy(landing, landing, recv_sem.at[side_at])

    loaded("tok")
    pl.semaphore_wait(barrier, expected)

    @pl.when(b > 0)
    def _():
        pl.semaphore_signal(ready_up, inc=1, device_id={"head": head - NM}, device_id_type=MESH)

    for k in near:
        source = (head + n.H - offset(k)) % n.H

        @pl.when(source < head)
        def _(k=k, source=source):
            pl.semaphore_signal(
                ready_near.at[k - 1], inc=1, device_id={"head": source}, device_id_type=MESH
            )

    own = G.at[m, b]
    downs = []
    for k in by_distance(NB):
        copy = remote(own, own, down_send.at[k - 1], down_recv.at[k - 1], {"head": head - k * NM})
        pl.when(b >= k)(copy.start)
        downs.append((k, copy))
    climbing = b < NB - 1
    ups = [
        remote(G.at[m, k], G.at[m, k], up_send.at[k], up_recv.at[k], {"head": head + NM})
        for k in range(NB - 1)
    ]

    @pl.when(climbing)
    def _():
        pl.semaphore_wait(ready_up, 1)

    top = NB - 1
    around_top = remote(G.at[m, 0], G.at[m, 0], wrap_sem.at[0], wrap_sem.at[1], {"head": top * NM + m})
    descent = remote(G.at[m, 0], G.at[m, 0], wrap_sem.at[0], wrap_sem.at[1], {"head": head - NM})
    below = b < NB // 2

    @pl.when(b == top)
    def _():
        pl.semaphore_signal(ready_wrap, inc=1, device_id={"head": m}, device_id_type=MESH)
        around_top.wait_recv()
        if top > NB // 2 + 1:
            descent.start()

    for k in range(NB - 2, 0, -1):
        pl.when(k < b)(ups[k].wait_recv)
        pl.when((k <= b) & climbing)(ups[k].start)
    pl.when((b > 0) & (b <= NB // 2))(ups[0].wait_recv)
    pl.when(below)(ups[0].start)

    @pl.when(b == 0)
    def _():
        pl.semaphore_wait(ready_wrap, 1)
        around_top.start()

    @pl.when((b > NB // 2) & (b < top))
    def _():
        around_top.wait_recv()
        pl.when(b > NB // 2 + 1)(descent.start)

    def from_above(last):
        for k, copy in sorted(downs, key=lambda t: t[0]):
            pl.when((b + k == NB - 1) if last else (b + k < NB - 1))(copy.wait_recv)

    def near_ready(k):
        target = (head + n.H + offset(k)) % n.H

        @pl.when(target > head)
        def _():
            pl.semaphore_wait(ready_near.at[k - 1], 1)

    from_above(False)
    early = G.at[m, 0 : NB - 1]
    sent_early = exchange(
        "tok_near", near, lambda k: (early, early), G.at[0 : NM - 1, 0 : NB - 1], near_ready
    )
    tok_bf = G[m, b]

    r_i, c_i = grid_of(T, n.H * R)
    tok_of = (div(mod(c_i, NB * R), R) * NM + div(c_i, NB * R)) * OWN + mod(c_i, OWN)
    match = tok_of == r_i
    which = mod(div(c_i, OWN), J)
    for j in range(J):
        pick[j] = ones_where(match & (which == j))
    r_i, c_i = grid_of(n.SLOTS, n.SLOTS * J)
    match = div(c_i, J * CAP) * CAP + mod(c_i, CAP) == r_i
    which = mod(div(c_i, CAP), J)
    for j in range(J):
        pick_row[j] = ones_where(match & (which == j))

    from_above(True)
    final = G.at[m, NB - 1]
    sent = exchange("tok_last", near, lambda k: (final, final), G.at[0, 0 : NM - 1])
    loaded("win", "mixn")
    arrive(sent_early)
    arrive(sent)

    gathered = G[...].reshape(n.H * R, LANES)
    conv_part = jnp.zeros((T, C), F32)
    gate_part = jnp.zeros((T, C), F32)
    squares = jnp.zeros((T, 1), F32)
    for j in range(J):
        tok_j = mm(pick[j], gathered)
        squares += jnp.sum(tok_j * tok_j, axis=1, keepdims=True)
        wide = tok_j * mixn_ref[j : j + 1, :]
        high = wide.astype(BF16)
        for half in (high, (wide - high.astype(F32)).astype(BF16)):
            conv_part += mm(half, win[0, j * LANES : (j + 1) * LANES, :])
            gate_part += mm(half, win[1, j * LANES : (j + 1) * LANES, :])
    XS[x] = jnp.broadcast_to(squares, (T, LANES)).T[:8, :]
    XC[x] = conv_part.astype(BF16)
    sent_sq = exchange("square", side, lambda k: (XS.at[x], XS.at[x]), XS.at[0 : X - 1])
    sent = exchange("branch", side, lambda k: (XC.at[x], XC.at[x]), XC.at[0 : X - 1])
    XG[x] = gate_part.astype(BF16)
    sent_gate = exchange("gate", side, lambda k: (XG.at[x], XG.at[x]), XG.at[0 : X - 1])

    loaded("conv", "keep", "cw", "cb", "sp")
    window = cb_ref[...] + cw_ref[0:1, :] * cs[...]
    for k in range(n.CONV - 2):
        window += cw_ref[k + 1 : k + 2, :] * nc_ref[k]
    P2[...] = jnp.zeros_like(P2)
    arrive(sent_sq)
    total = XS[0]
    for k in range(1, X):
        total += XS[k]
    inv_first = lax.rsqrt(jnp.broadcast_to(total[:1, :], (LANES, T)).T[:, :1] / n.D + NORM_EPS)
    arrive(sent)
    conv_in = XC[0].astype(F32)
    for k in range(1, X):
        conv_in += XC[k].astype(F32)
    conv_in = conv_in * inv_first
    nc_ref[n.CONV - 2] = conv_in
    conv_out = silu(window + cw_ref[n.CONV - 1 : n.CONV, :] * conv_in)
    cob[...] = conv_out.astype(BF16)

    quarter = T // X
    spare = n.PROJ - n.RANK

    def in_halves(wide):
        low, vectors = wide[:, : n.RANK], wide[:, n.RANK :]
        high = vectors.astype(BF16).astype(F32)
        rest = pltpu.roll(vectors - high, spare, 1)
        return jnp.concatenate([low, high + rest], axis=1).astype(BF16)

    part = mm_nt(cob[pl.ds(pl.multiple_of(x * quarter, quarter), quarter), :], sp[...])
    P2[:, :, : n.PROJ] = part.reshape(NM, n.TB, n.PROJ)
    R2[m] = P2[m]
    sent = exchange("proj_near", near, lambda k: (P2.at[(m + k) % NM], R2.at[m]), R2.at[0 : NM - 1])
    arrive(sent)
    total = R2[0]
    for k in range(1, NM):
        total += R2[k]
    F2[b] = in_halves(total)
    sent = exchange("proj_far", far, lambda k: (F2.at[b], F2.at[b]), F2.at[0 : NB - 1])
    loaded("tp", "ssm", "sg", "sb", "dl")
    arrive(sent)
    total = F2[0].astype(F32)
    for k in range(1, NB):
        total += F2[k].astype(F32)
    low, vectors = total[:, : n.RANK], total[:, n.RANK :]
    step_inv = lax.rsqrt(jnp.mean(low * low, axis=1, keepdims=True) + STEP_EPS)
    vectors = vectors + pltpu.roll(vectors, LANES - spare, 1)
    _, l_i = grid_of(n.TB, LANES)
    vectors = jnp.where(l_i < spare, vectors, 0.0)
    S2[x, m] = in_halves(jnp.concatenate([low * step_inv * sg_ref[...], vectors], axis=1))
    sent = by_pieces("low", near, S2, 0)
    arrive(sent_gate)
    gate = gate_part
    for k in range(1, X):
        gate += XG[(x + k) % X].astype(F32)
    gate = silu(gate * inv_first)
    rates = [jnp.exp(dl_ref[k : k + 1, :]) for k in range(S)]
    arrive(sent)

    projected = S2[...].astype(F32).reshape(T, n.PW)
    step_normed = projected[:, : n.RANK].astype(BF16)
    step_size = softplus(mm(step_normed, tp[...]) + sb_ref[...])
    vectors = projected[:, n.RANK :].astype(BF16)
    rows_i, _ = grid_of(LANES, C)
    driven = step_size * conv_out
    read = jnp.zeros((T, C), F32)
    for k in range(S):
        at = x * S + k
        b_in = mm(vectors, ones_where((rows_i == at) | (rows_i == spare + at)))
        at = at + n.STATE
        c_out = mm(vectors, ones_where((rows_i == at) | (rows_i == spare + at)))
        fresh = jnp.exp(-step_size * rates[k]) * ssm[k] + driven * b_in
        ns_ref[k] = fresh
        read += c_out * fresh
    XR[x] = read.astype(BF16)
    sent = exchange("read", side, lambda k: (XR.at[x], XR.at[x]), XR.at[0 : X - 1])
    loaded("op", "sk")
    r_i, c_i = grid_of(T, T)
    source = (div(mod(r_i, NB * OWN), OWN) * NM + div(r_i, NB * OWN)) * OWN + mod(r_i, OWN)
    by_member = ones_where(source == c_i)
    arrive(sent)
    for k in range(1, X):
        read += XR[(x + k) % X].astype(F32)
    act = ((read + sk_ref[...] * conv_out) * gate).astype(BF16)
    act = mm(by_member, act).astype(BF16)
    N3[...] = mm(act, op[...]).astype(BF16).reshape(NM, NB * OWN, n.Q)
    R3[m] = N3[m]
    sent = exchange("mix_near", near, lambda k: (N3.at[(m + k) % NM], R3.at[m]), R3.at[0 : NM - 1])
    arrive(sent)
    total = R3[0].astype(F32)
    for k in range(1, NM):
        total += R3[k].astype(F32)
    total = total.astype(BF16)
    r_i, c_i = grid_of(NB * R, NB * OWN)
    match = div(r_i, R) * OWN + mod(r_i, OWN) == c_i
    which = mod(div(r_i, OWN), J)
    spread = jnp.zeros((NB * R, LANES), F32)
    for j in range(J):
        spread += mm(ones_where(match & (which == j)), total[:, j * LANES : (j + 1) * LANES])
    F3[...] = spread.astype(BF16).reshape(NB, R, LANES)
    Q3[b] = F3[b]
    sent = exchange("mix_far", far, lambda k: (F3.at[(b + k) % NB], Q3.at[b]), Q3.at[0 : NB - 1])
    loaded("router", "mn", "eid", "sid")
    arrive(sent)
    total = Q3[0].astype(F32)
    for k in range(1, NB):
        total += Q3[k].astype(F32)

    resid_bf = (tok_bf.astype(F32) + total).astype(BF16)
    resid = resid_bf.astype(F32)
    row_i, lane_i = grid_of(R, LANES)
    hits, kept, slots = [], [], []
    i_i, t_i = grid_of(R, OWN)

    def by_row(ref, k):
        wide = jnp.broadcast_to(ref[k : k + 1, :], (R, OWN)).astype(F32)
        return jnp.sum(jnp.where(mod(i_i, OWN) == t_i, wide, 0.0), axis=1, keepdims=True).astype(jnp.int32)

    for k in range(TOPK):
        e_k, s_k = by_row(held["eid"], k), by_row(held["sid"], k)
        keep = s_k < CAP
        hits.append(lane_i == e_k)
        kept.append(keep)
        slots.append((lane_i == e_k * CAP + s_k) & keep)
    dispatch = sum(ones_where(s, F32) for s in slots).astype(BF16)
    d_i, q_i = grid_of(NB * J * CAP, LANES)
    slot_of = ones_where(q_i == div(d_i, J * CAP) * CAP + mod(d_i, CAP))
    d_i, c_i = grid_of(NB * J * CAP, R)
    chosen_rows = jnp.where(
        mod(div(d_i, CAP), J) == div(c_i, OWN), mm_nt(slot_of, dispatch), 0.0
    ).astype(BF16)
    F4[...] = mm(chosen_rows, resid_bf).reshape(NB, J * CAP, LANES).astype(BF16)
    G4[x, m, b] = F4[b]
    sent = exchange(
        "row_far", far, lambda k: (F4.at[(b + k) % NB], G4.at[x, m, b]), G4.at[x, m, 0 : NB - 1]
    )

    gain = jnp.zeros((R, LANES), F32)
    for j in range(J):
        gain = jnp.where(div(row_i, OWN) == j, mn_ref[pl.ds(x * J + j, 1), :], gain)
    scaled = resid * gain
    raw = jnp.zeros((R, EXPERTS), F32)
    for j in range(J):
        raw += mm_nt(
            jnp.where(div(row_i, OWN) == j, scaled, 0.0), rw[:, j * LANES : (j + 1) * LANES], HI
        )
    ST[x] = jnp.broadcast_to(jnp.sum(resid * resid, axis=1, keepdims=True), (R, LANES))
    ST[x, :, :EXPERTS] = raw
    sent_stat = exchange("stat", side, lambda k: (ST.at[x], ST.at[x]), ST.at[0 : X - 1])
    arrive(sent_stat)
    total = ST[0]
    for k in range(1, X):
        total += ST[k]
    r_i, c_i = grid_of(R, R)
    total = mm(ones_where(mod(r_i, OWN) == mod(c_i, OWN), F32), total, HI)
    inv_second = lax.rsqrt(total[:, EXPERTS : EXPERTS + 1] / n.D + NORM_EPS)
    logits = inv_second * total
    chosen = [jnp.sum(jnp.where(hit, logits, 0.0), axis=1, keepdims=True) for hit in hits]
    mixing = jnp.zeros((R, LANES), F32)
    for k in range(TOPK):
        weight = jax.nn.sigmoid(chosen[k] - chosen[1 - k])
        mixing += jnp.where(slots[k], weight, 0.0)
    first = row_i < OWN
    load = sum(ones_where(hits[k] & kept[k] & first, F32) for k in range(TOPK))
    load = jnp.sum(load, axis=0, keepdims=True)
    prob = jnp.where(first & (lane_i < EXPERTS), jax.nn.sigmoid(logits), 0.0)
    prob = jnp.sum(prob, axis=0, keepdims=True)
    a_i, l_i = grid_of(8, LANES)
    AN[m] = jnp.where(a_i == 0, load, jnp.where(a_i == 1, prob, 0.0))
    sent_aux = exchange("aux_near", block, lambda k: (AN.at[m], AN.at[m]), AN.at[0 : NM - 1])
    d_i, q_i = grid_of(R, NB * J * CAP)
    combine = jnp.where(
        mod(div(q_i, CAP), J) == div(d_i, OWN), mm_nt(mixing, slot_of.astype(F32), HI), 0.0
    )
    loaded("gp", "up", "dn")

    arrive(sent)

    sideways = by_pieces("row", block, G4, 1)
    arrive(sent_aux)
    total = AN[0]
    for k in range(1, NM):
        total += AN[k]
    AF[b] = total
    sent_aux = exchange("aux_far", far, lambda k: (AF.at[b], AF.at[b]), AF.at[0 : NB - 1])
    arrive(sideways)

    squares = jnp.zeros((n.SLOTS, 1), F32)
    for k in range(X):
        source = G4[k].astype(F32).reshape(n.SLOTS * J, LANES).astype(BF16)
        for j in range(J):
            at = k * J + j
            part = mm(pick_row[j], source)
            squares += jnp.sum(part * part, axis=1, keepdims=True)
            rows[:, at * LANES : (at + 1) * LANES] = part * mn_ref[at : at + 1, :]
    inv_rows = lax.rsqrt(squares / n.D + NORM_EPS)
    rn[...] = (rows[...] * inv_rows).astype(BF16)
    normed = rn[...]
    hidden = (silu(mm_nt(normed, held["gp"][0])) * mm_nt(normed, held["up"][0])).astype(BF16)

    def down_part(k):
        at = (x + k) % X
        columns = pl.ds(pl.multiple_of(at * n.Q, n.Q), n.Q)
        X5[at] = mm(hidden, held["dn"][0, :, columns]).astype(BF16)

    sent = exchange("out_state", side, lambda k: (X5.at[(x + k) % X], Y5.at[x]), Y5.at[0 : X - 1], down_part)
    down_part(0)
    Y5[x] = X5[x]
    arrive(sent)
    total = Y5[0].astype(F32)
    for k in range(1, X):
        total += Y5[k].astype(F32)
    N5[...] = total.reshape(NM, NB * CAP, n.Q).astype(BF16)
    R5[m] = N5[m]
    sent = exchange("out_near", block, lambda k: (N5.at[(m + k) % NM], R5.at[m]), R5.at[0 : NM - 1])
    arrive(sent)
    total = R5[0].astype(F32)
    for k in range(1, NM):
        total += R5[k].astype(F32)
    total = total.astype(BF16)
    r_i, c_i = grid_of(NB * J * CAP, NB * CAP)
    match = div(r_i, J * CAP) * CAP + mod(r_i, CAP) == c_i
    which = mod(div(r_i, CAP), J)
    spread = jnp.zeros((NB * J * CAP, LANES), F32)
    for j in range(J):
        spread += mm(ones_where(match & (which == j)), total[:, j * LANES : (j + 1) * LANES])
    F5[...] = spread.reshape(NB, J * CAP, LANES).astype(BF16)
    Q5[b] = F5[b]
    sent = exchange("out_far", far, lambda k: (F5.at[(b + k) % NB], Q5.at[b]), Q5.at[0 : NB - 1])
    arrive(sent_aux)
    total = AF[0]
    for k in range(1, NB):
        total += AF[k]
    share = total[0:1, :] / (T * TOPK) * (total[1:2, :] / T)
    loss = EXPERTS * jnp.sum(jnp.where(l_i[:1] < EXPERTS, share, 0.0), axis=1, keepdims=True)
    load_ref[...] = total[0:1, :EXPERTS]
    loss_ref[...] = loss
    arrive(sent)
    back = Q5[...].astype(F32).reshape(NB * J * CAP, LANES)
    lo_ref[...] = (resid + mm(combine, back, HI)).astype(BF16)
    for copy in pending:
        copy.wait()
    for k, copy in downs:
        pl.when(b >= k)(copy.wait_send)
    for k in range(1, NB - 1):
        pl.when((k <= b) & climbing)(ups[k].wait_send)
    pl.when(below)(ups[0].wait_send)
    pl.when((b == 0) | (b > NB // 2 + 1))(around_top.wait_send)


def finish_kernel(*refs):
    count = len(refs) // 2
    copies = [
        pltpu.make_async_copy(refs[k], refs[count + k], refs[-1].at[k]) for k in range(count)
    ]
    for copy in copies:
        copy.start()
    for copy in copies:
        copy.wait()


class Sizes:
    pass


def per_device(
    head_count, state_count,
    tokens, mixer_norm, input_proj, conv_weight, conv_bias, conv_state, state_proj, step_gain, step_proj,
    step_bias, decay_log, skip_gain, ssm_state, output_proj, moe_norm, router_weight, expert_ids, slot_ids,
    gate_proj, up_proj, down_proj,
):
    n = Sizes()
    n.H, n.X, n.NB = head_count, state_count, EXPERTS
    n.NM = n.H // n.NB
    n.OWN, n.Q = tokens.shape
    n.J = n.Q // LANES
    n.R = n.OWN * n.J
    n.D = n.Q * n.X
    n.CONV = conv_weight.shape[0]
    _, n.T, n.C = conv_state.shape
    n.S = decay_log.shape[0]
    n.STATE = n.S * n.X
    n.RANK, n.PROJ = step_proj.shape[0], state_proj.shape[1]
    n.PW = -(-n.PROJ // LANES) * LANES
    n.TB = n.T // n.X // n.NM
    n.SLOTS = n.NM * n.NB * CAP
    n.FF = gate_proj.shape[2]

    tok = tokens.reshape(n.OWN, n.J, LANES).transpose(1, 0, 2).reshape(n.R, LANES)
    V = pltpu.VMEM
    operands = (
        mixer_norm.reshape(n.J, LANES), input_proj, conv_weight, conv_bias.reshape(1, -1), state_proj.T,
        step_gain.reshape(1, -1), step_proj, step_bias.reshape(1, -1), decay_log, skip_gain.reshape(1, -1),
        ssm_state, output_proj, moe_norm.reshape(-1, LANES), expert_ids.T, slot_ids.T,
        gate_proj.transpose(0, 2, 1), up_proj.transpose(0, 2, 1), down_proj,
    )
    vm = pl.BlockSpec(memory_space=pltpu.VMEM)
    hbm = pl.BlockSpec(memory_space=pltpu.HBM)
    wide = n.J * CAP
    scratch = [V(a.shape, a.dtype) for a in operands]
    scratch += [
        V(conv_state.shape[1:], F32), V((EXPERTS, n.Q), F32),
        V((n.J, n.T, n.H * n.R), BF16),
        V((n.J, n.SLOTS, n.SLOTS * n.J), BF16),
        V((n.NM, n.NB, n.R, LANES), BF16),
        V((n.X, n.T, n.C), BF16), V((n.X, n.T, n.C), BF16),
        V((n.X, 8, n.T), F32),
        V((n.T, n.C), BF16),
        V((n.NM, n.TB, n.PW), F32), V((n.NM, n.TB, n.PW), F32),
        V((n.NB, n.TB, n.PW), BF16), V((n.X, n.NM, n.TB, n.PW), BF16),
        V((n.X, n.T, n.C), BF16),
        V((n.NM, n.NB * n.OWN, n.Q), BF16), V((n.NM, n.NB * n.OWN, n.Q), BF16),
        V((n.NB, n.R, LANES), BF16), V((n.NB, n.R, LANES), BF16),
        V((n.X, n.R, LANES), F32),
        V((n.NB, wide, LANES), BF16), V((n.X, n.NM, n.NB, wide, LANES), BF16),
        V((n.SLOTS, n.D), F32), V((n.SLOTS, n.D), BF16),
        V((n.X, n.SLOTS, n.Q), BF16), V((n.X, n.SLOTS, n.Q), BF16),
        V((n.NM, n.NB * CAP, n.Q), BF16), V((n.NM, n.NB * CAP, n.Q), BF16),
        V((n.NB, wide, LANES), BF16), V((n.NB, wide, LANES), BF16),
        V((n.NM, 8, LANES), F32), V((n.NB, 8, LANES), F32),
    ]
    dma, regular = pltpu.SemaphoreType.DMA, pltpu.SemaphoreType.REGULAR
    climb = dma((n.NB - 1,))
    scratch += [
        dma((len(STAGES),)), dma((len(STAGES),)), dma((2, n.NM - 1)), climb, climb, climb, climb,
        dma((2,)), regular, regular, regular((n.NM - 1,)), dma((len(OPERANDS) + 4,)),
    ]
    shapes = (
        jax.ShapeDtypeStruct((n.R, LANES), BF16),
        jax.ShapeDtypeStruct(conv_state.shape, F32),
        jax.ShapeDtypeStruct(ssm_state.shape, F32),
        jax.ShapeDtypeStruct((1, EXPERTS), F32),
        jax.ShapeDtypeStruct((1, 1), F32),
    )
    results = pl.pallas_call(
        functools.partial(step_kernel, n),
        out_shape=shapes,
        in_specs=[hbm] * (len(operands) + 3),
        out_specs=(vm,) * len(shapes),
        scratch_shapes=scratch,
        compiler_params=pltpu.CompilerParams(
            collective_id=0, has_side_effects=True, vmem_limit_bytes=48 * 1024 * 1024
        ),
        name="mixer_moe_step",
    )(*[pltpu.with_memory_space_constraint(a, pltpu.HBM) for a in (tok, conv_state, router_weight.T, *operands)])
    out, new_conv, new_state, load, loss = pl.pallas_call(
        finish_kernel,
        out_shape=shapes,
        in_specs=[vm] * len(shapes),
        out_specs=(hbm,) * len(shapes),
        scratch_shapes=[dma((len(shapes),))],
        compiler_params=pltpu.CompilerParams(vmem_limit_bytes=1024 * 1024),
        name="finish",
    )(*results)
    layer_out = out.reshape(n.J, n.OWN, LANES).transpose(1, 0, 2).reshape(n.OWN, n.Q)
    return layer_out, new_conv, new_state, load.reshape(-1), loss.reshape(1)


def solution(mesh):
    in_specs = (
        P(("groups", "head"), "state"),
        P("state"),
        P(None, "state", "head"),
        P(None, "head"),
        P("head"),
        P(None, "groups", "head"),
        P("head", None),
        P(),
        P(None, "head"),
        P("head"),
        P("state", "head"),
        P("head"),
        P("state", "groups", "head"),
        P("head", "state"),
        P(),
        P(),
        P(("groups", "head"), None),
        P(("groups", "head"), None),
        P("head", None, "state"),
        P("head", None, "state"),
        P("head", "state", None),
    )
    out_specs = (
        P(("groups", "head"), "state"),
        P(None, "groups", "head"),
        P("state", "groups", "head"),
        P("groups"),
        P("groups"),
    )
    return jax.shard_map(
        functools.partial(per_device, mesh.shape["head"], mesh.shape["state"]),
        mesh=mesh, in_specs=in_specs, out_specs=out_specs, check_vma=False,
    )
```

```python
import functools

import jax
import jax.numpy as jnp
from jax import lax
from jax.experimental import pallas as pl
from jax.experimental.pallas import tpu as pltpu
from jax.sharding import PartitionSpec as P

EXPERTS = 8
TOPK = 2
CAP = 2
LANES = 128
NORM_EPS = 1e-05
STEP_EPS = 1e-06
MESH = pl.DeviceIdType.MESH
F32 = jnp.float32
BF16 = jnp.bfloat16
HI = lax.Precision.HIGHEST


def div(a, n):
    assert n & (n - 1) == 0
    return lax.shift_right_logical(a, jnp.int32(n.bit_length() - 1)) if n > 1 else a


def mod(a, n):
    assert n & (n - 1) == 0
    return a & (n - 1)


def grid_of(rows, cols):
    return (
        lax.broadcasted_iota(jnp.int32, (rows, cols), 0),
        lax.broadcasted_iota(jnp.int32, (rows, cols), 1),
    )


def ones_where(cond, dtype=BF16):
    return jnp.where(cond, 1.0, 0.0).astype(dtype)


def mm(a, b, precision=None):
    return jnp.dot(a, b, preferred_element_type=F32, precision=precision)


def mm_nt(a, b, precision=None):
    return lax.dot_general(
        a, b, (((1,), (1,)), ((), ())), preferred_element_type=F32, precision=precision
    )


def silu(v):
    return v * jax.nn.sigmoid(v)


def softplus(v):
    return jnp.maximum(v, 0.0) + jnp.log1p(jnp.exp(-jnp.abs(v)))


def by_distance(n):
    return sorted(range(1, n), key=lambda k: -min(k, n - k))


STAGES = (
    "tok_near", "tok_last", "branch", "gate", "square", "proj_near", "proj_far", "low_near", "low_state",
    "read", "mix_near", "mix_far", "stat", "row_far", "row_near", "row_state", "out_state", "out_near",
    "out_far", "aux_near", "aux_far",
)
OPERANDS = (
    "mixn", "win", "cw", "cb", "sp", "sg", "tp", "sb", "dl", "sk", "ssm", "op", "mn", "eid", "sid", "gp",
    "up", "dn",
)


def step_kernel(n, tok_hbm, cs_hbm, rw_hbm, *refs):
    count = len(OPERANDS)
    sources = refs[:count]
    lo_ref, nc_ref, ns_ref, load_ref, loss_ref = refs[count : count + 5]
    held = dict(zip(OPERANDS, refs[count + 5 : 2 * count + 5]))
    (
        cs, rw, pick, pick_row, G, XC, XG, XS, cob, P2, R2, F2, S2, XR, N3, R3, F3, Q3, ST, F4, G4, rows,
        rn, X5, Y5, N5, R5, F5, Q5, AN, AF, send_sem, recv_sem, piece_sem, up_send, up_recv, down_send,
        down_recv, onward_send, wrap_sem, ready_up, ready_wrap, ready_zero, ready_near, load_sem,
    ) = refs[2 * count + 5 :]
    head = lax.axis_index("head")
    x = lax.axis_index("state")
    b = head // n.NM
    m = head % n.NM
    X, NB, NM, OWN, J, R, T, C, S = n.X, n.NB, n.NM, n.OWN, n.J, n.R, n.T, n.C, n.S

    def offset(k):
        return k if 2 * k <= NM else k - NM

    far = {k: {"head": ((b + k) % NB) * NM + m} for k in range(1, NB)}
    near = {k: {"head": (head + n.H + offset(k)) % n.H} for k in range(1, NM)}
    block = {k: {"head": b * NM + (m + k) % NM} for k in range(1, NM)}
    side = {k: {"state": (x + k) % X} for k in range(1, X)}

    barrier = pltpu.get_barrier_semaphore()
    around = [(head + n.H + o) % n.H for o in range(-(NM // 2), NM // 2 + 1) if o]

    def greet(partner):
        pl.semaphore_signal(barrier, inc=1, device_id=partner, device_id_type=MESH)

    for k in side:
        greet(side[k])
    for other in around:
        pl.when(other > head)(functools.partial(greet, {"head": other}))
    top = NB - 1
    for k in range(1, NB - 1):
        pl.when((b > 0) & (b + k < NB))(functools.partial(greet, {"head": (b + k) * NM + m}))
    pl.when(b == 0)(functools.partial(greet, {"head": top * NM + m}))
    pl.when(b == 1)(functools.partial(greet, {"head": m}))
    expected = (X - 1) + jnp.where(b == 0, 1, b - 1) + jnp.where(b == top, 1, 0)
    for other in around:
        expected += jnp.where(other < head, 1, 0)

    loads = {}

    def load(name, src, dst):
        loads[name] = pltpu.make_async_copy(src, dst, load_sem.at[len(loads)])
        loads[name].start()

    load("tok", tok_hbm, G.at[m, b])
    for name, src in zip(OPERANDS, sources):
        load(name, src, held[name])
    load("conv", cs_hbm.at[0], cs)
    load("keep", cs_hbm.at[1 : n.CONV - 1], nc_ref.at[0 : n.CONV - 2])
    load("router", rw_hbm.at[:, pl.ds(pl.multiple_of(x * n.Q, n.Q), n.Q)], rw)
    mixn_ref, win, cw_ref, cb_ref = held["mixn"], held["win"], held["cw"], held["cb"]
    sp, sg_ref, tp, sb_ref, dl_ref = held["sp"], held["sg"], held["tp"], held["sb"], held["dl"]
    sk_ref, ssm, op, mn_ref = held["sk"], held["ssm"], held["op"], held["mn"]

    def loaded(*names):
        for name in names:
            loads[name].wait()

    pending = []

    def remote(src, dst, send, recv, partner):
        return pltpu.make_async_remote_copy(
            src_ref=src, dst_ref=dst, send_sem=send, recv_sem=recv, device_id=partner, device_id_type=MESH
        )

    def exchange(stage, group, pair, landing, first=None):
        at = STAGES.index(stage)
        for k in by_distance(len(group) + 1):
            if first is not None:
                first(k)
            src, dst = pair(k)
            remote(src, dst, send_sem.at[at], recv_sem.at[at], group[k]).start()
        pending.append(pltpu.make_async_copy(landing, landing, send_sem.at[at]))
        return pltpu.make_async_copy(landing, landing, recv_sem.at[at])

    def arrive(copy):
        copy.wait()

    def by_pieces(name, group, ref, at):
        near_at, side_at = STAGES.index(name + "_near"), STAGES.index(name + "_state")
        sent = {}
        order = by_distance(NM)
        for k in order:
            sent[k] = remote(
                ref.at[x, m], ref.at[x, m], send_sem.at[near_at], piece_sem.at[at, k - 1], group[k]
            )
            sent[k].start()
        for step in [0] + order[::-1]:
            piece = (m + NM - step) % NM
            if step:
                sent[step].wait_recv()
            for k in by_distance(X):
                remote(
                    ref.at[x, piece], ref.at[x, piece], send_sem.at[side_at], recv_sem.at[side_at], side[k]
                ).start()
        landing = ref.at[0, 0 : NM - 1]
        pending.append(pltpu.make_async_copy(landing, landing, send_sem.at[near_at]))
        landing = ref.at[0 : X - 1]
        pending.append(pltpu.make_async_copy(landing, landing, send_sem.at[side_at]))
        return pltpu.make_async_copy(landing, landing, recv_sem.at[side_at])

    loaded("tok")
    pl.semaphore_wait(barrier, expected)

    @pl.when(b > 1)
    def _():
        pl.semaphore_signal(ready_up, inc=1, device_id={"head": head - NM}, device_id_type=MESH)

    @pl.when(b == 0)
    def _():
        pl.semaphore_signal(ready_zero, inc=1, device_id={"head": head + NM}, device_id_type=MESH)

    for k in near:
        source = (head + n.H - offset(k)) % n.H

        @pl.when(source < head)
        def _(k=k, source=source):
            pl.semaphore_signal(
                ready_near.at[k - 1], inc=1, device_id={"head": source}, device_id_type=MESH
            )

    own = G.at[m, b]
    downs = []
    for k in by_distance(NB):
        copy = remote(own, own, down_send.at[k - 1], down_recv.at[k - 1], {"head": head - k * NM})
        pl.when(b > k)(copy.start)
        downs.append((k, copy))
    climbing = b < NB - 1
    ups = [
        remote(G.at[m, k], G.at[m, k], up_send.at[k], up_recv.at[k], {"head": head + NM})
        for k in range(NB - 1)
    ]

    @pl.when((b > 0) & climbing)
    def _():
        pl.semaphore_wait(ready_up, 1)

    around_top = remote(G.at[m, 0], G.at[m, 0], wrap_sem.at[0], wrap_sem.at[1], {"head": top * NM + m})
    descent = remote(G.at[m, 0], G.at[m, 0], wrap_sem.at[0], wrap_sem.at[1], {"head": head - NM})
    below = b < NB // 2

    @pl.when(b == top)
    def _():
        pl.semaphore_signal(ready_wrap, inc=1, device_id={"head": m}, device_id_type=MESH)
        around_top.wait_recv()
        if top > NB // 2 + 1:
            descent.start()

    for k in range(NB - 2, 0, -1):
        pl.when(k < b)(ups[k].wait_recv)
        pl.when((k <= b) & climbing)(ups[k].start)
    pl.when((b > 0) & (b <= NB // 2))(ups[0].wait_recv)
    pl.when(below)(ups[0].start)

    @pl.when(b == 0)
    def _():
        pl.semaphore_wait(ready_wrap, 1)
        around_top.start()

    @pl.when((b > NB // 2) & (b < top))
    def _():
        around_top.wait_recv()
        pl.when(b > NB // 2 + 1)(descent.start)

    onward = [
        remote(G.at[m, k], G.at[m, k], onward_send.at[k - 1], down_recv.at[k - 1], {"head": head - NM})
        for k in range(1, NB)
    ]

    def from_above(last):
        for k, copy in sorted(downs, key=lambda t: t[0]):
            pl.when((b + k == NB - 1) if last else (b + k < NB - 1))(copy.wait_recv)
            if (k == NB - 2) == last and k < NB - 1:
                pl.when(b == 1)(onward[k].start)

    @pl.when(b == 1)
    def _():
        pl.semaphore_wait(ready_zero, 1)
        onward[0].start()

    def near_ready(k):
        target = (head + n.H + offset(k)) % n.H

        @pl.when(target > head)
        def _():
            pl.semaphore_wait(ready_near.at[k - 1], 1)

    from_above(False)
    early = G.at[m, 0 : NB - 1]
    sent_early = exchange(
        "tok_near", near, lambda k: (early, early), G.at[0 : NM - 1, 0 : NB - 1], near_ready
    )
    tok_bf = G[m, b]

    r_i, c_i = grid_of(T, n.H * R)
    tok_of = (div(mod(c_i, NB * R), R) * NM + div(c_i, NB * R)) * OWN + mod(c_i, OWN)
    match = tok_of == r_i
    which = mod(div(c_i, OWN), J)
    for j in range(J):
        pick[j] = ones_where(match & (which == j))
    r_i, c_i = grid_of(n.SLOTS, n.SLOTS * J)
    match = div(c_i, J * CAP) * CAP + mod(c_i, CAP) == r_i
    which = mod(div(c_i, CAP), J)
    for j in range(J):
        pick_row[j] = ones_where(match & (which == j))

    from_above(True)
    final = G.at[m, NB - 1]
    sent = exchange("tok_last", near, lambda k: (final, final), G.at[0, 0 : NM - 1])
    loaded("win", "mixn")
    arrive(sent_early)
    arrive(sent)

    gathered = G[...].reshape(n.H * R, LANES)
    conv_part = jnp.zeros((T, C), F32)
    gate_part = jnp.zeros((T, C), F32)
    squares = jnp.zeros((T, 1), F32)
    for j in range(J):
        tok_j = mm(pick[j], gathered)
        squares += jnp.sum(tok_j * tok_j, axis=1, keepdims=True)
        wide = tok_j * mixn_ref[j : j + 1, :]
        high = wide.astype(BF16)
        for half in (high, (wide - high.astype(F32)).astype(BF16)):
            conv_part += mm(half, win[0, j * LANES : (j + 1) * LANES, :])
            gate_part += mm(half, win[1, j * LANES : (j + 1) * LANES, :])
    XS[x] = jnp.broadcast_to(squares, (T, LANES)).T[:8, :]
    XC[x] = conv_part.astype(BF16)
    sent_sq = exchange("square", side, lambda k: (XS.at[x], XS.at[x]), XS.at[0 : X - 1])
    sent = exchange("branch", side, lambda k: (XC.at[x], XC.at[x]), XC.at[0 : X - 1])
    XG[x] = gate_part.astype(BF16)
    sent_gate = exchange("gate", side, lambda k: (XG.at[x], XG.at[x]), XG.at[0 : X - 1])

    loaded("conv", "keep", "cw", "cb", "sp")
    window = cb_ref[...] + cw_ref[0:1, :] * cs[...]
    for k in range(n.CONV - 2):
        window += cw_ref[k + 1 : k + 2, :] * nc_ref[k]
    P2[...] = jnp.zeros_like(P2)
    arrive(sent_sq)
    total = XS[0]
    for k in range(1, X):
        total += XS[k]
    inv_first = lax.rsqrt(jnp.broadcast_to(total[:1, :], (LANES, T)).T[:, :1] / n.D + NORM_EPS)
    arrive(sent)
    conv_in = XC[0].astype(F32)
    for k in range(1, X):
        conv_in += XC[k].astype(F32)
    conv_in = conv_in * inv_first
    nc_ref[n.CONV - 2] = conv_in
    conv_out = silu(window + cw_ref[n.CONV - 1 : n.CONV, :] * conv_in)
    cob[...] = conv_out.astype(BF16)

    quarter = T // X
    spare = n.PROJ - n.RANK

    def in_halves(wide):
        low, vectors = wide[:, : n.RANK], wide[:, n.RANK :]
        high = vectors.astype(BF16).astype(F32)
        rest = pltpu.roll(vectors - high, spare, 1)
        return jnp.concatenate([low, high + rest], axis=1).astype(BF16)

    part = mm_nt(cob[pl.ds(pl.multiple_of(x * quarter, quarter), quarter), :], sp[...])
    P2[:, :, : n.PROJ] = part.reshape(NM, n.TB, n.PROJ)
    R2[m] = P2[m]
    sent = exchange("proj_near", near, lambda k: (P2.at[(m + k) % NM], R2.at[m]), R2.at[0 : NM - 1])
    arrive(sent)
    total = R2[0]
    for k in range(1, NM):
        total += R2[k]
    F2[b] = in_halves(total)
    sent = exchange("proj_far", far, lambda k: (F2.at[b], F2.at[b]), F2.at[0 : NB - 1])
    loaded("tp", "ssm", "sg", "sb", "dl")
    arrive(sent)
    total = F2[0].astype(F32)
    for k in range(1, NB):
        total += F2[k].astype(F32)
    low, vectors = total[:, : n.RANK], total[:, n.RANK :]
    step_inv = lax.rsqrt(jnp.mean(low * low, axis=1, keepdims=True) + STEP_EPS)
    vectors = vectors + pltpu.roll(vectors, LANES - spare, 1)
    _, l_i = grid_of(n.TB, LANES)
    vectors = jnp.where(l_i < spare, vectors, 0.0)
    S2[x, m] = in_halves(jnp.concatenate([low * step_inv * sg_ref[...], vectors], axis=1))
    sent = by_pieces("low", near, S2, 0)
    arrive(sent_gate)
    gate = gate_part
    for k in range(1, X):
        gate += XG[(x + k) % X].astype(F32)
    gate = silu(gate * inv_first)
    rates = [jnp.exp(dl_ref[k : k + 1, :]) for k in range(S)]
    arrive(sent)

    projected = S2[...].astype(F32).reshape(T, n.PW)
    step_normed = projected[:, : n.RANK].astype(BF16)
    step_size = softplus(mm(step_normed, tp[...]) + sb_ref[...])
    vectors = projected[:, n.RANK :].astype(BF16)
    rows_i, _ = grid_of(LANES, C)
    driven = step_size * conv_out
    read = jnp.zeros((T, C), F32)
    for k in range(S):
        at = x * S + k
        b_in = mm(vectors, ones_where((rows_i == at) | (rows_i == spare + at)))
        at = at + n.STATE
        c_out = mm(vectors, ones_where((rows_i == at) | (rows_i == spare + at)))
        fresh = jnp.exp(-step_size * rates[k]) * ssm[k] + driven * b_in
        ns_ref[k] = fresh
        read += c_out * fresh
    XR[x] = read.astype(BF16)
    sent = exchange("read", side, lambda k: (XR.at[x], XR.at[x]), XR.at[0 : X - 1])
    loaded("op", "sk")
    r_i, c_i = grid_of(T, T)
    source = (div(mod(r_i, NB * OWN), OWN) * NM + div(r_i, NB * OWN)) * OWN + mod(r_i, OWN)
    by_member = ones_where(source == c_i)
    arrive(sent)
    for k in range(1, X):
        read += XR[(x + k) % X].astype(F32)
    act = ((read + sk_ref[...] * conv_out) * gate).astype(BF16)
    act = mm(by_member, act).astype(BF16)
    N3[...] = mm(act, op[...]).astype(BF16).reshape(NM, NB * OWN, n.Q)
    R3[m] = N3[m]
    sent = exchange("mix_near", near, lambda k: (N3.at[(m + k) % NM], R3.at[m]), R3.at[0 : NM - 1])
    arrive(sent)
    total = R3[0].astype(F32)
    for k in range(1, NM):
        total += R3[k].astype(F32)
    total = total.astype(BF16)
    r_i, c_i = grid_of(NB * R, NB * OWN)
    match = div(r_i, R) * OWN + mod(r_i, OWN) == c_i
    which = mod(div(r_i, OWN), J)
    spread = jnp.zeros((NB * R, LANES), F32)
    for j in range(J):
        spread += mm(ones_where(match & (which == j)), total[:, j * LANES : (j + 1) * LANES])
    F3[...] = spread.astype(BF16).reshape(NB, R, LANES)
    Q3[b] = F3[b]
    sent = exchange("mix_far", far, lambda k: (F3.at[(b + k) % NB], Q3.at[b]), Q3.at[0 : NB - 1])
    loaded("router", "mn", "eid", "sid")
    arrive(sent)
    total = Q3[0].astype(F32)
    for k in range(1, NB):
        total += Q3[k].astype(F32)

    resid_bf = (tok_bf.astype(F32) + total).astype(BF16)
    resid = resid_bf.astype(F32)
    row_i, lane_i = grid_of(R, LANES)
    hits, kept, slots = [], [], []
    i_i, t_i = grid_of(R, OWN)

    def by_row(ref, k):
        wide = jnp.broadcast_to(ref[k : k + 1, :], (R, OWN)).astype(F32)
        return jnp.sum(jnp.where(mod(i_i, OWN) == t_i, wide, 0.0), axis=1, keepdims=True).astype(jnp.int32)

    for k in range(TOPK):
        e_k, s_k = by_row(held["eid"], k), by_row(held["sid"], k)
        keep = s_k < CAP
        hits.append(lane_i == e_k)
        kept.append(keep)
        slots.append((lane_i == e_k * CAP + s_k) & keep)
    dispatch = sum(ones_where(s, F32) for s in slots).astype(BF16)
    d_i, q_i = grid_of(NB * J * CAP, LANES)
    slot_of = ones_where(q_i == div(d_i, J * CAP) * CAP + mod(d_i, CAP))
    d_i, c_i = grid_of(NB * J * CAP, R)
    chosen_rows = jnp.where(
        mod(div(d_i, CAP), J) == div(c_i, OWN), mm_nt(slot_of, dispatch), 0.0
    ).astype(BF16)
    F4[...] = mm(chosen_rows, resid_bf).reshape(NB, J * CAP, LANES).astype(BF16)
    G4[x, m, b] = F4[b]
    sent = exchange(
        "row_far", far, lambda k: (F4.at[(b + k) % NB], G4.at[x, m, b]), G4.at[x, m, 0 : NB - 1]
    )

    gain = jnp.zeros((R, LANES), F32)
    for j in range(J):
        gain = jnp.where(div(row_i, OWN) == j, mn_ref[pl.ds(x * J + j, 1), :], gain)
    scaled = resid * gain
    raw = jnp.zeros((R, EXPERTS), F32)
    for j in range(J):
        raw += mm_nt(
            jnp.where(div(row_i, OWN) == j, scaled, 0.0), rw[:, j * LANES : (j + 1) * LANES], HI
        )
    ST[x] = jnp.broadcast_to(jnp.sum(resid * resid, axis=1, keepdims=True), (R, LANES))
    ST[x, :, :EXPERTS] = raw
    sent_stat = exchange("stat", side, lambda k: (ST.at[x], ST.at[x]), ST.at[0 : X - 1])
    arrive(sent_stat)
    total = ST[0]
    for k in range(1, X):
        total += ST[k]
    r_i, c_i = grid_of(R, R)
    total = mm(ones_where(mod(r_i, OWN) == mod(c_i, OWN), F32), total, HI)
    inv_second = lax.rsqrt(total[:, EXPERTS : EXPERTS + 1] / n.D + NORM_EPS)
    logits = inv_second * total
    chosen = [jnp.sum(jnp.where(hit, logits, 0.0), axis=1, keepdims=True) for hit in hits]
    mixing = jnp.zeros((R, LANES), F32)
    for k in range(TOPK):
        weight = jax.nn.sigmoid(chosen[k] - chosen[1 - k])
        mixing += jnp.where(slots[k], weight, 0.0)
    first = row_i < OWN
    load = sum(ones_where(hits[k] & kept[k] & first, F32) for k in range(TOPK))
    load = jnp.sum(load, axis=0, keepdims=True)
    prob = jnp.where(first & (lane_i < EXPERTS), jax.nn.sigmoid(logits), 0.0)
    prob = jnp.sum(prob, axis=0, keepdims=True)
    a_i, l_i = grid_of(8, LANES)
    AN[m] = jnp.where(a_i == 0, load, jnp.where(a_i == 1, prob, 0.0))
    sent_aux = exchange("aux_near", block, lambda k: (AN.at[m], AN.at[m]), AN.at[0 : NM - 1])
    d_i, q_i = grid_of(R, NB * J * CAP)
    combine = jnp.where(
        mod(div(q_i, CAP), J) == div(d_i, OWN), mm_nt(mixing, slot_of.astype(F32), HI), 0.0
    )
    loaded("gp", "up", "dn")

    arrive(sent)

    sideways = by_pieces("row", block, G4, 1)
    arrive(sent_aux)
    total = AN[0]
    for k in range(1, NM):
        total += AN[k]
    AF[b] = total
    sent_aux = exchange("aux_far", far, lambda k: (AF.at[b], AF.at[b]), AF.at[0 : NB - 1])
    arrive(sideways)

    squares = jnp.zeros((n.SLOTS, 1), F32)
    for k in range(X):
        source = G4[k].astype(F32).reshape(n.SLOTS * J, LANES).astype(BF16)
        for j in range(J):
            at = k * J + j
            part = mm(pick_row[j], source)
            squares += jnp.sum(part * part, axis=1, keepdims=True)
            rows[:, at * LANES : (at + 1) * LANES] = part * mn_ref[at : at + 1, :]
    inv_rows = lax.rsqrt(squares / n.D + NORM_EPS)
    rn[...] = (rows[...] * inv_rows).astype(BF16)
    normed = rn[...]
    hidden = (silu(mm_nt(normed, held["gp"][0])) * mm_nt(normed, held["up"][0])).astype(BF16)

    def down_part(k):
        at = (x + k) % X
        columns = pl.ds(pl.multiple_of(at * n.Q, n.Q), n.Q)
        X5[at] = mm(hidden, held["dn"][0, :, columns]).astype(BF16)

    sent = exchange("out_state", side, lambda k: (X5.at[(x + k) % X], Y5.at[x]), Y5.at[0 : X - 1], down_part)
    down_part(0)
    Y5[x] = X5[x]
    arrive(sent)
    total = Y5[0].astype(F32)
    for k in range(1, X):
        total += Y5[k].astype(F32)
    N5[...] = total.reshape(NM, NB * CAP, n.Q).astype(BF16)
    R5[m] = N5[m]
    sent = exchange("out_near", block, lambda k: (N5.at[(m + k) % NM], R5.at[m]), R5.at[0 : NM - 1])
    arrive(sent)
    total = R5[0].astype(F32)
    for k in range(1, NM):
        total += R5[k].astype(F32)
    total = total.astype(BF16)
    r_i, c_i = grid_of(NB * J * CAP, NB * CAP)
    match = div(r_i, J * CAP) * CAP + mod(r_i, CAP) == c_i
    which = mod(div(r_i, CAP), J)
    spread = jnp.zeros((NB * J * CAP, LANES), F32)
    for j in range(J):
        spread += mm(ones_where(match & (which == j)), total[:, j * LANES : (j + 1) * LANES])
    F5[...] = spread.reshape(NB, J * CAP, LANES).astype(BF16)
    Q5[b] = F5[b]
    sent = exchange("out_far", far, lambda k: (F5.at[(b + k) % NB], Q5.at[b]), Q5.at[0 : NB - 1])
    arrive(sent_aux)
    total = AF[0]
    for k in range(1, NB):
        total += AF[k]
    share = total[0:1, :] / (T * TOPK) * (total[1:2, :] / T)
    loss = EXPERTS * jnp.sum(jnp.where(l_i[:1] < EXPERTS, share, 0.0), axis=1, keepdims=True)
    load_ref[...] = total[0:1, :EXPERTS]
    loss_ref[...] = loss
    arrive(sent)
    back = Q5[...].astype(F32).reshape(NB * J * CAP, LANES)
    lo_ref[...] = (resid + mm(combine, back, HI)).astype(BF16)
    for copy in pending:
        copy.wait()
    for k, copy in downs:
        pl.when(b > k)(copy.wait_send)
        pl.when(b == 1)(onward[k - 1].wait_send)
    for k in range(1, NB - 1):
        pl.when((k <= b) & climbing)(ups[k].wait_send)
    pl.when(below)(ups[0].wait_send)
    pl.when((b == 0) | (b > NB // 2 + 1))(around_top.wait_send)


def finish_kernel(*refs):
    count = len(refs) // 2
    copies = [
        pltpu.make_async_copy(refs[k], refs[count + k], refs[-1].at[k]) for k in range(count)
    ]
    for copy in copies:
        copy.start()
    for copy in copies:
        copy.wait()


class Sizes:
    pass


def per_device(
    head_count, state_count,
    tokens, mixer_norm, input_proj, conv_weight, conv_bias, conv_state, state_proj, step_gain, step_proj,
    step_bias, decay_log, skip_gain, ssm_state, output_proj, moe_norm, router_weight, expert_ids, slot_ids,
    gate_proj, up_proj, down_proj,
):
    n = Sizes()
    n.H, n.X, n.NB = head_count, state_count, EXPERTS
    n.NM = n.H // n.NB
    n.OWN, n.Q = tokens.shape
    n.J = n.Q // LANES
    n.R = n.OWN * n.J
    n.D = n.Q * n.X
    n.CONV = conv_weight.shape[0]
    _, n.T, n.C = conv_state.shape
    n.S = decay_log.shape[0]
    n.STATE = n.S * n.X
    n.RANK, n.PROJ = step_proj.shape[0], state_proj.shape[1]
    n.PW = -(-n.PROJ // LANES) * LANES
    n.TB = n.T // n.X // n.NM
    n.SLOTS = n.NM * n.NB * CAP
    n.FF = gate_proj.shape[2]

    tok = tokens.reshape(n.OWN, n.J, LANES).transpose(1, 0, 2).reshape(n.R, LANES)
    V = pltpu.VMEM
    operands = (
        mixer_norm.reshape(n.J, LANES), input_proj, conv_weight, conv_bias.reshape(1, -1), state_proj.T,
        step_gain.reshape(1, -1), step_proj, step_bias.reshape(1, -1), decay_log, skip_gain.reshape(1, -1),
        ssm_state, output_proj, moe_norm.reshape(-1, LANES), expert_ids.T, slot_ids.T,
        gate_proj.transpose(0, 2, 1), up_proj.transpose(0, 2, 1), down_proj,
    )
    vm = pl.BlockSpec(memory_space=pltpu.VMEM)
    hbm = pl.BlockSpec(memory_space=pltpu.HBM)
    wide = n.J * CAP
    scratch = [V(a.shape, a.dtype) for a in operands]
    scratch += [
        V(conv_state.shape[1:], F32), V((EXPERTS, n.Q), F32),
        V((n.J, n.T, n.H * n.R), BF16),
        V((n.J, n.SLOTS, n.SLOTS * n.J), BF16),
        V((n.NM, n.NB, n.R, LANES), BF16),
        V((n.X, n.T, n.C), BF16), V((n.X, n.T, n.C), BF16),
        V((n.X, 8, n.T), F32),
        V((n.T, n.C), BF16),
        V((n.NM, n.TB, n.PW), F32), V((n.NM, n.TB, n.PW), F32),
        V((n.NB, n.TB, n.PW), BF16), V((n.X, n.NM, n.TB, n.PW), BF16),
        V((n.X, n.T, n.C), BF16),
        V((n.NM, n.NB * n.OWN, n.Q), BF16), V((n.NM, n.NB * n.OWN, n.Q), BF16),
        V((n.NB, n.R, LANES), BF16), V((n.NB, n.R, LANES), BF16),
        V((n.X, n.R, LANES), F32),
        V((n.NB, wide, LANES), BF16), V((n.X, n.NM, n.NB, wide, LANES), BF16),
        V((n.SLOTS, n.D), F32), V((n.SLOTS, n.D), BF16),
        V((n.X, n.SLOTS, n.Q), BF16), V((n.X, n.SLOTS, n.Q), BF16),
        V((n.NM, n.NB * CAP, n.Q), BF16), V((n.NM, n.NB * CAP, n.Q), BF16),
        V((n.NB, wide, LANES), BF16), V((n.NB, wide, LANES), BF16),
        V((n.NM, 8, LANES), F32), V((n.NB, 8, LANES), F32),
    ]
    dma, regular = pltpu.SemaphoreType.DMA, pltpu.SemaphoreType.REGULAR
    climb = dma((n.NB - 1,))
    scratch += [
        dma((len(STAGES),)), dma((len(STAGES),)), dma((2, n.NM - 1)), climb, climb, climb, climb, climb,
        dma((2,)), regular, regular, regular, regular((n.NM - 1,)), dma((len(OPERANDS) + 4,)),
    ]
    shapes = (
        jax.ShapeDtypeStruct((n.R, LANES), BF16),
        jax.ShapeDtypeStruct(conv_state.shape, F32),
        jax.ShapeDtypeStruct(ssm_state.shape, F32),
        jax.ShapeDtypeStruct((1, EXPERTS), F32),
        jax.ShapeDtypeStruct((1, 1), F32),
    )
    results = pl.pallas_call(
        functools.partial(step_kernel, n),
        out_shape=shapes,
        in_specs=[hbm] * (len(operands) + 3),
        out_specs=(vm,) * len(shapes),
        scratch_shapes=scratch,
        compiler_params=pltpu.CompilerParams(
            collective_id=0, has_side_effects=True, vmem_limit_bytes=48 * 1024 * 1024
        ),
        name="mixer_moe_step",
    )(*[pltpu.with_memory_space_constraint(a, pltpu.HBM) for a in (tok, conv_state, router_weight.T, *operands)])
    out, new_conv, new_state, load, loss = pl.pallas_call(
        finish_kernel,
        out_shape=shapes,
        in_specs=[vm] * len(shapes),
        out_specs=(hbm,) * len(shapes),
        scratch_shapes=[dma((len(shapes),))],
        compiler_params=pltpu.CompilerParams(vmem_limit_bytes=1024 * 1024),
        name="finish",
    )(*results)
    layer_out = out.reshape(n.J, n.OWN, LANES).transpose(1, 0, 2).reshape(n.OWN, n.Q)
    return layer_out, new_conv, new_state, load.reshape(-1), loss.reshape(1)


def solution(mesh):
    in_specs = (
        P(("groups", "head"), "state"),
        P("state"),
        P(None, "state", "head"),
        P(None, "head"),
        P("head"),
        P(None, "groups", "head"),
        P("head", None),
        P(),
        P(None, "head"),
        P("head"),
        P("state", "head"),
        P("head"),
        P("state", "groups", "head"),
        P("head", "state"),
        P(),
        P(),
        P(("groups", "head"), None),
        P(("groups", "head"), None),
        P("head", None, "state"),
        P("head", None, "state"),
        P("head", "state", None),
    )
    out_specs = (
        P(("groups", "head"), "state"),
        P(None, "groups", "head"),
        P("state", "groups", "head"),
        P("groups"),
        P("groups"),
    )
    return jax.shard_map(
        functools.partial(per_device, mesh.shape["head"], mesh.shape["state"]),
        mesh=mesh, in_specs=in_specs, out_specs=out_specs, check_vma=False,
    )
```

```python
import functools

import jax
import jax.numpy as jnp
from jax import lax
from jax.experimental import pallas as pl
from jax.experimental.pallas import tpu as pltpu
from jax.sharding import PartitionSpec as P

EXPERTS = 8
TOPK = 2
CAP = 2
LANES = 128
NORM_EPS = 1e-05
STEP_EPS = 1e-06
MESH = pl.DeviceIdType.MESH
F32 = jnp.float32
BF16 = jnp.bfloat16
HI = lax.Precision.HIGHEST


def div(a, n):
    assert n & (n - 1) == 0
    return lax.shift_right_logical(a, jnp.int32(n.bit_length() - 1)) if n > 1 else a


def mod(a, n):
    assert n & (n - 1) == 0
    return a & (n - 1)


def grid_of(rows, cols):
    return (
        lax.broadcasted_iota(jnp.int32, (rows, cols), 0),
        lax.broadcasted_iota(jnp.int32, (rows, cols), 1),
    )


def ones_where(cond, dtype=BF16):
    return jnp.where(cond, 1.0, 0.0).astype(dtype)


def mm(a, b, precision=None):
    return jnp.dot(a, b, preferred_element_type=F32, precision=precision)


def mm_nt(a, b, precision=None):
    return lax.dot_general(
        a, b, (((1,), (1,)), ((), ())), preferred_element_type=F32, precision=precision
    )


def silu(v):
    return v * jax.nn.sigmoid(v)


def softplus(v):
    return jnp.maximum(v, 0.0) + jnp.log1p(jnp.exp(-jnp.abs(v)))


def by_distance(n):
    return sorted(range(1, n), key=lambda k: -min(k, n - k))


STAGES = (
    "tok_near", "tok_last", "branch", "gate", "square", "proj_near", "proj_far", "low_near", "low_state",
    "read", "mix_near", "mix_far", "stat", "row_far", "row_near", "row_state", "out_state", "out_near",
    "out_far", "aux_near", "aux_far",
)
OPERANDS = (
    "mixn", "win", "cw", "cb", "sp", "sg", "tp", "sb", "dl", "sk", "ssm", "op", "mn", "eid", "sid", "gp",
    "up", "dn",
)


def step_kernel(n, tok_hbm, cs_hbm, rw_hbm, *refs):
    count = len(OPERANDS)
    sources = refs[:count]
    lo_ref, nc_ref, ns_ref, load_ref, loss_ref = refs[count : count + 5]
    held = dict(zip(OPERANDS, refs[count + 5 : 2 * count + 5]))
    (
        cs, rw, pick, pick_row, G, XC, XG, XS, cob, P2, R2, F2, S2, XR, N3, R3, F3, Q3, ST, F4, G4, rows,
        rn, X5, Y5, N5, R5, F5, Q5, AN, AF, send_sem, recv_sem, piece_sem, up_send, up_recv, down_send,
        down_recv, onward_send, wrap_sem, ready_up, ready_wrap, ready_zero, ready_near, load_sem,
    ) = refs[2 * count + 5 :]
    head = lax.axis_index("head")
    x = lax.axis_index("state")
    b = head // n.NM
    m = head % n.NM
    X, NB, NM, OWN, J, R, T, C, S = n.X, n.NB, n.NM, n.OWN, n.J, n.R, n.T, n.C, n.S

    def offset(k):
        return k if 2 * k <= NM else k - NM

    far = {k: {"head": ((b + k) % NB) * NM + m} for k in range(1, NB)}
    near = {k: {"head": (head + n.H + offset(k)) % n.H} for k in range(1, NM)}
    block = {k: {"head": b * NM + (m + k) % NM} for k in range(1, NM)}
    side = {k: {"state": (x + k) % X} for k in range(1, X)}

    barrier = pltpu.get_barrier_semaphore()
    around = [(head + n.H + o) % n.H for o in range(-(NM // 2), NM // 2 + 1) if o]

    def greet(partner):
        pl.semaphore_signal(barrier, inc=1, device_id=partner, device_id_type=MESH)

    for k in side:
        greet(side[k])
    for other in around:
        pl.when(other > head)(functools.partial(greet, {"head": other}))
    top = NB - 1
    for k in range(1, NB - 1):
        pl.when((b > 0) & (b + k < NB))(functools.partial(greet, {"head": (b + k) * NM + m}))
    pl.when(b == 0)(functools.partial(greet, {"head": top * NM + m}))
    pl.when(b == 1)(functools.partial(greet, {"head": m}))
    expected = (X - 1) + jnp.where(b == 0, 1, b - 1) + jnp.where(b == top, 1, 0)
    for other in around:
        expected += jnp.where(other < head, 1, 0)

    loads = {}

    def load(name, src, dst):
        loads[name] = pltpu.make_async_copy(src, dst, load_sem.at[len(loads)])
        loads[name].start()

    load("tok", tok_hbm, G.at[m, b])
    for name, src in zip(OPERANDS, sources):
        load(name, src, held[name])
    load("conv", cs_hbm.at[0], cs)
    load("keep", cs_hbm.at[1 : n.CONV - 1], nc_ref.at[0 : n.CONV - 2])
    load("router", rw_hbm.at[:, pl.ds(pl.multiple_of(x * n.Q, n.Q), n.Q)], rw)
    mixn_ref, win, cw_ref, cb_ref = held["mixn"], held["win"], held["cw"], held["cb"]
    sp, sg_ref, tp, sb_ref, dl_ref = held["sp"], held["sg"], held["tp"], held["sb"], held["dl"]
    sk_ref, ssm, op, mn_ref = held["sk"], held["ssm"], held["op"], held["mn"]

    def loaded(*names):
        for name in names:
            loads[name].wait()

    pending = []

    def remote(src, dst, send, recv, partner):
        return pltpu.make_async_remote_copy(
            src_ref=src, dst_ref=dst, send_sem=send, recv_sem=recv, device_id=partner, device_id_type=MESH
        )

    def exchange(stage, group, pair, landing, first=None):
        at = STAGES.index(stage)
        for k in by_distance(len(group) + 1):
            if first is not None:
                first(k)
            src, dst = pair(k)
            remote(src, dst, send_sem.at[at], recv_sem.at[at], group[k]).start()
        pending.append(pltpu.make_async_copy(landing, landing, send_sem.at[at]))
        return pltpu.make_async_copy(landing, landing, recv_sem.at[at])

    def arrive(copy):
        copy.wait()

    def by_pieces(name, group, ref, at):
        near_at, side_at = STAGES.index(name + "_near"), STAGES.index(name + "_state")
        sent = {}
        order = by_distance(NM)
        for k in order:
            sent[k] = remote(
                ref.at[x, m], ref.at[x, m], send_sem.at[near_at], piece_sem.at[at, k - 1], group[k]
            )
            sent[k].start()
        for step in [0] + order[::-1]:
            piece = (m + NM - step) % NM
            if step:
                sent[step].wait_recv()
            for k in by_distance(X):
                remote(
                    ref.at[x, piece], ref.at[x, piece], send_sem.at[side_at], recv_sem.at[side_at], side[k]
                ).start()
        landing = ref.at[0, 0 : NM - 1]
        pending.append(pltpu.make_async_copy(landing, landing, send_sem.at[near_at]))
        landing = ref.at[0 : X - 1]
        pending.append(pltpu.make_async_copy(landing, landing, send_sem.at[side_at]))
        return pltpu.make_async_copy(landing, landing, recv_sem.at[side_at])

    loaded("tok")
    pl.semaphore_wait(barrier, expected)

    @pl.when(b > 1)
    def _():
        pl.semaphore_signal(ready_up, inc=1, device_id={"head": head - NM}, device_id_type=MESH)

    @pl.when(b == 0)
    def _():
        pl.semaphore_signal(ready_zero, inc=1, device_id={"head": head + NM}, device_id_type=MESH)

    for k in near:
        source = (head + n.H - offset(k)) % n.H

        @pl.when(source < head)
        def _(k=k, source=source):
            pl.semaphore_signal(
                ready_near.at[k - 1], inc=1, device_id={"head": source}, device_id_type=MESH
            )

    own = G.at[m, b]
    downs = []
    for k in by_distance(NB):
        copy = remote(own, own, down_send.at[k - 1], down_recv.at[k - 1], {"head": head - k * NM})
        pl.when((b > k) | (b == k if k == top else False))(copy.start)
        downs.append((k, copy))
    climbing = b < NB - 1
    ups = [
        remote(G.at[m, k], G.at[m, k], up_send.at[k], up_recv.at[k], {"head": head + NM})
        for k in range(NB - 1)
    ]

    @pl.when((b > 0) & climbing)
    def _():
        pl.semaphore_wait(ready_up, 1)

    around_top = remote(G.at[m, 0], G.at[m, 0], wrap_sem.at[1], wrap_sem.at[0], {"head": top * NM + m})
    descents = [
        remote(G.at[m, 0], G.at[m, 0], wrap_sem.at[1 + k], wrap_sem.at[0], {"head": head - k * NM})
        for k in range(1, top - NB // 2)
    ]
    below = b < NB // 2

    @pl.when(b == top)
    def _():
        pl.semaphore_signal(ready_wrap, inc=1, device_id={"head": m}, device_id_type=MESH)
        around_top.wait_recv()
        for copy in descents:
            copy.start()

    for k in range(NB - 2, 0, -1):
        pl.when(k < b)(ups[k].wait_recv)
        pl.when((k <= b) & climbing)(ups[k].start)
    pl.when((b > 0) & (b <= NB // 2))(ups[0].wait_recv)
    pl.when(below)(ups[0].start)

    @pl.when(b == 0)
    def _():
        pl.semaphore_wait(ready_wrap, 1)
        around_top.start()

    @pl.when((b > NB // 2) & (b < top))
    def _():
        around_top.wait_recv()

    onward = [
        remote(G.at[m, k], G.at[m, k], onward_send.at[k - 1], down_recv.at[k - 1], {"head": head - NM})
        for k in range(1, top)
    ]

    def from_above(last):
        for k, copy in sorted(downs, key=lambda t: t[0]):
            pl.when((b + k == NB - 1) if last else (b + k < NB - 1))(copy.wait_recv)
            if not last and k < top - 1:
                pl.when(b == 1)(onward[k].start)

    @pl.when(b == 1)
    def _():
        pl.semaphore_wait(ready_zero, 1)
        onward[0].start()

    def near_ready(k):
        target = (head + n.H + offset(k)) % n.H

        @pl.when(target > head)
        def _():
            pl.semaphore_wait(ready_near.at[k - 1], 1)

    from_above(False)
    early = G.at[m, 0 : NB - 1]
    sent_early = exchange(
        "tok_near", near, lambda k: (early, early), G.at[0 : NM - 1, 0 : NB - 1], near_ready
    )
    tok_bf = G[m, b]

    per = NM * OWN
    r_i, c_i = grid_of(NM * R, NM * R)
    pick[...] = ones_where(
        (mod(div(c_i, OWN), J) == div(r_i, per)) & (div(c_i, R) * OWN + mod(c_i, OWN) == mod(r_i, per))
    )
    pair = 2 * NB * CAP
    r_i, c_i = grid_of(pair * J, pair * J)
    pick_row[...] = ones_where(
        (mod(div(c_i, CAP), J) == div(r_i, pair))
        & (div(c_i, J * CAP) * CAP + mod(c_i, CAP) == mod(r_i, pair))
    )

    from_above(True)
    final = G.at[m, NB - 1]
    sent = exchange("tok_last", near, lambda k: (final, final), G.at[0, 0 : NM - 1])
    loaded("win", "mixn")
    arrive(sent_early)
    arrive(sent)

    by_block = [mm(pick[...], G[:, k].reshape(NM * R, LANES)) for k in range(NB)]
    conv_part = jnp.zeros((T, C), F32)
    gate_part = jnp.zeros((T, C), F32)
    squares = jnp.zeros((T, 1), F32)
    for j in range(J):
        tok_j = jnp.concatenate([rows_k[j * per : (j + 1) * per] for rows_k in by_block], axis=0)
        squares += jnp.sum(tok_j * tok_j, axis=1, keepdims=True)
        wide = tok_j * mixn_ref[j : j + 1, :]
        high = wide.astype(BF16)
        for half in (high, (wide - high.astype(F32)).astype(BF16)):
            conv_part += mm(half, win[0, j * LANES : (j + 1) * LANES, :])
            gate_part += mm(half, win[1, j * LANES : (j + 1) * LANES, :])
    XS[x] = jnp.broadcast_to(squares, (T, LANES)).T[:8, :]
    XC[x] = conv_part.astype(BF16)
    sent_sq = exchange("square", side, lambda k: (XS.at[x], XS.at[x]), XS.at[0 : X - 1])
    sent = exchange("branch", side, lambda k: (XC.at[x], XC.at[x]), XC.at[0 : X - 1])
    XG[x] = gate_part.astype(BF16)
    sent_gate = exchange("gate", side, lambda k: (XG.at[x], XG.at[x]), XG.at[0 : X - 1])

    loaded("conv", "keep", "cw", "cb", "sp")
    window = cb_ref[...] + cw_ref[0:1, :] * cs[...]
    for k in range(n.CONV - 2):
        window += cw_ref[k + 1 : k + 2, :] * nc_ref[k]
    P2[...] = jnp.zeros_like(P2)
    arrive(sent_sq)
    total = XS[0]
    for k in range(1, X):
        total += XS[k]
    inv_first = lax.rsqrt(jnp.broadcast_to(total[:1, :], (LANES, T)).T[:, :1] / n.D + NORM_EPS)
    arrive(sent)
    conv_in = XC[0].astype(F32)
    for k in range(1, X):
        conv_in += XC[k].astype(F32)
    conv_in = conv_in * inv_first
    nc_ref[n.CONV - 2] = conv_in
    conv_out = silu(window + cw_ref[n.CONV - 1 : n.CONV, :] * conv_in)
    cob[...] = conv_out.astype(BF16)

    quarter = T // X
    spare = n.PROJ - n.RANK

    def in_halves(wide):
        low, vectors = wide[:, : n.RANK], wide[:, n.RANK :]
        high = vectors.astype(BF16).astype(F32)
        rest = pltpu.roll(vectors - high, spare, 1)
        return jnp.concatenate([low, high + rest], axis=1).astype(BF16)

    part = mm_nt(cob[pl.ds(pl.multiple_of(x * quarter, quarter), quarter), :], sp[...])
    P2[:, :, : n.PROJ] = part.reshape(NM, n.TB, n.PROJ)
    R2[m] = P2[m]
    sent = exchange("proj_near", near, lambda k: (P2.at[(m + k) % NM], R2.at[m]), R2.at[0 : NM - 1])
    arrive(sent)
    total = R2[0]
    for k in range(1, NM):
        total += R2[k]
    F2[b] = in_halves(total)
    sent = exchange("proj_far", far, lambda k: (F2.at[b], F2.at[b]), F2.at[0 : NB - 1])
    loaded("tp", "ssm", "sg", "sb", "dl")
    arrive(sent)
    total = F2[0].astype(F32)
    for k in range(1, NB):
        total += F2[k].astype(F32)
    low, vectors = total[:, : n.RANK], total[:, n.RANK :]
    step_inv = lax.rsqrt(jnp.mean(low * low, axis=1, keepdims=True) + STEP_EPS)
    vectors = vectors + pltpu.roll(vectors, LANES - spare, 1)
    _, l_i = grid_of(n.TB, LANES)
    vectors = jnp.where(l_i < spare, vectors, 0.0)
    S2[x, m] = in_halves(jnp.concatenate([low * step_inv * sg_ref[...], vectors], axis=1))
    sent = by_pieces("low", near, S2, 0)
    arrive(sent_gate)
    gate = gate_part
    for k in range(1, X):
        gate += XG[(x + k) % X].astype(F32)
    gate = silu(gate * inv_first)
    rates = [jnp.exp(dl_ref[k : k + 1, :]) for k in range(S)]
    arrive(sent)

    projected = S2[...].astype(F32).reshape(T, n.PW)
    step_normed = projected[:, : n.RANK].astype(BF16)
    step_size = softplus(mm(step_normed, tp[...]) + sb_ref[...])
    vectors = projected[:, n.RANK :].astype(BF16)
    rows_i, _ = grid_of(LANES, C)
    driven = step_size * conv_out
    read = jnp.zeros((T, C), F32)
    for k in range(S):
        at = x * S + k
        b_in = mm(vectors, ones_where((rows_i == at) | (rows_i == spare + at)))
        at = at + n.STATE
        c_out = mm(vectors, ones_where((rows_i == at) | (rows_i == spare + at)))
        fresh = jnp.exp(-step_size * rates[k]) * ssm[k] + driven * b_in
        ns_ref[k] = fresh
        read += c_out * fresh
    XR[x] = read.astype(BF16)
    sent = exchange("read", side, lambda k: (XR.at[x], XR.at[x]), XR.at[0 : X - 1])
    loaded("op", "sk")
    r_i, c_i = grid_of(T, T)
    source = (div(mod(r_i, NB * OWN), OWN) * NM + div(r_i, NB * OWN)) * OWN + mod(r_i, OWN)
    by_member = ones_where(source == c_i)
    arrive(sent)
    for k in range(1, X):
        read += XR[(x + k) % X].astype(F32)
    act = ((read + sk_ref[...] * conv_out) * gate).astype(BF16)
    act = mm(by_member, act).astype(BF16)
    N3[...] = mm(act, op[...]).astype(BF16).reshape(NM, NB * OWN, n.Q)
    R3[m] = N3[m]
    sent = exchange("mix_near", near, lambda k: (N3.at[(m + k) % NM], R3.at[m]), R3.at[0 : NM - 1])
    arrive(sent)
    total = R3[0].astype(F32)
    for k in range(1, NM):
        total += R3[k].astype(F32)
    total = total.astype(BF16)
    r_i, c_i = grid_of(NB * R, NB * OWN)
    match = div(r_i, R) * OWN + mod(r_i, OWN) == c_i
    which = mod(div(r_i, OWN), J)
    spread = jnp.zeros((NB * R, LANES), F32)
    for j in range(J):
        spread += mm(ones_where(match & (which == j)), total[:, j * LANES : (j + 1) * LANES])
    F3[...] = spread.astype(BF16).reshape(NB, R, LANES)
    Q3[b] = F3[b]
    sent = exchange("mix_far", far, lambda k: (F3.at[(b + k) % NB], Q3.at[b]), Q3.at[0 : NB - 1])
    loaded("router", "mn", "eid", "sid")
    arrive(sent)
    total = Q3[0].astype(F32)
    for k in range(1, NB):
        total += Q3[k].astype(F32)

    resid_bf = (tok_bf.astype(F32) + total).astype(BF16)
    resid = resid_bf.astype(F32)
    row_i, lane_i = grid_of(R, LANES)
    hits, kept, slots = [], [], []
    i_i, t_i = grid_of(R, OWN)

    def by_row(ref, k):
        wide = jnp.broadcast_to(ref[k : k + 1, :], (R, OWN)).astype(F32)
        return jnp.sum(jnp.where(mod(i_i, OWN) == t_i, wide, 0.0), axis=1, keepdims=True).astype(jnp.int32)

    for k in range(TOPK):
        e_k, s_k = by_row(held["eid"], k), by_row(held["sid"], k)
        keep = s_k < CAP
        hits.append(lane_i == e_k)
        kept.append(keep)
        slots.append((lane_i == e_k * CAP + s_k) & keep)
    dispatch = sum(ones_where(s, F32) for s in slots).astype(BF16)
    d_i, q_i = grid_of(NB * J * CAP, LANES)
    slot_of = ones_where(q_i == div(d_i, J * CAP) * CAP + mod(d_i, CAP))
    d_i, c_i = grid_of(NB * J * CAP, R)
    chosen_rows = jnp.where(
        mod(div(d_i, CAP), J) == div(c_i, OWN), mm_nt(slot_of, dispatch), 0.0
    ).astype(BF16)
    F4[...] = mm(chosen_rows, resid_bf).reshape(NB, J * CAP, LANES).astype(BF16)
    G4[x, m, b] = F4[b]
    sent = exchange(
        "row_far", far, lambda k: (F4.at[(b + k) % NB], G4.at[x, m, b]), G4.at[x, m, 0 : NB - 1]
    )

    gain = jnp.zeros((R, LANES), F32)
    for j in range(J):
        gain = jnp.where(div(row_i, OWN) == j, mn_ref[pl.ds(x * J + j, 1), :], gain)
    scaled = resid * gain
    raw = jnp.zeros((R, EXPERTS), F32)
    for j in range(J):
        raw += mm_nt(
            jnp.where(div(row_i, OWN) == j, scaled, 0.0), rw[:, j * LANES : (j + 1) * LANES], HI
        )
    ST[x] = jnp.broadcast_to(jnp.sum(resid * resid, axis=1, keepdims=True), (R, LANES))
    ST[x, :, :EXPERTS] = raw
    sent_stat = exchange("stat", side, lambda k: (ST.at[x], ST.at[x]), ST.at[0 : X - 1])
    arrive(sent_stat)
    total = ST[0]
    for k in range(1, X):
        total += ST[k]
    r_i, c_i = grid_of(R, R)
    total = mm(ones_where(mod(r_i, OWN) == mod(c_i, OWN), F32), total, HI)
    inv_second = lax.rsqrt(total[:, EXPERTS : EXPERTS + 1] / n.D + NORM_EPS)
    logits = inv_second * total
    chosen = [jnp.sum(jnp.where(hit, logits, 0.0), axis=1, keepdims=True) for hit in hits]
    mixing = jnp.zeros((R, LANES), F32)
    for k in range(TOPK):
        weight = jax.nn.sigmoid(chosen[k] - chosen[1 - k])
        mixing += jnp.where(slots[k], weight, 0.0)
    first = row_i < OWN
    load = sum(ones_where(hits[k] & kept[k] & first, F32) for k in range(TOPK))
    load = jnp.sum(load, axis=0, keepdims=True)
    prob = jnp.where(first & (lane_i < EXPERTS), jax.nn.sigmoid(logits), 0.0)
    prob = jnp.sum(prob, axis=0, keepdims=True)
    a_i, l_i = grid_of(8, LANES)
    AN[m] = jnp.where(a_i == 0, load, jnp.where(a_i == 1, prob, 0.0))
    sent_aux = exchange("aux_near", block, lambda k: (AN.at[m], AN.at[m]), AN.at[0 : NM - 1])
    d_i, q_i = grid_of(R, NB * J * CAP)
    combine = jnp.where(
        mod(div(q_i, CAP), J) == div(d_i, OWN), mm_nt(mixing, slot_of.astype(F32), HI), 0.0
    )
    loaded("gp", "up", "dn")

    arrive(sent)

    sideways = by_pieces("row", block, G4, 1)
    arrive(sent_aux)
    total = AN[0]
    for k in range(1, NM):
        total += AN[k]
    AF[b] = total
    sent_aux = exchange("aux_far", far, lambda k: (AF.at[b], AF.at[b]), AF.at[0 : NB - 1])
    arrive(sideways)

    squares = jnp.zeros((n.SLOTS, 1), F32)
    for k in range(X):
        source = G4[k].astype(F32).reshape(n.SLOTS * J, LANES).astype(BF16)
        by_pair = [
            mm(pick_row[...], source[at : at + pair * J]) for at in range(0, n.SLOTS * J, pair * J)
        ]
        for j in range(J):
            at = k * J + j
            part = jnp.concatenate([rows_k[j * pair : (j + 1) * pair] for rows_k in by_pair], axis=0)
            squares += jnp.sum(part * part, axis=1, keepdims=True)
            rows[:, at * LANES : (at + 1) * LANES] = part * mn_ref[at : at + 1, :]
    inv_rows = lax.rsqrt(squares / n.D + NORM_EPS)
    rn[...] = (rows[...] * inv_rows).astype(BF16)
    normed = rn[...]
    hidden = (silu(mm_nt(normed, held["gp"][0])) * mm_nt(normed, held["up"][0])).astype(BF16)

    def down_part(k):
        at = (x + k) % X
        columns = pl.ds(pl.multiple_of(at * n.Q, n.Q), n.Q)
        X5[at] = mm(hidden, held["dn"][0, :, columns]).astype(BF16)

    sent = exchange("out_state", side, lambda k: (X5.at[(x + k) % X], Y5.at[x]), Y5.at[0 : X - 1], down_part)
    down_part(0)
    Y5[x] = X5[x]
    arrive(sent)
    total = Y5[0].astype(F32)
    for k in range(1, X):
        total += Y5[k].astype(F32)
    N5[...] = total.reshape(NM, NB * CAP, n.Q).astype(BF16)
    R5[m] = N5[m]
    sent = exchange("out_near", block, lambda k: (N5.at[(m + k) % NM], R5.at[m]), R5.at[0 : NM - 1])
    arrive(sent)
    total = R5[0].astype(F32)
    for k in range(1, NM):
        total += R5[k].astype(F32)
    total = total.astype(BF16)
    r_i, c_i = grid_of(NB * J * CAP, NB * CAP)
    match = div(r_i, J * CAP) * CAP + mod(r_i, CAP) == c_i
    which = mod(div(r_i, CAP), J)
    spread = jnp.zeros((NB * J * CAP, LANES), F32)
    for j in range(J):
        spread += mm(ones_where(match & (which == j)), total[:, j * LANES : (j + 1) * LANES])
    F5[...] = spread.reshape(NB, J * CAP, LANES).astype(BF16)
    Q5[b] = F5[b]
    sent = exchange("out_far", far, lambda k: (F5.at[(b + k) % NB], Q5.at[b]), Q5.at[0 : NB - 1])
    arrive(sent_aux)
    total = AF[0]
    for k in range(1, NB):
        total += AF[k]
    share = total[0:1, :] / (T * TOPK) * (total[1:2, :] / T)
    loss = EXPERTS * jnp.sum(jnp.where(l_i[:1] < EXPERTS, share, 0.0), axis=1, keepdims=True)
    load_ref[...] = total[0:1, :EXPERTS]
    loss_ref[...] = loss
    arrive(sent)
    back = Q5[...].astype(F32).reshape(NB * J * CAP, LANES)
    lo_ref[...] = (resid + mm(combine, back, HI)).astype(BF16)
    for copy in pending:
        copy.wait()
    for k, copy in downs:
        pl.when((b > k) | (b == k if k == top else False))(copy.wait_send)
        if k < top:
            pl.when(b == 1)(onward[k - 1].wait_send)
    for k in range(1, NB - 1):
        pl.when((k <= b) & climbing)(ups[k].wait_send)
    pl.when(below)(ups[0].wait_send)
    pl.when(b == 0)(around_top.wait_send)
    for copy in descents:
        pl.when(b == top)(copy.wait_send)


def finish_kernel(*refs):
    count = len(refs) // 2
    copies = [
        pltpu.make_async_copy(refs[k], refs[count + k], refs[-1].at[k]) for k in range(count)
    ]
    for copy in copies:
        copy.start()
    for copy in copies:
        copy.wait()


class Sizes:
    pass


def per_device(
    head_count, state_count,
    tokens, mixer_norm, input_proj, conv_weight, conv_bias, conv_state, state_proj, step_gain, step_proj,
    step_bias, decay_log, skip_gain, ssm_state, output_proj, moe_norm, router_weight, expert_ids, slot_ids,
    gate_proj, up_proj, down_proj,
):
    n = Sizes()
    n.H, n.X, n.NB = head_count, state_count, EXPERTS
    n.NM = n.H // n.NB
    n.OWN, n.Q = tokens.shape
    n.J = n.Q // LANES
    n.R = n.OWN * n.J
    n.D = n.Q * n.X
    n.CONV = conv_weight.shape[0]
    _, n.T, n.C = conv_state.shape
    n.S = decay_log.shape[0]
    n.STATE = n.S * n.X
    n.RANK, n.PROJ = step_proj.shape[0], state_proj.shape[1]
    n.PW = -(-n.PROJ // LANES) * LANES
    n.TB = n.T // n.X // n.NM
    n.SLOTS = n.NM * n.NB * CAP
    n.FF = gate_proj.shape[2]

    tok = tokens.reshape(n.OWN, n.J, LANES).transpose(1, 0, 2).reshape(n.R, LANES)
    V = pltpu.VMEM
    operands = (
        mixer_norm.reshape(n.J, LANES), input_proj, conv_weight, conv_bias.reshape(1, -1), state_proj.T,
        step_gain.reshape(1, -1), step_proj, step_bias.reshape(1, -1), decay_log, skip_gain.reshape(1, -1),
        ssm_state, output_proj, moe_norm.reshape(-1, LANES), expert_ids.T, slot_ids.T,
        gate_proj.transpose(0, 2, 1), up_proj.transpose(0, 2, 1), down_proj,
    )
    vm = pl.BlockSpec(memory_space=pltpu.VMEM)
    hbm = pl.BlockSpec(memory_space=pltpu.HBM)
    wide = n.J * CAP
    scratch = [V(a.shape, a.dtype) for a in operands]
    scratch += [
        V(conv_state.shape[1:], F32), V((EXPERTS, n.Q), F32),
        V((n.NM * n.R, n.NM * n.R), BF16),
        V((2 * n.NB * wide, 2 * n.NB * wide), BF16),
        V((n.NM, n.NB, n.R, LANES), BF16),
        V((n.X, n.T, n.C), BF16), V((n.X, n.T, n.C), BF16),
        V((n.X, 8, n.T), F32),
        V((n.T, n.C), BF16),
        V((n.NM, n.TB, n.PW), F32), V((n.NM, n.TB, n.PW), F32),
        V((n.NB, n.TB, n.PW), BF16), V((n.X, n.NM, n.TB, n.PW), BF16),
        V((n.X, n.T, n.C), BF16),
        V((n.NM, n.NB * n.OWN, n.Q), BF16), V((n.NM, n.NB * n.OWN, n.Q), BF16),
        V((n.NB, n.R, LANES), BF16), V((n.NB, n.R, LANES), BF16),
        V((n.X, n.R, LANES), F32),
        V((n.NB, wide, LANES), BF16), V((n.X, n.NM, n.NB, wide, LANES), BF16),
        V((n.SLOTS, n.D), F32), V((n.SLOTS, n.D), BF16),
        V((n.X, n.SLOTS, n.Q), BF16), V((n.X, n.SLOTS, n.Q), BF16),
        V((n.NM, n.NB * CAP, n.Q), BF16), V((n.NM, n.NB * CAP, n.Q), BF16),
        V((n.NB, wide, LANES), BF16), V((n.NB, wide, LANES), BF16),
        V((n.NM, 8, LANES), F32), V((n.NB, 8, LANES), F32),
    ]
    dma, regular = pltpu.SemaphoreType.DMA, pltpu.SemaphoreType.REGULAR
    climb = dma((n.NB - 1,))
    scratch += [
        dma((len(STAGES),)), dma((len(STAGES),)), dma((2, n.NM - 1)), climb, climb, climb, climb, climb,
        dma((n.NB,)), regular, regular, regular, regular((n.NM - 1,)), dma((len(OPERANDS) + 4,)),
    ]
    shapes = (
        jax.ShapeDtypeStruct((n.R, LANES), BF16),
        jax.ShapeDtypeStruct(conv_state.shape, F32),
        jax.ShapeDtypeStruct(ssm_state.shape, F32),
        jax.ShapeDtypeStruct((1, EXPERTS), F32),
        jax.ShapeDtypeStruct((1, 1), F32),
    )
    results = pl.pallas_call(
        functools.partial(step_kernel, n),
        out_shape=shapes,
        in_specs=[hbm] * (len(operands) + 3),
        out_specs=(vm,) * len(shapes),
        scratch_shapes=scratch,
        compiler_params=pltpu.CompilerParams(
            collective_id=0, has_side_effects=True, vmem_limit_bytes=48 * 1024 * 1024
        ),
        name="mixer_moe_step",
    )(*[pltpu.with_memory_space_constraint(a, pltpu.HBM) for a in (tok, conv_state, router_weight.T, *operands)])
    out, new_conv, new_state, load, loss = pl.pallas_call(
        finish_kernel,
        out_shape=shapes,
        in_specs=[vm] * len(shapes),
        out_specs=(hbm,) * len(shapes),
        scratch_shapes=[dma((len(shapes),))],
        compiler_params=pltpu.CompilerParams(vmem_limit_bytes=1024 * 1024),
        name="finish",
    )(*results)
    layer_out = out.reshape(n.J, n.OWN, LANES).transpose(1, 0, 2).reshape(n.OWN, n.Q)
    return layer_out, new_conv, new_state, load.reshape(-1), loss.reshape(1)


def solution(mesh):
    in_specs = (
        P(("groups", "head"), "state"),
        P("state"),
        P(None, "state", "head"),
        P(None, "head"),
        P("head"),
        P(None, "groups", "head"),
        P("head", None),
        P(),
        P(None, "head"),
        P("head"),
        P("state", "head"),
        P("head"),
        P("state", "groups", "head"),
        P("head", "state"),
        P(),
        P(),
        P(("groups", "head"), None),
        P(("groups", "head"), None),
        P("head", None, "state"),
        P("head", None, "state"),
        P("head", "state", None),
    )
    out_specs = (
        P(("groups", "head"), "state"),
        P(None, "groups", "head"),
        P("state", "groups", "head"),
        P("groups"),
        P("groups"),
    )
    return jax.shard_map(
        functools.partial(per_device, mesh.shape["head"], mesh.shape["state"]),
        mesh=mesh, in_specs=in_specs, out_specs=out_specs, check_vma=False,
    )
```

```python
import functools

import jax
import jax.numpy as jnp
from jax import lax
from jax.experimental import pallas as pl
from jax.experimental.pallas import tpu as pltpu
from jax.sharding import PartitionSpec as P

EXPERTS = 8
TOPK = 2
CAP = 2
LANES = 128
NORM_EPS = 1e-05
STEP_EPS = 1e-06
MESH = pl.DeviceIdType.MESH
F32 = jnp.float32
BF16 = jnp.bfloat16
HI = lax.Precision.HIGHEST


def div(a, n):
    assert n & (n - 1) == 0
    return lax.shift_right_logical(a, jnp.int32(n.bit_length() - 1)) if n > 1 else a


def mod(a, n):
    assert n & (n - 1) == 0
    return a & (n - 1)


def grid_of(rows, cols):
    return (
        lax.broadcasted_iota(jnp.int32, (rows, cols), 0),
        lax.broadcasted_iota(jnp.int32, (rows, cols), 1),
    )


def ones_where(cond, dtype=BF16):
    return jnp.where(cond, 1.0, 0.0).astype(dtype)


def mm(a, b, precision=None):
    return jnp.dot(a, b, preferred_element_type=F32, precision=precision)


def mm_nt(a, b, precision=None):
    return lax.dot_general(
        a, b, (((1,), (1,)), ((), ())), preferred_element_type=F32, precision=precision
    )


def silu(v):
    return v * jax.nn.sigmoid(v)


def softplus(v):
    return jnp.maximum(v, 0.0) + jnp.log1p(jnp.exp(-jnp.abs(v)))


def by_distance(n):
    return sorted(range(1, n), key=lambda k: -min(k, n - k))


STAGES = (
    "tok_near", "tok_last", "branch", "gate", "square", "proj_near", "proj_far", "low_near", "low_state",
    "read", "mix_near", "mix_far", "stat", "row_far", "row_near", "row_state", "out_pair", "out_state", "out_near",
    "out_far", "aux_near", "aux_far",
)
OPERANDS = (
    "mixn", "win", "cw", "cb", "sp", "sg", "tp", "sb", "dl", "sk", "ssm", "op", "mn", "eid", "sid", "gp",
    "up", "dn",
)


def step_kernel(n, tok_hbm, cs_hbm, rw_hbm, *refs):
    count = len(OPERANDS)
    sources = refs[:count]
    lo_ref, nc_ref, ns_ref, load_ref, loss_ref = refs[count : count + 5]
    held = dict(zip(OPERANDS, refs[count + 5 : 2 * count + 5]))
    (
        cs, rw, pick, pick_row, G, XC, XG, XS, cob, P2, R2, F2, S2, XR, N3, R3, F3, Q3, ST, F4, G4, rows,
        rn, X5, W5, V5, Y5, N5, R5, F5, Q5, AN, AF, send_sem, recv_sem, piece_sem, up_send, up_recv, down_send,
        down_recv, onward_send, wrap_sem, ready_up, ready_wrap, ready_zero, ready_near, load_sem,
    ) = refs[2 * count + 5 :]
    head = lax.axis_index("head")
    x = lax.axis_index("state")
    b = head // n.NM
    m = head % n.NM
    X, NB, NM, OWN, J, R, T, C, S = n.X, n.NB, n.NM, n.OWN, n.J, n.R, n.T, n.C, n.S

    def offset(k):
        return k if 2 * k <= NM else k - NM

    far = {k: {"head": ((b + k) % NB) * NM + m} for k in range(1, NB)}
    near = {k: {"head": (head + n.H + offset(k)) % n.H} for k in range(1, NM)}
    block = {k: {"head": b * NM + (m + k) % NM} for k in range(1, NM)}
    side = {k: {"state": (x + k) % X} for k in range(1, X)}

    loads = {}

    def load(name, src, dst):
        loads[name] = pltpu.make_async_copy(src, dst, load_sem.at[len(loads)])
        loads[name].start()

    load("tok", tok_hbm, G.at[m, b])

    barrier = pltpu.get_barrier_semaphore()
    around = [(head + n.H + o) % n.H for o in range(-(NM // 2), NM // 2 + 1) if o]

    def greet(partner):
        pl.semaphore_signal(barrier, inc=1, device_id=partner, device_id_type=MESH)

    for k in side:
        greet(side[k])
    for other in around:
        pl.when(other > head)(functools.partial(greet, {"head": other}))
    top = NB - 1
    for k in range(1, NB - 1):
        pl.when((b > 0) & (b + k < NB))(functools.partial(greet, {"head": (b + k) * NM + m}))
    pl.when(b == 0)(functools.partial(greet, {"head": top * NM + m}))
    pl.when(b == 1)(functools.partial(greet, {"head": m}))
    expected = (X - 1) + jnp.where(b == 0, 1, b - 1) + jnp.where(b == top, 1, 0)
    for other in around:
        expected += jnp.where(other < head, 1, 0)

    for name, src in zip(OPERANDS, sources):
        load(name, src, held[name])
    load("conv", cs_hbm.at[0], cs)
    load("keep", cs_hbm.at[1 : n.CONV - 1], nc_ref.at[0 : n.CONV - 2])
    load("router", rw_hbm.at[:, pl.ds(pl.multiple_of(x * n.Q, n.Q), n.Q)], rw)
    mixn_ref, win, cw_ref, cb_ref = held["mixn"], held["win"], held["cw"], held["cb"]
    sp, sg_ref, tp, sb_ref, dl_ref = held["sp"], held["sg"], held["tp"], held["sb"], held["dl"]
    sk_ref, ssm, op, mn_ref = held["sk"], held["ssm"], held["op"], held["mn"]

    def loaded(*names):
        for name in names:
            loads[name].wait()

    pending = []

    def remote(src, dst, send, recv, partner):
        return pltpu.make_async_remote_copy(
            src_ref=src, dst_ref=dst, send_sem=send, recv_sem=recv, device_id=partner, device_id_type=MESH
        )

    def exchange(stage, group, pair, landing, first=None):
        at = STAGES.index(stage)
        for k in by_distance(len(group) + 1):
            if first is not None:
                first(k)
            src, dst = pair(k)
            remote(src, dst, send_sem.at[at], recv_sem.at[at], group[k]).start()
        pending.append(pltpu.make_async_copy(landing, landing, send_sem.at[at]))
        return pltpu.make_async_copy(landing, landing, recv_sem.at[at])

    def arrive(copy):
        copy.wait()

    def by_pieces(name, group, ref, at):
        near_at, side_at = STAGES.index(name + "_near"), STAGES.index(name + "_state")
        sent = {}
        order = by_distance(NM)
        for k in order:
            sent[k] = remote(
                ref.at[x, m], ref.at[x, m], send_sem.at[near_at], piece_sem.at[at, k - 1], group[k]
            )
            sent[k].start()
        for step in [0] + order[::-1]:
            piece = (m + NM - step) % NM
            if step:
                sent[step].wait_recv()
            for k in by_distance(X):
                remote(
                    ref.at[x, piece], ref.at[x, piece], send_sem.at[side_at], recv_sem.at[side_at], side[k]
                ).start()
        landing = ref.at[0, 0 : NM - 1]
        pending.append(pltpu.make_async_copy(landing, landing, send_sem.at[near_at]))
        landing = ref.at[0 : X - 1]
        pending.append(pltpu.make_async_copy(landing, landing, send_sem.at[side_at]))
        return pltpu.make_async_copy(landing, landing, recv_sem.at[side_at])

    loaded("tok")
    pl.semaphore_wait(barrier, expected)

    @pl.when(b > 1)
    def _():
        pl.semaphore_signal(ready_up, inc=1, device_id={"head": head - NM}, device_id_type=MESH)

    @pl.when(b == 0)
    def _():
        pl.semaphore_signal(ready_zero, inc=1, device_id={"head": head + NM}, device_id_type=MESH)

    for k in near:
        source = (head + n.H - offset(k)) % n.H

        @pl.when(source < head)
        def _(k=k, source=source):
            pl.semaphore_signal(
                ready_near.at[k - 1], inc=1, device_id={"head": source}, device_id_type=MESH
            )

    own = G.at[m, b]
    downs = []
    for k in by_distance(NB):
        copy = remote(own, own, down_send.at[k - 1], down_recv.at[k - 1], {"head": head - k * NM})
        pl.when((b > k) | (b == k if k == top else False))(copy.start)
        downs.append((k, copy))
    climbing = b < NB - 1
    ups = [
        remote(G.at[m, k], G.at[m, k], up_send.at[k], up_recv.at[k], {"head": head + NM})
        for k in range(NB - 1)
    ]

    @pl.when((b > 0) & climbing)
    def _():
        pl.semaphore_wait(ready_up, 1)

    around_top = remote(G.at[m, 0], G.at[m, 0], wrap_sem.at[1], wrap_sem.at[0], {"head": top * NM + m})
    descents = [
        remote(G.at[m, 0], G.at[m, 0], wrap_sem.at[1 + k], wrap_sem.at[0], {"head": head - k * NM})
        for k in range(1, top - NB // 2)
    ]
    below = b < NB // 2

    @pl.when(b == top)
    def _():
        pl.semaphore_signal(ready_wrap, inc=1, device_id={"head": m}, device_id_type=MESH)
        around_top.wait_recv()
        for copy in descents:
            copy.start()

    for k in range(NB - 2, 0, -1):
        pl.when(k < b)(ups[k].wait_recv)
        pl.when((k <= b) & climbing)(ups[k].start)
    pl.when((b > 0) & (b <= NB // 2))(ups[0].wait_recv)
    pl.when(below)(ups[0].start)

    @pl.when(b == 0)
    def _():
        pl.semaphore_wait(ready_wrap, 1)
        around_top.start()

    @pl.when((b > NB // 2) & (b < top))
    def _():
        around_top.wait_recv()

    onward = [
        remote(G.at[m, k], G.at[m, k], onward_send.at[k - 1], down_recv.at[k - 1], {"head": head - NM})
        for k in range(1, top)
    ]

    def from_above(last):
        for k, copy in sorted(downs, key=lambda t: t[0]):
            pl.when((b + k == NB - 1) if last else (b + k < NB - 1))(copy.wait_recv)
            if not last and k < top - 1:
                pl.when(b == 1)(onward[k].start)

    @pl.when(b == 1)
    def _():
        pl.semaphore_wait(ready_zero, 1)
        onward[0].start()

    def near_ready(k):
        target = (head + n.H + offset(k)) % n.H

        @pl.when(target > head)
        def _():
            pl.semaphore_wait(ready_near.at[k - 1], 1)

    from_above(False)
    early = G.at[m, 0 : NB - 1]
    sent_early = exchange(
        "tok_near", near, lambda k: (early, early), G.at[0 : NM - 1, 0 : NB - 1], near_ready
    )
    tok_bf = G[m, b]

    per = NM * OWN
    r_i, c_i = grid_of(NM * R, NM * R)
    pick[...] = ones_where(
        (mod(div(c_i, OWN), J) == div(r_i, per)) & (div(c_i, R) * OWN + mod(c_i, OWN) == mod(r_i, per))
    )
    pair = 2 * NB * CAP
    r_i, c_i = grid_of(pair * J, pair * J)
    pick_row[...] = ones_where(
        (mod(div(c_i, CAP), J) == div(r_i, pair))
        & (div(c_i, J * CAP) * CAP + mod(c_i, CAP) == mod(r_i, pair))
    )

    from_above(True)
    final = G.at[m, NB - 1]
    sent = exchange("tok_last", near, lambda k: (final, final), G.at[0, 0 : NM - 1])
    loaded("win", "mixn")
    arrive(sent_early)
    arrive(sent)

    by_block = [mm(pick[...], G[:, k].reshape(NM * R, LANES)) for k in range(NB)]
    conv_part = jnp.zeros((T, C), F32)
    gate_part = jnp.zeros((T, C), F32)
    squares = jnp.zeros((T, 1), F32)
    for j in range(J):
        tok_j = jnp.concatenate([rows_k[j * per : (j + 1) * per] for rows_k in by_block], axis=0)
        squares += jnp.sum(tok_j * tok_j, axis=1, keepdims=True)
        wide = tok_j * mixn_ref[j : j + 1, :]
        high = wide.astype(BF16)
        for half in (high, (wide - high.astype(F32)).astype(BF16)):
            conv_part += mm(half, win[0, j * LANES : (j + 1) * LANES, :])
            gate_part += mm(half, win[1, j * LANES : (j + 1) * LANES, :])
    XS[x] = jnp.broadcast_to(squares, (T, LANES)).T[:8, :]
    XC[x] = conv_part.astype(BF16)
    sent_sq = exchange("square", side, lambda k: (XS.at[x], XS.at[x]), XS.at[0 : X - 1])
    sent = exchange("branch", side, lambda k: (XC.at[x], XC.at[x]), XC.at[0 : X - 1])
    XG[x] = gate_part.astype(BF16)
    sent_gate = exchange("gate", side, lambda k: (XG.at[x], XG.at[x]), XG.at[0 : X - 1])

    loaded("conv", "keep", "cw", "cb", "sp")
    window = cb_ref[...] + cw_ref[0:1, :] * cs[...]
    for k in range(n.CONV - 2):
        window += cw_ref[k + 1 : k + 2, :] * nc_ref[k]
    P2[...] = jnp.zeros_like(P2)
    arrive(sent_sq)
    total = XS[0]
    for k in range(1, X):
        total += XS[k]
    inv_first = lax.rsqrt(jnp.broadcast_to(total[:1, :], (LANES, T)).T[:, :1] / n.D + NORM_EPS)
    arrive(sent)
    conv_in = XC[0].astype(F32)
    for k in range(1, X):
        conv_in += XC[k].astype(F32)
    conv_in = conv_in * inv_first
    nc_ref[n.CONV - 2] = conv_in
    conv_out = silu(window + cw_ref[n.CONV - 1 : n.CONV, :] * conv_in)
    cob[...] = conv_out.astype(BF16)

    quarter = T // X
    spare = n.PROJ - n.RANK

    def in_halves(wide):
        low, vectors = wide[:, : n.RANK], wide[:, n.RANK :]
        high = vectors.astype(BF16).astype(F32)
        rest = pltpu.roll(vectors - high, spare, 1)
        return jnp.concatenate([low, high + rest], axis=1).astype(BF16)

    part = mm_nt(cob[pl.ds(pl.multiple_of(x * quarter, quarter), quarter), :], sp[...])
    P2[:, :, : n.PROJ] = part.reshape(NM, n.TB, n.PROJ)
    R2[m] = P2[m]
    sent = exchange("proj_near", near, lambda k: (P2.at[(m + k) % NM], R2.at[m]), R2.at[0 : NM - 1])
    arrive(sent)
    total = R2[0]
    for k in range(1, NM):
        total += R2[k]
    F2[b] = in_halves(total)
    sent = exchange("proj_far", far, lambda k: (F2.at[b], F2.at[b]), F2.at[0 : NB - 1])
    loaded("tp", "ssm", "sg", "sb", "dl")
    arrive(sent)
    total = F2[0].astype(F32)
    for k in range(1, NB):
        total += F2[k].astype(F32)
    low, vectors = total[:, : n.RANK], total[:, n.RANK :]
    step_inv = lax.rsqrt(jnp.mean(low * low, axis=1, keepdims=True) + STEP_EPS)
    vectors = vectors + pltpu.roll(vectors, LANES - spare, 1)
    _, l_i = grid_of(n.TB, LANES)
    vectors = jnp.where(l_i < spare, vectors, 0.0)
    S2[x, m] = in_halves(jnp.concatenate([low * step_inv * sg_ref[...], vectors], axis=1))
    sent = by_pieces("low", near, S2, 0)
    arrive(sent_gate)
    gate = gate_part
    for k in range(1, X):
        gate += XG[(x + k) % X].astype(F32)
    gate = silu(gate * inv_first)
    rates = [jnp.exp(dl_ref[k : k + 1, :]) for k in range(S)]
    arrive(sent)

    projected = S2[...].astype(F32).reshape(T, n.PW)
    step_normed = projected[:, : n.RANK].astype(BF16)
    step_size = softplus(mm(step_normed, tp[...]) + sb_ref[...])
    vectors = projected[:, n.RANK :].astype(BF16)
    rows_i, _ = grid_of(LANES, C)
    driven = step_size * conv_out
    read = jnp.zeros((T, C), F32)
    for k in range(S):
        at = x * S + k
        b_in = mm(vectors, ones_where((rows_i == at) | (rows_i == spare + at)))
        at = at + n.STATE
        c_out = mm(vectors, ones_where((rows_i == at) | (rows_i == spare + at)))
        fresh = jnp.exp(-step_size * rates[k]) * ssm[k] + driven * b_in
        ns_ref[k] = fresh
        read += c_out * fresh
    XR[x] = read.astype(BF16)
    sent = exchange("read", side, lambda k: (XR.at[x], XR.at[x]), XR.at[0 : X - 1])
    loaded("op", "sk")
    r_i, c_i = grid_of(T, T)
    source = (div(mod(r_i, NB * OWN), OWN) * NM + div(r_i, NB * OWN)) * OWN + mod(r_i, OWN)
    by_member = ones_where(source == c_i)
    arrive(sent)
    for k in range(1, X):
        read += XR[(x + k) % X].astype(F32)
    act = ((read + sk_ref[...] * conv_out) * gate).astype(BF16)
    act = mm(by_member, act).astype(BF16)
    N3[...] = mm(act, op[...]).astype(BF16).reshape(NM, NB * OWN, n.Q)
    R3[m] = N3[m]
    sent = exchange("mix_near", near, lambda k: (N3.at[(m + k) % NM], R3.at[m]), R3.at[0 : NM - 1])
    arrive(sent)
    total = R3[0].astype(F32)
    for k in range(1, NM):
        total += R3[k].astype(F32)
    total = total.astype(BF16)
    r_i, c_i = grid_of(NB * R, NB * OWN)
    match = div(r_i, R) * OWN + mod(r_i, OWN) == c_i
    which = mod(div(r_i, OWN), J)
    spread = jnp.zeros((NB * R, LANES), F32)
    for j in range(J):
        spread += mm(ones_where(match & (which == j)), total[:, j * LANES : (j + 1) * LANES])
    F3[...] = spread.astype(BF16).reshape(NB, R, LANES)
    Q3[b] = F3[b]
    sent = exchange("mix_far", far, lambda k: (F3.at[(b + k) % NB], Q3.at[b]), Q3.at[0 : NB - 1])
    loaded("router", "mn", "eid", "sid")
    arrive(sent)
    total = Q3[0].astype(F32)
    for k in range(1, NB):
        total += Q3[k].astype(F32)

    resid_bf = (tok_bf.astype(F32) + total).astype(BF16)
    resid = resid_bf.astype(F32)
    row_i, lane_i = grid_of(R, LANES)
    hits, kept, slots = [], [], []
    i_i, t_i = grid_of(R, OWN)

    def by_row(ref, k):
        wide = jnp.broadcast_to(ref[k : k + 1, :], (R, OWN)).astype(F32)
        return jnp.sum(jnp.where(mod(i_i, OWN) == t_i, wide, 0.0), axis=1, keepdims=True).astype(jnp.int32)

    for k in range(TOPK):
        e_k, s_k = by_row(held["eid"], k), by_row(held["sid"], k)
        keep = s_k < CAP
        hits.append(lane_i == e_k)
        kept.append(keep)
        slots.append((lane_i == e_k * CAP + s_k) & keep)
    dispatch = sum(ones_where(s, F32) for s in slots).astype(BF16)
    d_i, q_i = grid_of(NB * J * CAP, LANES)
    slot_of = ones_where(q_i == div(d_i, J * CAP) * CAP + mod(d_i, CAP))
    d_i, c_i = grid_of(NB * J * CAP, R)
    chosen_rows = jnp.where(
        mod(div(d_i, CAP), J) == div(c_i, OWN), mm_nt(slot_of, dispatch), 0.0
    ).astype(BF16)
    F4[...] = mm(chosen_rows, resid_bf).reshape(NB, J * CAP, LANES).astype(BF16)
    G4[x, m, b] = F4[b]
    sent = exchange(
        "row_far", far, lambda k: (F4.at[(b + k) % NB], G4.at[x, m, b]), G4.at[x, m, 0 : NB - 1]
    )

    gain = jnp.zeros((R, LANES), F32)
    for j in range(J):
        gain = jnp.where(div(row_i, OWN) == j, mn_ref[pl.ds(x * J + j, 1), :], gain)
    scaled = resid * gain
    raw = jnp.zeros((R, EXPERTS), F32)
    for j in range(J):
        raw += mm_nt(
            jnp.where(div(row_i, OWN) == j, scaled, 0.0), rw[:, j * LANES : (j + 1) * LANES], HI
        )
    ST[x] = jnp.broadcast_to(jnp.sum(resid * resid, axis=1, keepdims=True), (R, LANES))
    ST[x, :, :EXPERTS] = raw
    sent_stat = exchange("stat", side, lambda k: (ST.at[x], ST.at[x]), ST.at[0 : X - 1])
    arrive(sent_stat)
    total = ST[0]
    for k in range(1, X):
        total += ST[k]
    r_i, c_i = grid_of(R, R)
    total = mm(ones_where(mod(r_i, OWN) == mod(c_i, OWN), F32), total, HI)
    inv_second = lax.rsqrt(total[:, EXPERTS : EXPERTS + 1] / n.D + NORM_EPS)
    logits = inv_second * total
    chosen = [jnp.sum(jnp.where(hit, logits, 0.0), axis=1, keepdims=True) for hit in hits]
    mixing = jnp.zeros((R, LANES), F32)
    for k in range(TOPK):
        weight = jax.nn.sigmoid(chosen[k] - chosen[1 - k])
        mixing += jnp.where(slots[k], weight, 0.0)
    first = row_i < OWN
    load = sum(ones_where(hits[k] & kept[k] & first, F32) for k in range(TOPK))
    load = jnp.sum(load, axis=0, keepdims=True)
    prob = jnp.where(first & (lane_i < EXPERTS), jax.nn.sigmoid(logits), 0.0)
    prob = jnp.sum(prob, axis=0, keepdims=True)
    a_i, l_i = grid_of(8, LANES)
    AN[m] = jnp.where(a_i == 0, load, jnp.where(a_i == 1, prob, 0.0))
    sent_aux = exchange("aux_near", block, lambda k: (AN.at[m], AN.at[m]), AN.at[0 : NM - 1])
    d_i, q_i = grid_of(R, NB * J * CAP)
    combine = jnp.where(
        mod(div(q_i, CAP), J) == div(d_i, OWN), mm_nt(mixing, slot_of.astype(F32), HI), 0.0
    )
    loaded("gp", "up", "dn")

    arrive(sent)

    sideways = by_pieces("row", block, G4, 1)
    arrive(sent_aux)
    total = AN[0]
    for k in range(1, NM):
        total += AN[k]
    AF[b] = total
    sent_aux = exchange("aux_far", far, lambda k: (AF.at[b], AF.at[b]), AF.at[0 : NB - 1])
    arrive(sideways)

    squares = jnp.zeros((n.SLOTS, 1), F32)
    for k in range(X):
        source = G4[k].astype(F32).reshape(n.SLOTS * J, LANES).astype(BF16)
        by_pair = [
            mm(pick_row[...], source[at : at + pair * J]) for at in range(0, n.SLOTS * J, pair * J)
        ]
        for j in range(J):
            at = k * J + j
            starts = [j * pair + c * NB * CAP for c in range(2)]
            part = jnp.concatenate(
                [rows_k[start : start + NB * CAP] for start in starts for rows_k in by_pair], axis=0
            )
            squares += jnp.sum(part * part, axis=1, keepdims=True)
            rows[:, at * LANES : (at + 1) * LANES] = part * mn_ref[at : at + 1, :]
    inv_rows = lax.rsqrt(squares / n.D + NORM_EPS)
    rn[...] = (rows[...] * inv_rows).astype(BF16)
    normed = rn[...]
    hidden = (silu(mm_nt(normed, held["gp"][0])) * mm_nt(normed, held["up"][0])).astype(BF16)

    core, half = m % 2, n.SLOTS // 2
    pair_at = STAGES.index("out_pair")
    for k in by_distance(X) + [0]:
        at = (x + k) % X
        columns = pl.ds(pl.multiple_of(at * n.Q, n.Q), n.Q)
        X5[at] = mm(hidden, held["dn"][0, :, columns]).astype(BF16).reshape(2, half, n.Q)
        remote(
            X5.at[at, 1 - core], W5.at[at], send_sem.at[pair_at], recv_sem.at[pair_at],
            {"head": head + 1 - 2 * core},
        ).start()
    pending.append(pltpu.make_async_copy(W5, W5, send_sem.at[pair_at]))
    arrive(pltpu.make_async_copy(W5, W5, recv_sem.at[pair_at]))

    def both(k):
        at = (x + k) % X
        V5[at] = (X5[at, core].astype(F32) + W5[at].astype(F32)).astype(BF16)

    sent = exchange("out_state", side, lambda k: (V5.at[(x + k) % X], Y5.at[x]), Y5.at[0 : X - 1], both)
    both(0)
    Y5[x] = V5[x]
    arrive(sent)
    total = Y5[0].astype(F32)
    for k in range(1, X):
        total += Y5[k].astype(F32)
    chips, chip = NM // 2, m // 2
    N5[...] = total.astype(BF16).reshape(chips, NB * CAP, n.Q)
    R5[chip] = N5[chip]
    if chips > 1:
        alike = {k: {"head": b * NM + (chip + k) % chips * 2 + core} for k in range(1, chips)}
        sent = exchange(
            "out_near", alike, lambda k: (N5.at[(chip + k) % chips], R5.at[chip]), R5.at[0 : chips - 1]
        )
        arrive(sent)
    total = R5[0].astype(F32)
    for k in range(1, chips):
        total += R5[k].astype(F32)
    total = total.astype(BF16)
    r_i, c_i = grid_of(NB * J * CAP, NB * CAP)
    match = div(r_i, J * CAP) * CAP + mod(r_i, CAP) == c_i
    which = mod(div(r_i, CAP), J)
    spread = jnp.zeros((NB * J * CAP, LANES), F32)
    for j in range(J):
        spread += mm(ones_where(match & (which == j)), total[:, j * LANES : (j + 1) * LANES])
    F5[...] = spread.reshape(NB, J * CAP, LANES).astype(BF16)
    Q5[b] = F5[b]
    sent = exchange("out_far", far, lambda k: (F5.at[(b + k) % NB], Q5.at[b]), Q5.at[0 : NB - 1])
    arrive(sent_aux)
    total = AF[0]
    for k in range(1, NB):
        total += AF[k]
    share = total[0:1, :] / (T * TOPK) * (total[1:2, :] / T)
    loss = EXPERTS * jnp.sum(jnp.where(l_i[:1] < EXPERTS, share, 0.0), axis=1, keepdims=True)
    load_ref[...] = total[0:1, :EXPERTS]
    loss_ref[...] = loss
    arrive(sent)
    back = Q5[...].astype(F32).reshape(NB * J * CAP, LANES)
    lo_ref[...] = (resid + mm(combine, back, HI)).astype(BF16)
    for copy in pending:
        copy.wait()
    for k, copy in downs:
        pl.when((b > k) | (b == k if k == top else False))(copy.wait_send)
        if k < top:
            pl.when(b == 1)(onward[k - 1].wait_send)
    for k in range(1, NB - 1):
        pl.when((k <= b) & climbing)(ups[k].wait_send)
    pl.when(below)(ups[0].wait_send)
    pl.when(b == 0)(around_top.wait_send)
    for copy in descents:
        pl.when(b == top)(copy.wait_send)


def finish_kernel(*refs):
    count = len(refs) // 2
    copies = [
        pltpu.make_async_copy(refs[k], refs[count + k], refs[-1].at[k]) for k in range(count)
    ]
    for copy in copies:
        copy.start()
    for copy in copies:
        copy.wait()


class Sizes:
    pass


def per_device(
    head_count, state_count,
    tokens, mixer_norm, input_proj, conv_weight, conv_bias, conv_state, state_proj, step_gain, step_proj,
    step_bias, decay_log, skip_gain, ssm_state, output_proj, moe_norm, router_weight, expert_ids, slot_ids,
    gate_proj, up_proj, down_proj,
):
    n = Sizes()
    n.H, n.X, n.NB = head_count, state_count, EXPERTS
    n.NM = n.H // n.NB
    n.OWN, n.Q = tokens.shape
    n.J = n.Q // LANES
    n.R = n.OWN * n.J
    n.D = n.Q * n.X
    n.CONV = conv_weight.shape[0]
    _, n.T, n.C = conv_state.shape
    n.S = decay_log.shape[0]
    n.STATE = n.S * n.X
    n.RANK, n.PROJ = step_proj.shape[0], state_proj.shape[1]
    n.PW = -(-n.PROJ // LANES) * LANES
    n.TB = n.T // n.X // n.NM
    n.SLOTS = n.NM * n.NB * CAP
    n.FF = gate_proj.shape[2]

    tok = tokens.reshape(n.OWN, n.J, LANES).transpose(1, 0, 2).reshape(n.R, LANES)
    V = pltpu.VMEM
    operands = (
        mixer_norm.reshape(n.J, LANES), input_proj, conv_weight, conv_bias.reshape(1, -1), state_proj.T,
        step_gain.reshape(1, -1), step_proj, step_bias.reshape(1, -1), decay_log, skip_gain.reshape(1, -1),
        ssm_state, output_proj, moe_norm.reshape(-1, LANES), expert_ids.T, slot_ids.T,
        gate_proj.transpose(0, 2, 1), up_proj.transpose(0, 2, 1), down_proj,
    )
    vm = pl.BlockSpec(memory_space=pltpu.VMEM)
    hbm = pl.BlockSpec(memory_space=pltpu.HBM)
    wide = n.J * CAP
    scratch = [V(a.shape, a.dtype) for a in operands]
    scratch += [
        V(conv_state.shape[1:], F32), V((EXPERTS, n.Q), F32),
        V((n.NM * n.R, n.NM * n.R), BF16),
        V((2 * n.NB * wide, 2 * n.NB * wide), BF16),
        V((n.NM, n.NB, n.R, LANES), BF16),
        V((n.X, n.T, n.C), BF16), V((n.X, n.T, n.C), BF16),
        V((n.X, 8, n.T), F32),
        V((n.T, n.C), BF16),
        V((n.NM, n.TB, n.PW), F32), V((n.NM, n.TB, n.PW), F32),
        V((n.NB, n.TB, n.PW), BF16), V((n.X, n.NM, n.TB, n.PW), BF16),
        V((n.X, n.T, n.C), BF16),
        V((n.NM, n.NB * n.OWN, n.Q), BF16), V((n.NM, n.NB * n.OWN, n.Q), BF16),
        V((n.NB, n.R, LANES), BF16), V((n.NB, n.R, LANES), BF16),
        V((n.X, n.R, LANES), F32),
        V((n.NB, wide, LANES), BF16), V((n.X, n.NM, n.NB, wide, LANES), BF16),
        V((n.SLOTS, n.D), F32), V((n.SLOTS, n.D), BF16),
        V((n.X, 2, n.SLOTS // 2, n.Q), BF16), V((n.X, n.SLOTS // 2, n.Q), BF16),
        V((n.X, n.SLOTS // 2, n.Q), BF16), V((n.X, n.SLOTS // 2, n.Q), BF16),
        V((n.NM // 2, n.NB * CAP, n.Q), BF16), V((n.NM // 2, n.NB * CAP, n.Q), BF16),
        V((n.NB, wide, LANES), BF16), V((n.NB, wide, LANES), BF16),
        V((n.NM, 8, LANES), F32), V((n.NB, 8, LANES), F32),
    ]
    dma, regular = pltpu.SemaphoreType.DMA, pltpu.SemaphoreType.REGULAR
    climb = dma((n.NB - 1,))
    scratch += [
        dma((len(STAGES),)), dma((len(STAGES),)), dma((2, n.NM - 1)), climb, climb, climb, climb, climb,
        dma((n.NB,)), regular, regular, regular, regular((n.NM - 1,)), dma((len(OPERANDS) + 4,)),
    ]
    shapes = (
        jax.ShapeDtypeStruct((n.R, LANES), BF16),
        jax.ShapeDtypeStruct(conv_state.shape, F32),
        jax.ShapeDtypeStruct(ssm_state.shape, F32),
        jax.ShapeDtypeStruct((1, EXPERTS), F32),
        jax.ShapeDtypeStruct((1, 1), F32),
    )
    results = pl.pallas_call(
        functools.partial(step_kernel, n),
        out_shape=shapes,
        in_specs=[hbm] * (len(operands) + 3),
        out_specs=(vm,) * len(shapes),
        scratch_shapes=scratch,
        compiler_params=pltpu.CompilerParams(
            collective_id=0, has_side_effects=True, vmem_limit_bytes=48 * 1024 * 1024
        ),
        name="mixer_moe_step",
    )(*[pltpu.with_memory_space_constraint(a, pltpu.HBM) for a in (tok, conv_state, router_weight.T, *operands)])
    out, new_conv, new_state, load, loss = pl.pallas_call(
        finish_kernel,
        out_shape=shapes,
        in_specs=[vm] * len(shapes),
        out_specs=(hbm,) * len(shapes),
        scratch_shapes=[dma((len(shapes),))],
        compiler_params=pltpu.CompilerParams(vmem_limit_bytes=1024 * 1024),
        name="finish",
    )(*results)
    layer_out = out.reshape(n.J, n.OWN, LANES).transpose(1, 0, 2).reshape(n.OWN, n.Q)
    return layer_out, new_conv, new_state, load.reshape(-1), loss.reshape(1)


def solution(mesh):
    in_specs = (
        P(("groups", "head"), "state"),
        P("state"),
        P(None, "state", "head"),
        P(None, "head"),
        P("head"),
        P(None, "groups", "head"),
        P("head", None),
        P(),
        P(None, "head"),
        P("head"),
        P("state", "head"),
        P("head"),
        P("state", "groups", "head"),
        P("head", "state"),
        P(),
        P(),
        P(("groups", "head"), None),
        P(("groups", "head"), None),
        P("head", None, "state"),
        P("head", None, "state"),
        P("head", "state", None),
    )
    out_specs = (
        P(("groups", "head"), "state"),
        P(None, "groups", "head"),
        P("state", "groups", "head"),
        P("groups"),
        P("groups"),
    )
    return jax.shard_map(
        functools.partial(per_device, mesh.shape["head"], mesh.shape["state"]),
        mesh=mesh, in_specs=in_specs, out_specs=out_specs, check_vma=False,
    )
```

```python
import functools

import jax
import jax.numpy as jnp
from jax import lax
from jax.experimental import pallas as pl
from jax.experimental.pallas import tpu as pltpu
from jax.sharding import PartitionSpec as P

EXPERTS = 8
TOPK = 2
CAP = 2
LANES = 128
NORM_EPS = 1e-05
STEP_EPS = 1e-06
MESH = pl.DeviceIdType.MESH
F32 = jnp.float32
BF16 = jnp.bfloat16
HI = lax.Precision.HIGHEST


def div(a, n):
    assert n & (n - 1) == 0
    return lax.shift_right_logical(a, jnp.int32(n.bit_length() - 1)) if n > 1 else a


def mod(a, n):
    assert n & (n - 1) == 0
    return a & (n - 1)


def grid_of(rows, cols):
    return (
        lax.broadcasted_iota(jnp.int32, (rows, cols), 0),
        lax.broadcasted_iota(jnp.int32, (rows, cols), 1),
    )


def ones_where(cond, dtype=BF16):
    return jnp.where(cond, 1.0, 0.0).astype(dtype)


def mm(a, b, precision=None):
    return jnp.dot(a, b, preferred_element_type=F32, precision=precision)


def mm_nt(a, b, precision=None):
    return lax.dot_general(
        a, b, (((1,), (1,)), ((), ())), preferred_element_type=F32, precision=precision
    )


def silu(v):
    return v * jax.nn.sigmoid(v)


def softplus(v):
    return jnp.maximum(v, 0.0) + jnp.log1p(jnp.exp(-jnp.abs(v)))


def by_distance(n):
    return sorted(range(1, n), key=lambda k: -min(k, n - k))


STAGES = (
    "tok_near", "tok_last", "branch", "gate", "square", "proj_near", "proj_far", "low_near", "low_state",
    "read", "mix_near", "mix_far", "stat", "row_far", "row_near", "row_state", "row_pair", "out_pair", "out_state", "out_near",
    "out_far", "aux_near", "aux_far",
)
OPERANDS = (
    "mixn", "win", "cw", "cb", "sp", "sg", "tp", "sb", "dl", "sk", "ssm", "op", "mn", "eid", "sid", "gp",
    "up", "dn",
)


def step_kernel(n, tok_hbm, cs_hbm, rw_hbm, *refs):
    count = len(OPERANDS)
    sources = refs[:count]
    lo_ref, nc_ref, ns_ref, load_ref, loss_ref = refs[count : count + 5]
    held = dict(zip(OPERANDS, refs[count + 5 : 2 * count + 5]))
    (
        cs, rw, pick, pick_row, G, XC, XG, XS, cob, P2, R2, F2, S2, XR, N3, R3, F3, Q3, ST, F4, G4, rows,
        rn, X5, W5, V5, Y5, N5, R5, F5, Q5, AN, AF, send_sem, recv_sem, piece_sem, up_send, up_recv, down_send,
        down_recv, onward_send, wrap_sem, ready_up, ready_wrap, ready_zero, ready_near, load_sem,
    ) = refs[2 * count + 5 :]
    head = lax.axis_index("head")
    x = lax.axis_index("state")
    b = head // n.NM
    m = head % n.NM
    X, NB, NM, OWN, J, R, T, C, S = n.X, n.NB, n.NM, n.OWN, n.J, n.R, n.T, n.C, n.S

    def offset(k):
        return k if 2 * k <= NM else k - NM

    far = {k: {"head": ((b + k) % NB) * NM + m} for k in range(1, NB)}
    near = {k: {"head": (head + n.H + offset(k)) % n.H} for k in range(1, NM)}
    block = {k: {"head": b * NM + (m + k) % NM} for k in range(1, NM)}
    side = {k: {"state": (x + k) % X} for k in range(1, X)}

    loads = {}

    def load(name, src, dst):
        loads[name] = pltpu.make_async_copy(src, dst, load_sem.at[len(loads)])
        loads[name].start()

    load("tok", tok_hbm, G.at[m, b])

    barrier = pltpu.get_barrier_semaphore()
    around = [(head + n.H + o) % n.H for o in range(-(NM // 2), NM // 2 + 1) if o]

    def greet(partner):
        pl.semaphore_signal(barrier, inc=1, device_id=partner, device_id_type=MESH)

    for k in side:
        greet(side[k])
    for other in around:
        pl.when(other > head)(functools.partial(greet, {"head": other}))
    top = NB - 1
    for k in range(1, NB - 1):
        pl.when((b > 0) & (b + k < NB))(functools.partial(greet, {"head": (b + k) * NM + m}))
    pl.when(b == 0)(functools.partial(greet, {"head": top * NM + m}))
    pl.when(b == 1)(functools.partial(greet, {"head": m}))
    expected = (X - 1) + jnp.where(b == 0, 1, b - 1) + jnp.where(b == top, 1, 0)
    for other in around:
        expected += jnp.where(other < head, 1, 0)

    for name, src in zip(OPERANDS, sources):
        load(name, src, held[name])
    load("conv", cs_hbm.at[0], cs)
    load("keep", cs_hbm.at[1 : n.CONV - 1], nc_ref.at[0 : n.CONV - 2])
    load("router", rw_hbm.at[:, pl.ds(pl.multiple_of(x * n.Q, n.Q), n.Q)], rw)
    mixn_ref, win, cw_ref, cb_ref = held["mixn"], held["win"], held["cw"], held["cb"]
    sp, sg_ref, tp, sb_ref, dl_ref = held["sp"], held["sg"], held["tp"], held["sb"], held["dl"]
    sk_ref, ssm, op, mn_ref = held["sk"], held["ssm"], held["op"], held["mn"]

    def loaded(*names):
        for name in names:
            loads[name].wait()

    pending = []

    def remote(src, dst, send, recv, partner):
        return pltpu.make_async_remote_copy(
            src_ref=src, dst_ref=dst, send_sem=send, recv_sem=recv, device_id=partner, device_id_type=MESH
        )

    def exchange(stage, group, pair, landing, first=None):
        at = STAGES.index(stage)
        for k in by_distance(len(group) + 1):
            if first is not None:
                first(k)
            src, dst = pair(k)
            remote(src, dst, send_sem.at[at], recv_sem.at[at], group[k]).start()
        pending.append(pltpu.make_async_copy(landing, landing, send_sem.at[at]))
        return pltpu.make_async_copy(landing, landing, recv_sem.at[at])

    def arrive(copy):
        copy.wait()

    def by_pieces(name, group, view, own, count, near_landing, side_landing, at):
        near_at, side_at = STAGES.index(name + "_near"), STAGES.index(name + "_state")
        sent = {}
        order = by_distance(count)
        for k in order:
            sent[k] = remote(view(own), view(own), send_sem.at[near_at], piece_sem.at[at, k - 1], group[k])
            sent[k].start()
        for step in [0] + order[::-1]:
            piece = (own + count - step) % count
            if step:
                sent[step].wait_recv()
            for k in by_distance(X):
                remote(
                    view(piece), view(piece), send_sem.at[side_at], recv_sem.at[side_at], side[k]
                ).start()
        if order:
            pending.append(pltpu.make_async_copy(near_landing, near_landing, send_sem.at[near_at]))
        pending.append(pltpu.make_async_copy(side_landing, side_landing, send_sem.at[side_at]))
        return pltpu.make_async_copy(side_landing, side_landing, recv_sem.at[side_at])

    core, chip, chips = m % 2, m // 2, NM // 2
    partner = {"head": head + 1 - 2 * core}
    alike = {k: {"head": b * NM + (chip + k) % chips * 2 + core} for k in range(1, chips)}

    loaded("tok")
    pl.semaphore_wait(barrier, expected)

    @pl.when(b > 1)
    def _():
        pl.semaphore_signal(ready_up, inc=1, device_id={"head": head - NM}, device_id_type=MESH)

    @pl.when(b == 0)
    def _():
        pl.semaphore_signal(ready_zero, inc=1, device_id={"head": head + NM}, device_id_type=MESH)

    for k in near:
        source = (head + n.H - offset(k)) % n.H

        @pl.when(source < head)
        def _(k=k, source=source):
            pl.semaphore_signal(
                ready_near.at[k - 1], inc=1, device_id={"head": source}, device_id_type=MESH
            )

    own = G.at[m, b]
    downs = []
    for k in by_distance(NB):
        copy = remote(own, own, down_send.at[k - 1], down_recv.at[k - 1], {"head": head - k * NM})
        pl.when((b > k) | (b == k if k == top else False))(copy.start)
        downs.append((k, copy))
    climbing = b < NB - 1
    ups = [
        remote(G.at[m, k], G.at[m, k], up_send.at[k], up_recv.at[k], {"head": head + NM})
        for k in range(NB - 1)
    ]

    @pl.when((b > 0) & climbing)
    def _():
        pl.semaphore_wait(ready_up, 1)

    around_top = remote(G.at[m, 0], G.at[m, 0], wrap_sem.at[1], wrap_sem.at[0], {"head": top * NM + m})
    descents = [
        remote(G.at[m, 0], G.at[m, 0], wrap_sem.at[1 + k], wrap_sem.at[0], {"head": head - k * NM})
        for k in range(1, top - NB // 2)
    ]
    below = b < NB // 2

    @pl.when(b == top)
    def _():
        pl.semaphore_signal(ready_wrap, inc=1, device_id={"head": m}, device_id_type=MESH)
        around_top.wait_recv()
        for copy in descents:
            copy.start()

    for k in range(NB - 2, 0, -1):
        pl.when(k < b)(ups[k].wait_recv)
        pl.when((k <= b) & climbing)(ups[k].start)
    pl.when((b > 0) & (b <= NB // 2))(ups[0].wait_recv)
    pl.when(below)(ups[0].start)

    @pl.when(b == 0)
    def _():
        pl.semaphore_wait(ready_wrap, 1)
        around_top.start()

    @pl.when((b > NB // 2) & (b < top))
    def _():
        around_top.wait_recv()

    onward = [
        remote(G.at[m, k], G.at[m, k], onward_send.at[k - 1], down_recv.at[k - 1], {"head": head - NM})
        for k in range(1, top)
    ]

    def from_above(last):
        for k, copy in sorted(downs, key=lambda t: t[0]):
            pl.when((b + k == NB - 1) if last else (b + k < NB - 1))(copy.wait_recv)
            if not last and k < top - 1:
                pl.when(b == 1)(onward[k].start)

    @pl.when(b == 1)
    def _():
        pl.semaphore_wait(ready_zero, 1)
        onward[0].start()

    def near_ready(k):
        target = (head + n.H + offset(k)) % n.H

        @pl.when(target > head)
        def _():
            pl.semaphore_wait(ready_near.at[k - 1], 1)

    from_above(False)
    early = G.at[m, 0 : NB - 1]
    sent_early = exchange(
        "tok_near", near, lambda k: (early, early), G.at[0 : NM - 1, 0 : NB - 1], near_ready
    )
    tok_bf = G[m, b]

    per = NM * OWN
    r_i, c_i = grid_of(NM * R, NM * R)
    pick[...] = ones_where(
        (mod(div(c_i, OWN), J) == div(r_i, per)) & (div(c_i, R) * OWN + mod(c_i, OWN) == mod(r_i, per))
    )
    pair = 2 * NB * CAP
    r_i, c_i = grid_of(pair * J, pair * J)
    pick_row[...] = ones_where(
        (mod(div(c_i, CAP), J) == div(r_i, pair))
        & (div(c_i, J * CAP) * CAP + mod(c_i, CAP) == mod(r_i, pair))
    )

    from_above(True)
    final = G.at[m, NB - 1]
    sent = exchange("tok_last", near, lambda k: (final, final), G.at[0, 0 : NM - 1])
    loaded("win", "mixn")
    arrive(sent_early)
    arrive(sent)

    by_block = [mm(pick[...], G[:, k].reshape(NM * R, LANES)) for k in range(NB)]
    conv_part = jnp.zeros((T, C), F32)
    gate_part = jnp.zeros((T, C), F32)
    squares = jnp.zeros((T, 1), F32)
    for j in range(J):
        tok_j = jnp.concatenate([rows_k[j * per : (j + 1) * per] for rows_k in by_block], axis=0)
        squares += jnp.sum(tok_j * tok_j, axis=1, keepdims=True)
        wide = tok_j * mixn_ref[j : j + 1, :]
        high = wide.astype(BF16)
        for half in (high, (wide - high.astype(F32)).astype(BF16)):
            conv_part += mm(half, win[0, j * LANES : (j + 1) * LANES, :])
            gate_part += mm(half, win[1, j * LANES : (j + 1) * LANES, :])
    XS[x] = jnp.broadcast_to(squares, (T, LANES)).T[:8, :]
    XC[x] = conv_part.astype(BF16)
    sent_sq = exchange("square", side, lambda k: (XS.at[x], XS.at[x]), XS.at[0 : X - 1])
    sent = exchange("branch", side, lambda k: (XC.at[x], XC.at[x]), XC.at[0 : X - 1])
    XG[x] = gate_part.astype(BF16)
    sent_gate = exchange("gate", side, lambda k: (XG.at[x], XG.at[x]), XG.at[0 : X - 1])

    loaded("conv", "keep", "cw", "cb", "sp")
    window = cb_ref[...] + cw_ref[0:1, :] * cs[...]
    for k in range(n.CONV - 2):
        window += cw_ref[k + 1 : k + 2, :] * nc_ref[k]
    P2[...] = jnp.zeros_like(P2)
    arrive(sent_sq)
    total = XS[0]
    for k in range(1, X):
        total += XS[k]
    inv_first = lax.rsqrt(jnp.broadcast_to(total[:1, :], (LANES, T)).T[:, :1] / n.D + NORM_EPS)
    arrive(sent)
    conv_in = XC[0].astype(F32)
    for k in range(1, X):
        conv_in += XC[k].astype(F32)
    conv_in = conv_in * inv_first
    nc_ref[n.CONV - 2] = conv_in
    conv_out = silu(window + cw_ref[n.CONV - 1 : n.CONV, :] * conv_in)
    cob[...] = conv_out.astype(BF16)

    quarter = T // X
    spare = n.PROJ - n.RANK

    def in_halves(wide):
        low, vectors = wide[:, : n.RANK], wide[:, n.RANK :]
        high = vectors.astype(BF16).astype(F32)
        rest = pltpu.roll(vectors - high, spare, 1)
        return jnp.concatenate([low, high + rest], axis=1).astype(BF16)

    part = mm_nt(cob[pl.ds(pl.multiple_of(x * quarter, quarter), quarter), :], sp[...])
    P2[:, :, : n.PROJ] = part.reshape(NM, n.TB, n.PROJ)
    R2[m] = P2[m]
    sent = exchange("proj_near", near, lambda k: (P2.at[(m + k) % NM], R2.at[m]), R2.at[0 : NM - 1])
    arrive(sent)
    total = R2[0]
    for k in range(1, NM):
        total += R2[k]
    F2[b] = in_halves(total)
    sent = exchange("proj_far", far, lambda k: (F2.at[b], F2.at[b]), F2.at[0 : NB - 1])
    loaded("tp", "ssm", "sg", "sb", "dl")
    arrive(sent)
    total = F2[0].astype(F32)
    for k in range(1, NB):
        total += F2[k].astype(F32)
    low, vectors = total[:, : n.RANK], total[:, n.RANK :]
    step_inv = lax.rsqrt(jnp.mean(low * low, axis=1, keepdims=True) + STEP_EPS)
    vectors = vectors + pltpu.roll(vectors, LANES - spare, 1)
    _, l_i = grid_of(n.TB, LANES)
    vectors = jnp.where(l_i < spare, vectors, 0.0)
    S2[x, m] = in_halves(jnp.concatenate([low * step_inv * sg_ref[...], vectors], axis=1))
    sent = by_pieces("low", near, lambda p: S2.at[x, p], m, NM, S2.at[0, 0 : NM - 1], S2.at[0 : X - 1], 0)
    arrive(sent_gate)
    gate = gate_part
    for k in range(1, X):
        gate += XG[(x + k) % X].astype(F32)
    gate = silu(gate * inv_first)
    rates = [jnp.exp(dl_ref[k : k + 1, :]) for k in range(S)]
    arrive(sent)

    projected = S2[...].astype(F32).reshape(T, n.PW)
    step_normed = projected[:, : n.RANK].astype(BF16)
    step_size = softplus(mm(step_normed, tp[...]) + sb_ref[...])
    vectors = projected[:, n.RANK :].astype(BF16)
    rows_i, _ = grid_of(LANES, C)
    driven = step_size * conv_out
    read = jnp.zeros((T, C), F32)
    for k in range(S):
        at = x * S + k
        b_in = mm(vectors, ones_where((rows_i == at) | (rows_i == spare + at)))
        at = at + n.STATE
        c_out = mm(vectors, ones_where((rows_i == at) | (rows_i == spare + at)))
        fresh = jnp.exp(-step_size * rates[k]) * ssm[k] + driven * b_in
        ns_ref[k] = fresh
        read += c_out * fresh
    XR[x] = read.astype(BF16)
    sent = exchange("read", side, lambda k: (XR.at[x], XR.at[x]), XR.at[0 : X - 1])
    loaded("op", "sk")
    r_i, c_i = grid_of(T, T)
    source = (div(mod(r_i, NB * OWN), OWN) * NM + div(r_i, NB * OWN)) * OWN + mod(r_i, OWN)
    by_member = ones_where(source == c_i)
    arrive(sent)
    for k in range(1, X):
        read += XR[(x + k) % X].astype(F32)
    act = ((read + sk_ref[...] * conv_out) * gate).astype(BF16)
    act = mm(by_member, act).astype(BF16)
    N3[...] = mm(act, op[...]).astype(BF16).reshape(NM, NB * OWN, n.Q)
    R3[m] = N3[m]
    sent = exchange("mix_near", near, lambda k: (N3.at[(m + k) % NM], R3.at[m]), R3.at[0 : NM - 1])
    r_i, c_i = grid_of(NB * R, NB * OWN)
    match = div(r_i, R) * OWN + mod(r_i, OWN) == c_i
    which = mod(div(r_i, OWN), J)
    to_owner = [ones_where(match & (which == j)) for j in range(J)]
    arrive(sent)
    total = R3[0].astype(F32)
    for k in range(1, NM):
        total += R3[k].astype(F32)
    total = total.astype(BF16)
    spread = jnp.zeros((NB * R, LANES), F32)
    for j in range(J):
        spread += mm(to_owner[j], total[:, j * LANES : (j + 1) * LANES])
    F3[...] = spread.astype(BF16).reshape(NB, R, LANES)
    Q3[b] = F3[b]
    sent = exchange("mix_far", far, lambda k: (F3.at[(b + k) % NB], Q3.at[b]), Q3.at[0 : NB - 1])
    loaded("router", "mn", "eid", "sid")
    row_i, lane_i = grid_of(R, LANES)
    hits, kept, slots = [], [], []
    i_i, t_i = grid_of(R, OWN)

    def by_row(ref, k):
        wide = jnp.broadcast_to(ref[k : k + 1, :], (R, OWN)).astype(F32)
        return jnp.sum(jnp.where(mod(i_i, OWN) == t_i, wide, 0.0), axis=1, keepdims=True).astype(jnp.int32)

    for k in range(TOPK):
        e_k, s_k = by_row(held["eid"], k), by_row(held["sid"], k)
        keep = s_k < CAP
        hits.append(lane_i == e_k)
        kept.append(keep)
        slots.append((lane_i == e_k * CAP + s_k) & keep)
    dispatch = sum(ones_where(s, F32) for s in slots).astype(BF16)
    d_i, q_i = grid_of(NB * J * CAP, LANES)
    slot_of = ones_where(q_i == div(d_i, J * CAP) * CAP + mod(d_i, CAP))
    d_i, c_i = grid_of(NB * J * CAP, R)
    chosen_rows = jnp.where(
        mod(div(d_i, CAP), J) == div(c_i, OWN), mm_nt(slot_of, dispatch), 0.0
    ).astype(BF16)
    arrive(sent)
    total = Q3[0].astype(F32)
    for k in range(1, NB):
        total += Q3[k].astype(F32)

    resid_bf = (tok_bf.astype(F32) + total).astype(BF16)
    resid = resid_bf.astype(F32)
    F4[...] = mm(chosen_rows, resid_bf).reshape(NB, J * CAP, LANES).astype(BF16)
    G4[x, core, chip, b] = F4[b]
    own = G4.at[x, core, chip, b]
    sent = exchange(
        "row_far", far, lambda k: (F4.at[(b + k) % NB], own), G4.at[x, core, chip, 0 : NB - 1]
    )

    gain = jnp.zeros((R, LANES), F32)
    for j in range(J):
        gain = jnp.where(div(row_i, OWN) == j, mn_ref[pl.ds(x * J + j, 1), :], gain)
    scaled = resid * gain
    raw = jnp.zeros((R, EXPERTS), F32)
    for j in range(J):
        raw += mm_nt(
            jnp.where(div(row_i, OWN) == j, scaled, 0.0), rw[:, j * LANES : (j + 1) * LANES], HI
        )
    ST[x] = jnp.broadcast_to(jnp.sum(resid * resid, axis=1, keepdims=True), (R, LANES))
    ST[x, :, :EXPERTS] = raw
    sent_stat = exchange("stat", side, lambda k: (ST.at[x], ST.at[x]), ST.at[0 : X - 1])
    arrive(sent_stat)
    total = ST[0]
    for k in range(1, X):
        total += ST[k]
    r_i, c_i = grid_of(R, R)
    total = mm(ones_where(mod(r_i, OWN) == mod(c_i, OWN), F32), total, HI)
    inv_second = lax.rsqrt(total[:, EXPERTS : EXPERTS + 1] / n.D + NORM_EPS)
    logits = inv_second * total
    chosen = [jnp.sum(jnp.where(hit, logits, 0.0), axis=1, keepdims=True) for hit in hits]
    mixing = jnp.zeros((R, LANES), F32)
    for k in range(TOPK):
        weight = jax.nn.sigmoid(chosen[k] - chosen[1 - k])
        mixing += jnp.where(slots[k], weight, 0.0)
    first = row_i < OWN
    load = sum(ones_where(hits[k] & kept[k] & first, F32) for k in range(TOPK))
    load = jnp.sum(load, axis=0, keepdims=True)
    prob = jnp.where(first & (lane_i < EXPERTS), jax.nn.sigmoid(logits), 0.0)
    prob = jnp.sum(prob, axis=0, keepdims=True)
    a_i, l_i = grid_of(8, LANES)
    AN[m] = jnp.where(a_i == 0, load, jnp.where(a_i == 1, prob, 0.0))
    sent_aux = exchange("aux_near", block, lambda k: (AN.at[m], AN.at[m]), AN.at[0 : NM - 1])
    d_i, q_i = grid_of(R, NB * J * CAP)
    combine = jnp.where(
        mod(div(q_i, CAP), J) == div(d_i, OWN), mm_nt(mixing, slot_of.astype(F32), HI), 0.0
    )
    loaded("gp", "up", "dn")

    arrive(sent)

    sideways = by_pieces(
        "row", alike, lambda p: G4.at[x, core, p], chip, chips, G4.at[0, 0, 0 : chips - 1],
        G4.at[0 : X - 1, 0], 1,
    )
    pair_at = STAGES.index("row_pair")

    def swap(at):
        rows_at = G4.at[at, core]
        remote(rows_at, rows_at, send_sem.at[pair_at], recv_sem.at[pair_at], partner).start()

    swap(x)
    arrive(sent_aux)
    total = AN[0]
    for k in range(1, NM):
        total += AN[k]
    AF[b] = total
    sent_aux = exchange("aux_far", far, lambda k: (AF.at[b], AF.at[b]), AF.at[0 : NB - 1])
    arrive(sideways)
    for k in range(1, X):
        swap((x + k) % X)
    landing = G4.at[0:X, 0]
    pending.append(pltpu.make_async_copy(landing, landing, send_sem.at[pair_at]))
    arrive(pltpu.make_async_copy(landing, landing, recv_sem.at[pair_at]))

    squares = jnp.zeros((n.SLOTS, 1), F32)
    for k in range(X):
        source = G4[k].astype(F32).reshape(n.SLOTS * J, LANES).astype(BF16)
        by_pair = [
            mm(pick_row[...], source[at : at + pair * J]) for at in range(0, n.SLOTS * J, pair * J)
        ]
        for j in range(J):
            at = k * J + j
            part = jnp.concatenate([rows_k[j * pair : (j + 1) * pair] for rows_k in by_pair], axis=0)
            squares += jnp.sum(part * part, axis=1, keepdims=True)
            rows[:, at * LANES : (at + 1) * LANES] = part * mn_ref[at : at + 1, :]
    inv_rows = lax.rsqrt(squares / n.D + NORM_EPS)
    rn[...] = (rows[...] * inv_rows).astype(BF16)
    normed = rn[...]
    hidden = (silu(mm_nt(normed, held["gp"][0])) * mm_nt(normed, held["up"][0])).astype(BF16)

    half = n.SLOTS // 2
    pair_at = STAGES.index("out_pair")
    for k in by_distance(X) + [0]:
        at = (x + k) % X
        columns = pl.ds(pl.multiple_of(at * n.Q, n.Q), n.Q)
        X5[at] = mm(hidden, held["dn"][0, :, columns]).astype(BF16).reshape(2, half, n.Q)
        remote(
            X5.at[at, 1 - core], W5.at[at], send_sem.at[pair_at], recv_sem.at[pair_at],
            partner,
        ).start()
    pending.append(pltpu.make_async_copy(W5, W5, send_sem.at[pair_at]))
    arrive(pltpu.make_async_copy(W5, W5, recv_sem.at[pair_at]))

    def both(k):
        at = (x + k) % X
        V5[at] = (X5[at, core].astype(F32) + W5[at].astype(F32)).astype(BF16)

    sent = exchange("out_state", side, lambda k: (V5.at[(x + k) % X], Y5.at[x]), Y5.at[0 : X - 1], both)
    both(0)
    Y5[x] = V5[x]
    r_i, c_i = grid_of(NB * J * CAP, NB * CAP)
    match = div(r_i, J * CAP) * CAP + mod(r_i, CAP) == c_i
    which = mod(div(r_i, CAP), J)
    to_home = [ones_where(match & (which == j)) for j in range(J)]
    arrive(sent)
    total = Y5[0].astype(F32)
    for k in range(1, X):
        total += Y5[k].astype(F32)
    N5[...] = total.astype(BF16).reshape(chips, NB * CAP, n.Q)
    R5[chip] = N5[chip]
    if chips > 1:
        sent = exchange(
            "out_near", alike, lambda k: (N5.at[(chip + k) % chips], R5.at[chip]), R5.at[0 : chips - 1]
        )
        arrive(sent)
    total = R5[0].astype(F32)
    for k in range(1, chips):
        total += R5[k].astype(F32)
    total = total.astype(BF16)
    spread = jnp.zeros((NB * J * CAP, LANES), F32)
    for j in range(J):
        spread += mm(to_home[j], total[:, j * LANES : (j + 1) * LANES])
    F5[...] = spread.reshape(NB, J * CAP, LANES).astype(BF16)
    Q5[b] = F5[b]
    sent = exchange("out_far", far, lambda k: (F5.at[(b + k) % NB], Q5.at[b]), Q5.at[0 : NB - 1])
    arrive(sent_aux)
    total = AF[0]
    for k in range(1, NB):
        total += AF[k]
    share = total[0:1, :] / (T * TOPK) * (total[1:2, :] / T)
    loss = EXPERTS * jnp.sum(jnp.where(l_i[:1] < EXPERTS, share, 0.0), axis=1, keepdims=True)
    load_ref[...] = total[0:1, :EXPERTS]
    loss_ref[...] = loss
    arrive(sent)
    back = Q5[...].astype(F32).reshape(NB * J * CAP, LANES)
    lo_ref[...] = (resid + mm(combine, back, HI)).astype(BF16)
    for copy in pending:
        copy.wait()
    for k, copy in downs:
        pl.when((b > k) | (b == k if k == top else False))(copy.wait_send)
        if k < top:
            pl.when(b == 1)(onward[k - 1].wait_send)
    for k in range(1, NB - 1):
        pl.when((k <= b) & climbing)(ups[k].wait_send)
    pl.when(below)(ups[0].wait_send)
    pl.when(b == 0)(around_top.wait_send)
    for copy in descents:
        pl.when(b == top)(copy.wait_send)


def finish_kernel(*refs):
    count = len(refs) // 2
    copies = [
        pltpu.make_async_copy(refs[k], refs[count + k], refs[-1].at[k]) for k in range(count)
    ]
    for copy in copies:
        copy.start()
    for copy in copies:
        copy.wait()


class Sizes:
    pass


def per_device(
    head_count, state_count,
    tokens, mixer_norm, input_proj, conv_weight, conv_bias, conv_state, state_proj, step_gain, step_proj,
    step_bias, decay_log, skip_gain, ssm_state, output_proj, moe_norm, router_weight, expert_ids, slot_ids,
    gate_proj, up_proj, down_proj,
):
    n = Sizes()
    n.H, n.X, n.NB = head_count, state_count, EXPERTS
    n.NM = n.H // n.NB
    n.OWN, n.Q = tokens.shape
    n.J = n.Q // LANES
    n.R = n.OWN * n.J
    n.D = n.Q * n.X
    n.CONV = conv_weight.shape[0]
    _, n.T, n.C = conv_state.shape
    n.S = decay_log.shape[0]
    n.STATE = n.S * n.X
    n.RANK, n.PROJ = step_proj.shape[0], state_proj.shape[1]
    n.PW = -(-n.PROJ // LANES) * LANES
    n.TB = n.T // n.X // n.NM
    n.SLOTS = n.NM * n.NB * CAP
    n.FF = gate_proj.shape[2]

    tok = tokens.reshape(n.OWN, n.J, LANES).transpose(1, 0, 2).reshape(n.R, LANES)
    V = pltpu.VMEM
    operands = (
        mixer_norm.reshape(n.J, LANES), input_proj, conv_weight, conv_bias.reshape(1, -1), state_proj.T,
        step_gain.reshape(1, -1), step_proj, step_bias.reshape(1, -1), decay_log, skip_gain.reshape(1, -1),
        ssm_state, output_proj, moe_norm.reshape(-1, LANES), expert_ids.T, slot_ids.T,
        gate_proj.transpose(0, 2, 1), up_proj.transpose(0, 2, 1), down_proj,
    )
    vm = pl.BlockSpec(memory_space=pltpu.VMEM)
    hbm = pl.BlockSpec(memory_space=pltpu.HBM)
    wide = n.J * CAP
    scratch = [V(a.shape, a.dtype) for a in operands]
    scratch += [
        V(conv_state.shape[1:], F32), V((EXPERTS, n.Q), F32),
        V((n.NM * n.R, n.NM * n.R), BF16),
        V((2 * n.NB * wide, 2 * n.NB * wide), BF16),
        V((n.NM, n.NB, n.R, LANES), BF16),
        V((n.X, n.T, n.C), BF16), V((n.X, n.T, n.C), BF16),
        V((n.X, 8, n.T), F32),
        V((n.T, n.C), BF16),
        V((n.NM, n.TB, n.PW), F32), V((n.NM, n.TB, n.PW), F32),
        V((n.NB, n.TB, n.PW), BF16), V((n.X, n.NM, n.TB, n.PW), BF16),
        V((n.X, n.T, n.C), BF16),
        V((n.NM, n.NB * n.OWN, n.Q), BF16), V((n.NM, n.NB * n.OWN, n.Q), BF16),
        V((n.NB, n.R, LANES), BF16), V((n.NB, n.R, LANES), BF16),
        V((n.X, n.R, LANES), F32),
        V((n.NB, wide, LANES), BF16), V((n.X, 2, n.NM // 2, n.NB, wide, LANES), BF16),
        V((n.SLOTS, n.D), F32), V((n.SLOTS, n.D), BF16),
        V((n.X, 2, n.SLOTS // 2, n.Q), BF16), V((n.X, n.SLOTS // 2, n.Q), BF16),
        V((n.X, n.SLOTS // 2, n.Q), BF16), V((n.X, n.SLOTS // 2, n.Q), BF16),
        V((n.NM // 2, n.NB * CAP, n.Q), BF16), V((n.NM // 2, n.NB * CAP, n.Q), BF16),
        V((n.NB, wide, LANES), BF16), V((n.NB, wide, LANES), BF16),
        V((n.NM, 8, LANES), F32), V((n.NB, 8, LANES), F32),
    ]
    dma, regular = pltpu.SemaphoreType.DMA, pltpu.SemaphoreType.REGULAR
    climb = dma((n.NB - 1,))
    scratch += [
        dma((len(STAGES),)), dma((len(STAGES),)), dma((2, n.NM - 1)), climb, climb, climb, climb, climb,
        dma((n.NB,)), regular, regular, regular, regular((n.NM - 1,)), dma((len(OPERANDS) + 4,)),
    ]
    shapes = (
        jax.ShapeDtypeStruct((n.R, LANES), BF16),
        jax.ShapeDtypeStruct(conv_state.shape, F32),
        jax.ShapeDtypeStruct(ssm_state.shape, F32),
        jax.ShapeDtypeStruct((1, EXPERTS), F32),
        jax.ShapeDtypeStruct((1, 1), F32),
    )
    results = pl.pallas_call(
        functools.partial(step_kernel, n),
        out_shape=shapes,
        in_specs=[hbm] * (len(operands) + 3),
        out_specs=(vm,) * len(shapes),
        scratch_shapes=scratch,
        compiler_params=pltpu.CompilerParams(
            collective_id=0, has_side_effects=True, vmem_limit_bytes=48 * 1024 * 1024
        ),
        name="mixer_moe_step",
    )(*[pltpu.with_memory_space_constraint(a, pltpu.HBM) for a in (tok, conv_state, router_weight.T, *operands)])
    out, new_conv, new_state, load, loss = pl.pallas_call(
        finish_kernel,
        out_shape=shapes,
        in_specs=[vm] * len(shapes),
        out_specs=(hbm,) * len(shapes),
        scratch_shapes=[dma((len(shapes),))],
        compiler_params=pltpu.CompilerParams(vmem_limit_bytes=1024 * 1024),
        name="finish",
    )(*results)
    layer_out = out.reshape(n.J, n.OWN, LANES).transpose(1, 0, 2).reshape(n.OWN, n.Q)
    return layer_out, new_conv, new_state, load.reshape(-1), loss.reshape(1)


def solution(mesh):
    in_specs = (
        P(("groups", "head"), "state"),
        P("state"),
        P(None, "state", "head"),
        P(None, "head"),
        P("head"),
        P(None, "groups", "head"),
        P("head", None),
        P(),
        P(None, "head"),
        P("head"),
        P("state", "head"),
        P("head"),
        P("state", "groups", "head"),
        P("head", "state"),
        P(),
        P(),
        P(("groups", "head"), None),
        P(("groups", "head"), None),
        P("head", None, "state"),
        P("head", None, "state"),
        P("head", "state", None),
    )
    out_specs = (
        P(("groups", "head"), "state"),
        P(None, "groups", "head"),
        P("state", "groups", "head"),
        P("groups"),
        P("groups"),
    )
    return jax.shard_map(
        functools.partial(per_device, mesh.shape["head"], mesh.shape["state"]),
        mesh=mesh, in_specs=in_specs, out_specs=out_specs, check_vma=False,
    )
```
